128 devices in a mesh: group: 32 (over y, z, core), rep: 4 (over x).
Axes of the slice: x: 4, y: 4, z: 4, core: 2. Of those that a mesh axis runs over, the one named last changes fastest.
Arguments:
- grad_parts: bfloat16 [4, 96, 1024, 1024], P('rep', None, 'group'), may hold values from -40 to 40
- params: bfloat16 [96, 1024, 1024], P('rep', 'group'), may hold values from -6 to 6
- accum: float32 [96, 1024, 1024], P('rep', 'group'), may hold values from 1 to 50
- left_pre: bfloat16 [4, 32, 1, 1024, 1024], P('rep', 'group'), may hold values from -1 to 4
- right_pre: bfloat16 [4, 32, 1, 1024, 1024], P('rep', 'group'), may hold values from -1 to 4
- slot_block: int32 [4, 32, 1], replicated, may hold values from -1 to 23, as said below
- layer_of: int32 [96], replicated, may hold values from 0 to 7
Outputs:
- new_params: bfloat16 [96, 1024, 1024], P(None, 'group')
- new_accum: float32 [96, 1024, 1024], P('rep', 'group')
The draws below stay inside these ranges and needn't reach their ends.
Inputs may be any that keep to these rules, and one draw needn't show every extreme that they name: For every replica q each of its 24 blocks is named by exactly one slot of slot_block[q]; a device's used slots come first and the others hold -1; in every replica some device has all 1 slots used.
All inputs are finite; a program needn't handle non-finite values.
Results may differ from the reference program's by a relative error of at most 0.018.
Values may be sent and summed in bfloat16 or wider, within the bound.
No kernel may reach another device: no remote copies, remote signals or barrier semaphores. Data moves between devices by JAX's collectives and lax.ppermute only.
A program may use at most 128 MiB of HBM per device.

```python
import math
import jax
import jax.numpy as jnp
from jax import lax

B = 1024
SLOTS = 1
LAYERS = 8
RB = 24
NB = 96
N_GROUP = 32
N_REP = 4


def draw_grad_parts(key, part):
    key_noise, key_cols, key_blocks = jax.random.split(jax.random.fold_in(key, 11), 3)
    full_shape = (N_REP, NB, B, B)
    row_place = jnp.arange(B, dtype=jnp.float32) / (B - 1)
    col_scale = 10.0 ** (jax.random.uniform(key_cols, (B,), jnp.float32) - 0.5)
    block_scale = jnp.exp(jax.random.uniform(key_blocks, (NB,), jnp.float32, -1.6, 1.6))
    pattern = jax.random.normal(key_noise, full_shape, jnp.float32)
    row_scale = 10.0 ** (row_place - 0.5)
    drawn = pattern * row_scale[:, None] * col_scale[None, :] * block_scale[:, None, None]
    return jnp.clip(drawn, -40.0, 40.0).astype(jnp.bfloat16)


def precond_matrices(key, salt):
    key_noise, key_diagonal = jax.random.split(jax.random.fold_in(key, salt))
    full_shape = (N_REP, N_GROUP, SLOTS, B, B)
    noise = jnp.clip(jax.random.normal(key_noise, full_shape, jnp.float32), -6.0, 6.0)
    symmetric = (noise + jnp.swapaxes(noise, -1, -2)) * (0.45 / math.sqrt(2.0 * B))
    diagonal = jnp.exp(jax.random.uniform(key_diagonal, full_shape[:-1], jnp.float32, math.log(1.2), math.log(4.0)))
    on_diagonal = jnp.arange(B)[:, None] == jnp.arange(B)[None, :]
    return jnp.where(on_diagonal, diagonal[..., :, None], symmetric).astype(jnp.bfloat16)


def draw_left_pre(key, part):
    return precond_matrices(key, 21)


def draw_right_pre(key, part):
    return precond_matrices(key, 37)


def replica_table(replica_key):
    key_order, key_blocks = jax.random.split(replica_key, 2)
    device_order = jax.random.permutation(key_order, N_GROUP)
    device_rank = jnp.arange(N_GROUP, dtype=jnp.int32)
    owned = device_rank < RB
    block_order = jax.random.permutation(key_blocks, RB)
    block_position = jnp.clip(device_rank, 0, RB - 1)
    entries = jnp.where(owned, block_order[block_position], -1)[:, None]
    inverse = jnp.argsort(device_order, stable=True)
    return entries[inverse]


def draw_slot_block(key, part):
    replica_keys = jax.random.split(jax.random.fold_in(key, 5), N_REP)
    return jax.vmap(replica_table)(replica_keys).astype(jnp.int32)


def place_ends(array, stream_key, least, top_value):
    place = [jax.random.randint(jax.random.fold_in(stream_key, axis), (), 0, length) for axis, length in enumerate(array.shape)]
    longest = array.shape.index(max(array.shape))
    next_to = place[:longest] + [(place[longest] + 1) % array.shape[longest]] + place[longest + 1:]
    return array.at[tuple(place)].set(least).at[tuple(next_to)].set(top_value)


def shard_levels(own_key, extent, pieces, smallest, largest):
    def one(dim, blocks):
        draws = jax.random.uniform(jax.random.fold_in(jax.random.fold_in(own_key, 6), dim), (blocks,), jnp.float32, smallest / len(pieces), largest / len(pieces))
        return jnp.repeat(jnp.exp(draws), extent[dim] // blocks).reshape((-1,) + (1,) * (len(extent) - dim - 1))

    factor_of = one(*pieces[0])
    for cut in pieces[1:]:
        factor_of = factor_of * one(*cut)
    return factor_of


def bell_draw(key, shape, spread, bound, cuts=(), kind=jnp.bfloat16):
    array = spread * jax.random.normal(key, shape, jnp.float32)
    if cuts:
        array = array * shard_levels(key, shape, cuts, -0.22, 0.18)
    return jnp.clip(array, -bound, bound).astype(kind)


def setup_inputs(seed: int = 0) -> dict:
    streams_of = jax.random.split(jax.random.key(seed), 8)
    return {
        "grad_parts": draw_grad_parts(jax.random.fold_in(streams_of[7], 71), 0),
        "params": bell_draw(streams_of[1], (NB, B, B), 1.0, 6.0, ((0, 4), (1, 32))),
        "accum": jnp.clip(jnp.exp(math.log(50.0) - 3.912023 * jax.random.uniform(streams_of[2], (NB, B, B), jnp.float32) ** shard_levels(streams_of[2], (NB, B, B), ((0, 4), (1, 32)), -0.2, 0.2)), 1.0, 50.0),
        "left_pre": draw_left_pre(jax.random.fold_in(streams_of[7], 71), 0),
        "right_pre": draw_right_pre(jax.random.fold_in(streams_of[7], 71), 0),
        "slot_block": draw_slot_block(jax.random.fold_in(streams_of[7], 71), 0),
        "layer_of": place_ends(jax.random.randint(streams_of[6], (NB,), 0, LAYERS), jax.random.fold_in(streams_of[6], 1), 0, LAYERS - 1).astype(jnp.int32),
    }


step_rate = 0.5

def reference(grad_parts, params, accum, left_pre, right_pre, slot_block, layer_of):
    summed = jnp.zeros(grad_parts.shape[1:], jnp.float32)
    for replica in range(N_REP):
        summed = summed + grad_parts[replica].astype(jnp.float32)
    gradient = summed.astype(jnp.bfloat16)
    gradient_wide = gradient.astype(jnp.float32)
    new_accum = accum + gradient_wide * gradient_wide
    graft = gradient_wide * lax.rsqrt(new_accum)
    graft_blocks = lax.optimization_barrier(jnp.sum(graft * graft, axis=(1, 2)))
    flat_table = slot_block.reshape(-1)
    slot_total = flat_table.shape[0]
    owner_replica = jnp.arange(slot_total, dtype=jnp.int32) // (N_GROUP * SLOTS)
    global_block = jnp.where(flat_table >= 0, owner_replica * RB + flat_table, -1)
    position = lax.optimization_barrier(jnp.sum(jnp.where(global_block[None, :] == jnp.arange(NB, dtype=jnp.int32)[:, None], jnp.arange(slot_total, dtype=jnp.int32)[None, :], 0), axis=1)).astype(jnp.int32)
    lefts = left_pre.reshape(slot_total, B, B)
    rights = right_pre.reshape(slot_total, B, B)

    def one_block(block_index):
        slot_index = position[block_index]
        left_product = jnp.dot(lefts[slot_index], gradient[block_index], preferred_element_type=jnp.float32).astype(jnp.bfloat16)
        return jnp.dot(left_product, rights[slot_index], preferred_element_type=jnp.float32).astype(jnp.bfloat16)
    precond = lax.map(one_block, jnp.arange(NB, dtype=jnp.int32))
    precond_wide = precond.astype(jnp.float32)
    shampoo_blocks = lax.optimization_barrier(jnp.sum(precond_wide * precond_wide, axis=(1, 2)))
    onehot = (layer_of[:, None] == jnp.arange(LAYERS, dtype=jnp.int32)[None, :]).astype(jnp.float32)
    graft_sq = lax.optimization_barrier(jnp.sum(onehot * graft_blocks[:, None], axis=0))
    shampoo_sq = lax.optimization_barrier(jnp.sum(onehot * shampoo_blocks[:, None], axis=0))
    layer_scale = jnp.sqrt(graft_sq) * lax.rsqrt(shampoo_sq + 1e-06)
    block_scale = lax.optimization_barrier(jnp.sum(onehot * layer_scale[None, :], axis=1))
    new_params = (params.astype(jnp.float32) - step_rate * block_scale[:, None, None] * precond_wide).astype(jnp.bfloat16)
    return (new_params, new_accum)
```

```python
import jax
import jax.numpy as jnp
from jax import lax
from jax.sharding import Mesh
from jax.sharding import PartitionSpec as P

LAYERS = 8
GROUP = ("group_0", "group_1", "group_2")
EVERY = ("group_0", "group_1", "group_2", "rep")
CHUNKS = 2


step_rate = 0.5


def ring(count, step):
    return [(i, (i + step) % count) for i in range(count)]


def local(grad_parts, params, accum, left_pre, right_pre, slot_block, layer_of):
    group_size = lax.axis_size(GROUP)
    reps = lax.axis_size("rep")
    me = lax.axis_index("rep")
    group_index = lax.axis_index(GROUP)
    blocks, rows, width = params.shape
    half = blocks // 2
    cols = width // CHUNKS
    up, down = ring(reps, 1), ring(reps, -1)
    parts = grad_parts[0].reshape(reps, blocks, rows, width)
    table = lax.dynamic_index_in_dim(slot_block, me, 0, keepdims=False).reshape(-1)
    wanted = jnp.maximum(table, 0)
    left, right = left_pre[0, 0, 0], right_pre[0, 0, 0]

    def part(offset, first, start):
        who = lax.rem(me + offset, reps)
        return lax.dynamic_slice(parts, (who, first, 0, start), (1, half, rows, cols))[0]

    def plus(*terms):
        total = terms[0].astype(jnp.float32)
        for term in terms[1:]:
            total = total + term.astype(jnp.float32)
        return total.astype(jnp.bfloat16)

    gradients, owned = [], []
    for chunk in range(CHUNKS):
        start = chunk * cols
        far_up = lax.ppermute(part(2, 0, start), "rep", up)
        far_down = lax.ppermute(part(2, half, start), "rep", down)
        near_up = lax.ppermute(part(1, half, start), "rep", up)
        near_down = lax.ppermute(part(3, 0, start), "rep", down)
        both_up = lax.ppermute(plus(part(1, 0, start), far_up), "rep", up)
        both_down = lax.ppermute(plus(part(3, half, start), far_down), "rep", down)
        low = plus(part(0, 0, start), near_down, both_up)
        high = plus(part(0, half, start), near_up, both_down)
        gradient = jnp.concatenate([low, high], axis=0)
        gradients.append(gradient)
        outgoing = jnp.take(gradient, wanted, axis=0)
        arrived = lax.all_to_all(outgoing, GROUP, split_axis=0, concat_axis=0, tiled=True)
        owned.append(arrived.reshape(group_size * rows, cols))

    my_layers = lax.dynamic_slice_in_dim(layer_of, me * blocks, blocks)
    onehot = (my_layers[:, None] == jnp.arange(LAYERS, dtype=jnp.int32)[None, :]).astype(jnp.float32)
    wide = jnp.concatenate(gradients, axis=2).astype(jnp.float32)
    new_accum = accum + wide * wide
    graft = wide * lax.rsqrt(new_accum)
    graft_blocks = jnp.sum(graft * graft, axis=(1, 2))
    graft_layer = jnp.sum(onehot * graft_blocks[:, None], axis=0)

    total = None
    for chunk in range(CHUNKS):
        product = jnp.dot(left, owned[chunk], preferred_element_type=jnp.float32).astype(jnp.bfloat16)
        term = jnp.dot(product, right[chunk * cols : (chunk + 1) * cols], preferred_element_type=jnp.float32)
        total = term if total is None else total + term
    precond = total.astype(jnp.bfloat16)
    squares = jnp.sum(jnp.square(precond.astype(jnp.float32)))
    mine = lax.dynamic_index_in_dim(table, group_index, 0, keepdims=False)
    chosen = (jnp.arange(blocks, dtype=jnp.int32) == mine).astype(jnp.float32)
    shampoo_layer = jnp.sum(chosen[:, None] * onehot, axis=0) * squares
    sums = lax.psum(jnp.stack([graft_layer, shampoo_layer]), EVERY)
    layer_scale = jnp.sqrt(sums[0]) * lax.rsqrt(sums[1] + 1e-06)
    block_scale = step_rate * jnp.sum(onehot * layer_scale[None, :], axis=1)
    position = jnp.sum(
        jnp.where(
            table[None, :] == jnp.arange(blocks, dtype=jnp.int32)[:, None],
            jnp.arange(group_size, dtype=jnp.int32)[None, :],
            0,
        ),
        axis=1,
    )

    new_params = jnp.zeros((reps, blocks, rows, width), jnp.bfloat16)
    for chunk in range(CHUNKS):
        start = chunk * cols
        outgoing = precond[:, start : start + cols].reshape(group_size, rows, cols)
        returned = lax.all_to_all(outgoing, GROUP, split_axis=0, concat_axis=0, tiled=True)
        picked = jnp.take(returned, position, axis=0)
        updated = (
            params[:, :, start : start + cols].astype(jnp.float32)
            - block_scale[:, None, None] * picked.astype(jnp.float32)
        ).astype(jnp.bfloat16)
        low, high = updated[:half], updated[half:]
        low_up = lax.ppermute(low, "rep", up)
        high_down = lax.ppermute(high, "rep", down)
        high_up = lax.ppermute(high, "rep", up)
        low_down = lax.ppermute(low, "rep", down)
        far_low = lax.ppermute(low_up, "rep", up)
        far_high = lax.ppermute(high_down, "rep", down)
        for offset, first, piece in (
            (0, 0, updated),
            (3, 0, low_up),
            (3, half, high_up),
            (1, 0, low_down),
            (1, half, high_down),
            (2, 0, far_low),
            (2, half, far_high),
        ):
            who = lax.rem(me + offset, reps)
            new_params = lax.dynamic_update_slice(new_params, piece[None], (who, first, 0, start))
    return (new_params.reshape(reps * blocks, rows, width), new_accum)


def solution(mesh):
    split = Mesh(mesh.devices.reshape(4, 4, 2, mesh.shape["rep"]), EVERY)
    placed = (
        P("rep", None, GROUP, None),
        P("rep", GROUP, None),
        P("rep", GROUP, None),
        P("rep", GROUP, None, None, None),
        P("rep", GROUP, None, None, None),
        P(),
        P(),
    )
    return jax.shard_map(
        local,
        mesh=split,
        in_specs=placed,
        out_specs=(P(None, GROUP, None), P("rep", GROUP, None)),
        check_vma=False,
    )
```

```python
import jax
import jax.numpy as jnp
from jax import lax
from jax.experimental import pallas as pl
from jax.experimental.pallas import tpu as pltpu
from jax.sharding import Mesh
from jax.sharding import PartitionSpec as P


LAYERS = 8
GROUP = ("group_0", "group_1", "group_2")
EVERY = ("group_0", "group_1", "group_2", "rep")
LANES = 128
SENT = (512, 512)
RETURNED = (512, 512)


step_rate = 0.5
f32 = jnp.float32
bf16 = jnp.bfloat16


def ring(count, step):
    return [(i, (i + step) % count) for i in range(count)]


def starts(widths):
    return [sum(widths[:i]) for i in range(len(widths))]


def merge(who, parts, far_up, far_down, start, cols):
    _, blocks, rows, _ = parts.shape
    half = blocks // 2
    first = start // LANES

    def body(who_ref, above, below, from_down, from_up, out_up, out_down):
        low = above[0, :half].astype(f32) + from_down[...].astype(f32)
        out_up[:half] = low.astype(bf16)
        out_up[half:] = above[0, half:]
        out_down[:half] = below[0, :half]
        high = below[0, half:].astype(f32) + from_up[...].astype(f32)
        out_down[half:] = high.astype(bf16)

    piece = pl.BlockSpec((half, rows, LANES), lambda i, w: (0, 0, i))
    whole = pl.BlockSpec((blocks, rows, LANES), lambda i, w: (0, 0, i))
    shape = jax.ShapeDtypeStruct((blocks, rows, cols), bf16)
    return pl.pallas_call(
        body,
        grid_spec=pltpu.PrefetchScalarGridSpec(
            num_scalar_prefetch=1,
            grid=(cols // LANES,),
            in_specs=[
                pl.BlockSpec((1, blocks, rows, LANES), lambda i, w: (w[1], 0, 0, first + i)),
                pl.BlockSpec((1, blocks, rows, LANES), lambda i, w: (w[3], 0, 0, first + i)),
                piece,
                piece,
            ],
            out_specs=[whole, whole],
        ),
        out_shape=[shape, shape],
        name="merge",
    )(who, parts, parts, far_up, far_down)


def finish(who, table, parts, up, down, start, cols):
    _, blocks, rows, _ = parts.shape
    slots = table.shape[0]
    first = start // LANES

    def body(who_ref, table_ref, own, one, two, gradient, slotted):
        total = own[0].astype(f32) + one[...].astype(f32) + two[...].astype(f32)
        gradient[...] = total.astype(bf16)
        for slot in range(slots):
            slotted[slot] = gradient[table_ref[slot]]

    block = pl.BlockSpec((blocks, rows, LANES), lambda i, w, t: (0, 0, i))
    return pl.pallas_call(
        body,
        grid_spec=pltpu.PrefetchScalarGridSpec(
            num_scalar_prefetch=2,
            grid=(cols // LANES,),
            in_specs=[
                pl.BlockSpec((1, blocks, rows, LANES), lambda i, w, t: (w[0], 0, 0, first + i)),
                block,
                block,
            ],
            out_specs=[block, pl.BlockSpec((slots, rows, LANES), lambda i, w, t: (0, 0, i))],
        ),
        out_shape=[
            jax.ShapeDtypeStruct((blocks, rows, cols), bf16),
            jax.ShapeDtypeStruct((slots, rows, cols), bf16),
        ],
        name="finish",
    )(who, table, parts, up, down)


def left_times(left, owned):
    order, cols = owned.shape
    tile = order // 4

    def body(left_ref, owned_ref, out):
        out[...] = jnp.dot(left_ref[...], owned_ref[...], preferred_element_type=f32).astype(bf16)

    return pl.pallas_call(
        body,
        grid=(4,),
        in_specs=[
            pl.BlockSpec((tile, order), lambda i: (i, 0)),
            pl.BlockSpec((order, cols), lambda i: (0, 0)),
        ],
        out_specs=pl.BlockSpec((tile, cols), lambda i: (i, 0)),
        out_shape=jax.ShapeDtypeStruct((order, cols), bf16),
        name="left_times",
    )(left, owned)


def products(left, right, owned, earlier):
    order, cols = owned.shape
    tile = order // 4
    offsets = starts(SENT)

    def body(left_ref, right_ref, owned_ref, *rest):
        before, outs, squares = rest[: len(earlier)], rest[len(earlier) : -1], rest[-1]
        last = jnp.dot(left_ref[...], owned_ref[...], preferred_element_type=f32).astype(bf16)
        total = jnp.dot(last, right_ref[offsets[-1] :], preferred_element_type=f32)
        for ref, at, size in zip(before, offsets, SENT):
            total += jnp.dot(ref[...], right_ref[at : at + size], preferred_element_type=f32)
        rounded = total.astype(bf16)
        for out, at, size in zip(outs, starts(RETURNED), RETURNED):
            out[...] = rounded[:, at : at + size]
        wide = rounded.astype(f32)
        part = jnp.sum(jnp.sum(wide * wide, axis=0, keepdims=True), axis=1, keepdims=True)

        @pl.when(pl.program_id(0) == 0)
        def _():
            squares[...] = jnp.zeros_like(squares)

        squares[...] += part

    return pl.pallas_call(
        body,
        grid=(4,),
        in_specs=[
            pl.BlockSpec((tile, order), lambda i: (i, 0)),
            pl.BlockSpec((order, order), lambda i: (0, 0)),
            pl.BlockSpec((order, cols), lambda i: (0, 0)),
            *[pl.BlockSpec((tile, e.shape[1]), lambda i: (i, 0)) for e in earlier],
        ],
        out_specs=[
            *[pl.BlockSpec((tile, size), lambda i: (i, 0)) for size in RETURNED],
            pl.BlockSpec((1, 1), lambda i: (0, 0)),
        ],
        out_shape=[
            *[jax.ShapeDtypeStruct((order, size), bf16) for size in RETURNED],
            jax.ShapeDtypeStruct((1, 1), f32),
        ],
        name="products",
    )(left, right, owned, *earlier)


def update(position, scale, returned, params, start, cols):
    blocks, rows, _ = params.shape
    slots = returned.shape[0]
    first = start // LANES

    def body(position_ref, scale_ref, returned_ref, params_ref, out):
        for block in range(blocks):
            change = scale_ref[block] * returned_ref[position_ref[block]].astype(f32)
            out[block] = (params_ref[block].astype(f32) - change).astype(bf16)

    return pl.pallas_call(
        body,
        grid_spec=pltpu.PrefetchScalarGridSpec(
            num_scalar_prefetch=2,
            grid=(cols // LANES,),
            in_specs=[
                pl.BlockSpec((slots, rows, LANES), lambda i, p, s: (0, 0, i)),
                pl.BlockSpec((blocks, rows, LANES), lambda i, p, s: (0, 0, first + i)),
            ],
            out_specs=pl.BlockSpec((blocks, rows, LANES), lambda i, p, s: (0, 0, i)),
        ),
        out_shape=jax.ShapeDtypeStruct((blocks, rows, cols), bf16),
        name="update",
    )(position, scale, returned, params)


def everywhere(value):
    value = value + lax.ppermute(value, "group_2", [(0, 1), (1, 0)])
    for axis in ("rep", "group_0", "group_1"):
        for pairs in ([(0, 1), (1, 0), (2, 3), (3, 2)], [(0, 3), (3, 0), (1, 2), (2, 1)]):
            value = value + lax.ppermute(value, axis, pairs)
    return value


def local(grad_parts, params, accum, left_pre, right_pre, slot_block, layer_of):
    group_size = lax.axis_size(GROUP)
    reps = lax.axis_size("rep")
    me = lax.axis_index("rep")
    group_index = lax.axis_index(GROUP)
    blocks, rows, width = params.shape
    half = blocks // 2
    up, down = ring(reps, 1), ring(reps, -1)
    parts = grad_parts[0].reshape(reps, blocks, rows, width)
    who = lax.rem(me + jnp.arange(reps, dtype=jnp.int32), reps)
    table = lax.dynamic_index_in_dim(slot_block, me, 0, keepdims=False).reshape(-1)
    wanted = jnp.maximum(table, 0)
    left, right = left_pre[0, 0, 0], right_pre[0, 0, 0]

    far = lax.rem(me + 2, reps)
    gradients, earlier, owned = [], [], None
    for start, cols in zip(starts(SENT), SENT):
        low = lax.dynamic_slice(parts, (far, 0, 0, start), (1, half, rows, cols))[0]
        high = lax.dynamic_slice(parts, (far, half, 0, start), (1, half, rows, cols))[0]
        far_up = lax.ppermute(low, "rep", up)
        far_down = lax.ppermute(high, "rep", down)
        to_up, to_down = merge(who, parts, far_up, far_down, start, cols)
        near_up = lax.ppermute(to_up, "rep", up)
        near_down = lax.ppermute(to_down, "rep", down)
        gradient, outgoing = finish(who, wanted, parts, near_up, near_down, start, cols)
        gradients.append(gradient)
        arrived = lax.all_to_all(outgoing, GROUP, split_axis=0, concat_axis=0, tiled=True)
        if owned is not None:
            earlier.append(left_times(left, owned))
        owned = arrived.reshape(group_size * rows, cols)

    my_layers = lax.dynamic_slice_in_dim(layer_of, me * blocks, blocks)
    onehot = (my_layers[:, None] == jnp.arange(LAYERS, dtype=jnp.int32)[None, :]).astype(f32)
    wide = jnp.concatenate(gradients, axis=2).astype(f32)
    new_accum = accum + wide * wide
    graft = wide * lax.rsqrt(new_accum)
    graft_blocks = jnp.sum(graft * graft, axis=(1, 2))
    graft_layer = jnp.sum(onehot * graft_blocks[:, None], axis=0)
    mine = lax.dynamic_index_in_dim(table, group_index, 0, keepdims=False)
    chosen = (jnp.arange(blocks, dtype=jnp.int32) == mine).astype(f32)
    my_layer = jnp.sum(chosen[:, None] * onehot, axis=0)
    position = jnp.sum(
        jnp.where(
            table[None, :] == jnp.arange(blocks, dtype=jnp.int32)[:, None],
            jnp.arange(group_size, dtype=jnp.int32)[None, :],
            0,
        ),
        axis=1,
    )
    owned, earlier, graft_layer, my_layer, position, onehot, new_accum = lax.optimization_barrier(
        (owned, earlier, graft_layer, my_layer, position, onehot, new_accum)
    )

    *preconds, squares = products(left, right, owned, earlier)
    sums = everywhere(jnp.stack([graft_layer, my_layer * squares[0, 0]]))
    layer_scale = jnp.sqrt(sums[0]) * lax.rsqrt(sums[1] + 1e-06)
    block_scale = step_rate * jnp.sum(onehot * layer_scale[None, :], axis=1)

    new_params = jnp.zeros((reps, blocks, rows, width), bf16)
    for start, cols, precond in zip(starts(RETURNED), RETURNED, preconds):
        outgoing = precond.reshape(group_size, rows, cols)
        returned = lax.all_to_all(outgoing, GROUP, split_axis=0, concat_axis=0, tiled=True)
        updated = update(position, block_scale, returned, params, start, cols)
        from_down = lax.ppermute(updated, "rep", up)
        from_up = lax.ppermute(updated, "rep", down)
        far_low = lax.ppermute(from_down[:half], "rep", up)
        far_high = lax.ppermute(from_up[half:], "rep", down)
        for at, first, piece in (
            (0, 0, updated),
            (3, 0, from_down),
            (1, 0, from_up),
            (2, 0, far_low),
            (2, half, far_high),
        ):
            new_params = lax.dynamic_update_slice(new_params, piece[None], (who[at], first, 0, start))
    return (new_params.reshape(reps * blocks, rows, width), new_accum)


def solution(mesh):
    split = Mesh(mesh.devices.reshape(4, 4, 2, mesh.shape["rep"]), EVERY)
    placed = (
        P("rep", None, GROUP, None),
        P("rep", GROUP, None),
        P("rep", GROUP, None),
        P("rep", GROUP, None, None, None),
        P("rep", GROUP, None, None, None),
        P(),
        P(),
    )
    return jax.shard_map(
        local,
        mesh=split,
        in_specs=placed,
        out_specs=(P(None, GROUP, None), P("rep", GROUP, None)),
        check_vma=False,
    )
```

```python
import jax
import jax.numpy as jnp
from jax import lax
from jax.experimental import pallas as pl
from jax.experimental.pallas import tpu as pltpu
from jax.sharding import Mesh
from jax.sharding import PartitionSpec as P


LAYERS = 8
GROUP = ("group_0", "group_1", "group_2")
EVERY = ("group_0", "group_1", "group_2", "rep")
SENT = ((0, 512), (512, 512))
RETURNED = ((0, 256), (256, 256), (512, 512))


step_rate = 0.5
f32 = jnp.float32
bf16 = jnp.bfloat16


def ring(count, step):
    return [(i, (i + step) % count) for i in range(count)]


def merge(who, parts, far_up, far_down, start, cols):
    _, blocks, rows, _ = parts.shape
    half = blocks // 2
    at = start // cols

    def body(who_ref, above, below, from_down, from_up, out_up, out_down):
        first = pl.program_id(0) == 0

        @pl.when(first)
        def _():
            out_up[...] = (above[0].astype(f32) + from_down[...].astype(f32)).astype(bf16)
            out_down[...] = below[0]

        @pl.when(jnp.logical_not(first))
        def _():
            out_up[...] = above[0]
            out_down[...] = (below[0].astype(f32) + from_up[...].astype(f32)).astype(bf16)

    piece = pl.BlockSpec((half, rows, cols), lambda i, w: (0, 0, 0))
    out = pl.BlockSpec((half, rows, cols), lambda i, w: (i, 0, 0))
    shape = jax.ShapeDtypeStruct((blocks, rows, cols), bf16)
    return pl.pallas_call(
        body,
        grid_spec=pltpu.PrefetchScalarGridSpec(
            num_scalar_prefetch=1,
            grid=(2,),
            in_specs=[
                pl.BlockSpec((1, half, rows, cols), lambda i, w: (w[1], i, 0, at)),
                pl.BlockSpec((1, half, rows, cols), lambda i, w: (w[3], i, 0, at)),
                piece,
                piece,
            ],
            out_specs=[out, out],
        ),
        out_shape=[shape, shape],
        name="merge",
    )(who, parts, parts, far_up, far_down)


def finish(who, table, parts, up, down, start, cols):
    _, blocks, rows, _ = parts.shape
    slots = table.shape[0]
    at = start // cols

    def body(who_ref, table_ref, own, one, two, gradient, slotted):
        total = own[0].astype(f32) + one[...].astype(f32) + two[...].astype(f32)
        gradient[...] = total.astype(bf16)
        for slot in range(slots):
            slotted[slot] = gradient[table_ref[slot]]

    block = pl.BlockSpec((blocks, rows, cols), lambda i, w, t: (0, 0, 0))
    return pl.pallas_call(
        body,
        grid_spec=pltpu.PrefetchScalarGridSpec(
            num_scalar_prefetch=2,
            grid=(1,),
            in_specs=[
                pl.BlockSpec((1, blocks, rows, cols), lambda i, w, t: (w[0], 0, 0, at)),
                block,
                block,
            ],
            out_specs=[block, pl.BlockSpec((slots, rows, cols), lambda i, w, t: (0, 0, 0))],
        ),
        out_shape=[
            jax.ShapeDtypeStruct((blocks, rows, cols), bf16),
            jax.ShapeDtypeStruct((slots, rows, cols), bf16),
        ],
        name="finish",
    )(who, table, parts, up, down)


def early(left, right, owned, start, so_far, split):
    order, cols = owned.shape
    tile = order // 2
    at = start // cols

    def body(left_ref, right_ref, owned_ref, *rest):
        before, outs = rest[: len(so_far)], rest[len(so_far) :]
        mid = jnp.dot(left_ref[...], owned_ref[...], preferred_element_type=f32).astype(bf16)
        term = jnp.dot(mid, right_ref[...], preferred_element_type=f32)
        pieces = (term[:, :split], term[:, split:])
        for i, (out, piece) in enumerate(zip(outs, pieces)):
            out[...] = piece + before[i][...] if before else piece

    sums = [pl.BlockSpec((tile, split), lambda i: (i, 0)), pl.BlockSpec((tile, order - split), lambda i: (i, 0))]
    return pl.pallas_call(
        body,
        grid=(2,),
        in_specs=[
            pl.BlockSpec((tile, order), lambda i: (i, 0)),
            pl.BlockSpec((cols, order), lambda i: (at, 0)),
            pl.BlockSpec((order, cols), lambda i: (0, 0)),
            *sums[: len(so_far)],
        ],
        out_specs=sums,
        out_shape=[
            jax.ShapeDtypeStruct((order, split), f32),
            jax.ShapeDtypeStruct((order, order - split), f32),
        ],
        name="early",
    )(left, right, owned, *so_far)


def squared(value):
    wide = value.astype(f32)
    return jnp.sum((wide * wide).reshape(-1, 8, value.shape[1]), axis=0)


def accumulate(ref, value):
    @pl.when(pl.program_id(0) == 0)
    def _():
        ref[...] = value

    @pl.when(pl.program_id(0) > 0)
    def _():
        ref[...] += value


def first_product(left, right, owned, so_far, start):
    order, cols = owned.shape
    split = so_far.shape[1]
    tile = order // 2
    at = start // cols

    def body(left_ref, right_ref, owned_ref, before, mid, out, squares):
        mid[...] = jnp.dot(left_ref[...], owned_ref[...], preferred_element_type=f32).astype(bf16)
        total = before[...] + jnp.dot(mid[...], right_ref[...], preferred_element_type=f32)
        out[...] = total.astype(bf16)
        accumulate(squares, squared(out[...]))

    return pl.pallas_call(
        body,
        grid=(2,),
        in_specs=[
            pl.BlockSpec((tile, order), lambda i: (i, 0)),
            pl.BlockSpec((cols, split), lambda i: (at, 0)),
            pl.BlockSpec((order, cols), lambda i: (0, 0)),
            pl.BlockSpec((tile, split), lambda i: (i, 0)),
        ],
        out_specs=[
            pl.BlockSpec((tile, cols), lambda i: (i, 0)),
            pl.BlockSpec((tile, split), lambda i: (i, 0)),
            pl.BlockSpec((8, split), lambda i: (0, 0)),
        ],
        out_shape=[
            jax.ShapeDtypeStruct((order, cols), bf16),
            jax.ShapeDtypeStruct((order, split), bf16),
            jax.ShapeDtypeStruct((8, split), f32),
        ],
        name="first_product",
    )(left, right, owned, so_far)


def other_products(mid, right, so_far, start):
    order, cols = mid.shape
    rest = so_far.shape[1]
    split = order - rest
    tile = order // 2
    at = start // cols
    wanted = RETURNED[1:]

    def body(mid_ref, right_ref, before, *outs):
        squares = outs[-1]
        total = before[...] + jnp.dot(mid_ref[...], right_ref[:, split:], preferred_element_type=f32)
        rounded = total.astype(bf16)
        for out, (first, size) in zip(outs, wanted):
            out[...] = rounded[:, first - split : first - split + size]
        accumulate(squares, squared(rounded))

    return pl.pallas_call(
        body,
        grid=(2,),
        in_specs=[
            pl.BlockSpec((tile, cols), lambda i: (i, 0)),
            pl.BlockSpec((cols, order), lambda i: (at, 0)),
            pl.BlockSpec((tile, rest), lambda i: (i, 0)),
        ],
        out_specs=[
            *[pl.BlockSpec((tile, size), lambda i: (i, 0)) for _, size in wanted],
            pl.BlockSpec((8, rest), lambda i: (0, 0)),
        ],
        out_shape=[
            *[jax.ShapeDtypeStruct((order, size), bf16) for _, size in wanted],
            jax.ShapeDtypeStruct((8, rest), f32),
        ],
        name="other_products",
    )(mid, right, so_far)


def pick(position, returned):
    blocks = position.shape[0]
    slots, rows, cols = returned.shape

    def body(position_ref, returned_ref, out):
        for block in range(blocks):
            out[block] = returned_ref[position_ref[block]]

    return pl.pallas_call(
        body,
        grid_spec=pltpu.PrefetchScalarGridSpec(
            num_scalar_prefetch=1,
            grid=(1,),
            in_specs=[pl.BlockSpec((slots, rows, cols), lambda i, p: (0, 0, 0))],
            out_specs=pl.BlockSpec((blocks, rows, cols), lambda i, p: (0, 0, 0)),
        ),
        out_shape=jax.ShapeDtypeStruct((blocks, rows, cols), bf16),
        name="pick",
    )(position, returned)


def update(position, scale, returned, params, start, cols):
    blocks, rows, _ = params.shape
    slots = returned.shape[0]
    at = start // cols

    def body(position_ref, scale_ref, returned_ref, params_ref, out):
        for block in range(blocks):
            change = scale_ref[block] * returned_ref[position_ref[block]].astype(f32)
            out[block] = (params_ref[block].astype(f32) - change).astype(bf16)

    return pl.pallas_call(
        body,
        grid_spec=pltpu.PrefetchScalarGridSpec(
            num_scalar_prefetch=2,
            grid=(1,),
            in_specs=[
                pl.BlockSpec((slots, rows, cols), lambda i, p, s: (0, 0, 0)),
                pl.BlockSpec((blocks, rows, cols), lambda i, p, s: (0, 0, at)),
            ],
            out_specs=pl.BlockSpec((blocks, rows, cols), lambda i, p, s: (0, 0, 0)),
        ),
        out_shape=jax.ShapeDtypeStruct((blocks, rows, cols), bf16),
        name="update",
    )(position, scale, returned, params)


def everywhere(value):
    swap, near, wrap = [(0, 1), (1, 0)], [(0, 1), (1, 0), (2, 3), (3, 2)], [(0, 3), (3, 0), (1, 2), (2, 1)]
    steps = [("group_2", swap)]
    for axis in ("rep", "group_0", "group_1"):
        steps += [(axis, near), (axis, wrap)]
    for axis, pairs in steps:
        value = value + lax.ppermute(value, axis, pairs)
    return value


def spread(value, reps):
    half = value.shape[0] // 2
    up, down = ring(reps, 1), ring(reps, -1)
    from_down = lax.ppermute(value, "rep", up)
    from_up = lax.ppermute(value, "rep", down)
    far_low = lax.ppermute(from_down[:half], "rep", up)
    far_high = lax.ppermute(from_up[half:], "rep", down)
    return (
        (0, slice(None), value),
        (3, slice(None), from_down),
        (1, slice(None), from_up),
        (2, slice(0, half), far_low),
        (2, slice(half, 2 * half), far_high),
    )


def local(grad_parts, params, accum, left_pre, right_pre, slot_block, layer_of):
    group_size = lax.axis_size(GROUP)
    reps = lax.axis_size("rep")
    me = lax.axis_index("rep")
    group_index = lax.axis_index(GROUP)
    blocks, rows, width = params.shape
    half = blocks // 2
    up, down = ring(reps, 1), ring(reps, -1)
    parts = grad_parts[0].reshape(reps, blocks, rows, width)
    who = lax.rem(me + jnp.arange(reps, dtype=jnp.int32), reps)
    table = lax.dynamic_index_in_dim(slot_block, me, 0, keepdims=False).reshape(-1)
    wanted = jnp.maximum(table, 0)
    left, right = left_pre[0, 0, 0], right_pre[0, 0, 0]
    split = RETURNED[0][1]

    far = lax.rem(me + 2, reps)
    gradients, so_far, owned = [None] * len(SENT), [], None
    for chunk, (start, cols) in enumerate(SENT):
        low = lax.dynamic_slice(parts, (far, 0, 0, start), (1, half, rows, cols))[0]
        high = lax.dynamic_slice(parts, (far, half, 0, start), (1, half, rows, cols))[0]
        far_up = lax.ppermute(low, "rep", up)
        far_down = lax.ppermute(high, "rep", down)
        to_up, to_down = merge(who, parts, far_up, far_down, start, cols)
        near_up = lax.ppermute(to_up, "rep", up)
        near_down = lax.ppermute(to_down, "rep", down)
        gradient, outgoing = finish(who, wanted, parts, near_up, near_down, start, cols)
        gradients[chunk] = gradient
        arrived = lax.all_to_all(outgoing, GROUP, split_axis=0, concat_axis=0, tiled=True)
        if chunk > 0:
            so_far = early(left, right, owned, SENT[chunk - 1][0], so_far, split)
        owned = arrived.reshape(group_size * rows, cols)

    first, size = RETURNED[0]
    ahead = spread(params[:, :, first : first + size], reps)

    onehots = (layer_of[:, None] == jnp.arange(LAYERS, dtype=jnp.int32)[None, :]).astype(f32)
    onehot = lax.dynamic_slice_in_dim(onehots, me * blocks, blocks)
    in_order = sorted(range(len(SENT)), key=lambda c: SENT[c][0])
    wide = jnp.concatenate([gradients[c] for c in in_order], axis=2).astype(f32)
    new_accum = accum + wide * wide
    graft = wide * lax.rsqrt(new_accum)
    graft_blocks = jnp.sum(graft * graft, axis=(1, 2))
    graft_layer = jnp.sum(onehot * graft_blocks[:, None], axis=0)
    mine = lax.dynamic_index_in_dim(table, group_index, 0, keepdims=False)
    chosen = (jnp.arange(blocks, dtype=jnp.int32) == mine).astype(f32)
    my_layer = jnp.sum(chosen[:, None] * onehot, axis=0)
    position = jnp.sum(
        jnp.where(
            table[None, :] == jnp.arange(blocks, dtype=jnp.int32)[:, None],
            jnp.arange(group_size, dtype=jnp.int32)[None, :],
            0,
        ),
        axis=1,
    )
    owned, so_far, graft_layer, my_layer, position, onehots, new_accum = lax.optimization_barrier(
        (owned, so_far, graft_layer, my_layer, position, onehots, new_accum)
    )

    last = SENT[-1][0]
    mid, precond, some = first_product(left, right, owned, so_far[0], last)
    *preconds, others = other_products(mid, right, so_far[1], last)
    preconds = [precond, *preconds]
    squares = jnp.sum(some) + jnp.sum(others)
    sums = everywhere(jnp.stack([graft_layer, my_layer * squares]))
    layer_scale = jnp.sqrt(sums[0]) * lax.rsqrt(sums[1] + 1e-06)
    scales = (step_rate * jnp.sum(onehots * layer_scale[None, :], axis=1)).reshape(reps, blocks)

    new_params = jnp.zeros((reps, blocks, rows, width), bf16)
    for chunk, ((start, cols), precond) in enumerate(zip(RETURNED, preconds)):
        outgoing = precond.reshape(group_size, rows, cols)
        returned = lax.all_to_all(outgoing, GROUP, split_axis=0, concat_axis=0, tiled=True)
        if chunk == 0:
            changes = spread(pick(position, returned), reps)
            pieces = []
            for (offset, part, old), (_, _, change) in zip(ahead, changes):
                scale = scales[who[offset]][part, None, None]
                new = (old.astype(f32) - scale * change.astype(f32)).astype(bf16)
                pieces.append((offset, part, new))
        else:
            pieces = spread(update(position, scales[me], returned, params, start, cols), reps)
        for offset, part, piece in pieces:
            where = (who[offset], part.start or 0, 0, start)
            new_params = lax.dynamic_update_slice(new_params, piece[None], where)
    return (new_params.reshape(reps * blocks, rows, width), new_accum)


def solution(mesh):
    split = Mesh(mesh.devices.reshape(4, 4, 2, mesh.shape["rep"]), EVERY)
    placed = (
        P("rep", None, GROUP, None),
        P("rep", GROUP, None),
        P("rep", GROUP, None),
        P("rep", GROUP, None, None, None),
        P("rep", GROUP, None, None, None),
        P(),
        P(),
    )
    return jax.shard_map(
        local,
        mesh=split,
        in_specs=placed,
        out_specs=(P(None, GROUP, None), P("rep", GROUP, None)),
        check_vma=False,
    )
```

```python
import jax
import jax.numpy as jnp
from jax import lax
from jax.experimental import pallas as pl
from jax.experimental.pallas import tpu as pltpu
from jax.sharding import Mesh
from jax.sharding import PartitionSpec as P


LAYERS = 8
GROUP = ("group_0", "group_1", "group_2")
EVERY = ("group_0", "group_1", "group_2", "rep")
SENT = ((768, 256), (0, 768))
RETURNED = ((0, 512), (512, 512))


step_rate = 0.5
f32 = jnp.float32
bf16 = jnp.bfloat16


def ring(count, step):
    return [(i, (i + step) % count) for i in range(count)]


def merge(who, parts, far_up, far_down, start, cols):
    _, blocks, rows, _ = parts.shape
    half = blocks // 2
    at = start // cols

    def body(who_ref, above, below, from_down, from_up, out_up, out_down):
        first = pl.program_id(0) == 0

        @pl.when(first)
        def _():
            out_up[...] = (above[0].astype(f32) + from_down[...].astype(f32)).astype(bf16)
            out_down[...] = below[0]

        @pl.when(jnp.logical_not(first))
        def _():
            out_up[...] = above[0]
            out_down[...] = (below[0].astype(f32) + from_up[...].astype(f32)).astype(bf16)

    piece = pl.BlockSpec((half, rows, cols), lambda i, w: (0, 0, 0))
    out = pl.BlockSpec((half, rows, cols), lambda i, w: (i, 0, 0))
    shape = jax.ShapeDtypeStruct((blocks, rows, cols), bf16)
    return pl.pallas_call(
        body,
        grid_spec=pltpu.PrefetchScalarGridSpec(
            num_scalar_prefetch=1,
            grid=(2,),
            in_specs=[
                pl.BlockSpec((1, half, rows, cols), lambda i, w: (w[1], i, 0, at)),
                pl.BlockSpec((1, half, rows, cols), lambda i, w: (w[3], i, 0, at)),
                piece,
                piece,
            ],
            out_specs=[out, out],
        ),
        out_shape=[shape, shape],
        name="merge",
    )(who, parts, parts, far_up, far_down)


def finish(who, table, parts, up, down, start, cols):
    _, blocks, rows, _ = parts.shape
    slots = table.shape[0]
    at = start // cols

    def body(who_ref, table_ref, own, one, two, gradient, slotted):
        total = own[0].astype(f32) + one[...].astype(f32) + two[...].astype(f32)
        gradient[...] = total.astype(bf16)
        for slot in range(slots):
            slotted[slot] = gradient[table_ref[slot]]

    block = pl.BlockSpec((blocks, rows, cols), lambda i, w, t: (0, 0, 0))
    return pl.pallas_call(
        body,
        grid_spec=pltpu.PrefetchScalarGridSpec(
            num_scalar_prefetch=2,
            grid=(1,),
            in_specs=[
                pl.BlockSpec((1, blocks, rows, cols), lambda i, w, t: (w[0], 0, 0, at)),
                block,
                block,
            ],
            out_specs=[block, pl.BlockSpec((slots, rows, cols), lambda i, w, t: (0, 0, 0))],
        ),
        out_shape=[
            jax.ShapeDtypeStruct((blocks, rows, cols), bf16),
            jax.ShapeDtypeStruct((slots, rows, cols), bf16),
        ],
        name="finish",
    )(who, table, parts, up, down)


def early(left, right, owned, start, so_far, split):
    order, cols = owned.shape
    tile = order // 2
    at = start // cols

    def body(left_ref, right_ref, owned_ref, *rest):
        before, outs = rest[: len(so_far)], rest[len(so_far) :]
        mid = jnp.dot(left_ref[...], owned_ref[...], preferred_element_type=f32).astype(bf16)
        term = jnp.dot(mid, right_ref[...], preferred_element_type=f32)
        pieces = (term[:, :split], term[:, split:])
        for i, (out, piece) in enumerate(zip(outs, pieces)):
            out[...] = piece + before[i][...] if before else piece

    sums = [pl.BlockSpec((tile, split), lambda i: (i, 0)), pl.BlockSpec((tile, order - split), lambda i: (i, 0))]
    return pl.pallas_call(
        body,
        grid=(2,),
        in_specs=[
            pl.BlockSpec((tile, order), lambda i: (i, 0)),
            pl.BlockSpec((cols, order), lambda i: (at, 0)),
            pl.BlockSpec((order, cols), lambda i: (0, 0)),
            *sums[: len(so_far)],
        ],
        out_specs=sums,
        out_shape=[
            jax.ShapeDtypeStruct((order, split), f32),
            jax.ShapeDtypeStruct((order, order - split), f32),
        ],
        name="early",
    )(left, right, owned, *so_far)


def squared(value):
    wide = value.astype(f32)
    return jnp.sum((wide * wide).reshape(-1, 8, value.shape[1]), axis=0)


def accumulate(ref, value):
    @pl.when(pl.program_id(0) == 0)
    def _():
        ref[...] = value

    @pl.when(pl.program_id(0) > 0)
    def _():
        ref[...] += value


def first_product(left, right, owned, so_far, start):
    order, cols = owned.shape
    split = so_far.shape[1]
    tile = order // 2
    at = start // cols

    def body(left_ref, right_ref, owned_ref, before, mid, out, squares):
        mid[...] = jnp.dot(left_ref[...], owned_ref[...], preferred_element_type=f32).astype(bf16)
        total = before[...] + jnp.dot(mid[...], right_ref[...], preferred_element_type=f32)
        out[...] = total.astype(bf16)
        accumulate(squares, squared(out[...]))

    return pl.pallas_call(
        body,
        grid=(2,),
        in_specs=[
            pl.BlockSpec((tile, order), lambda i: (i, 0)),
            pl.BlockSpec((cols, split), lambda i: (at, 0)),
            pl.BlockSpec((order, cols), lambda i: (0, 0)),
            pl.BlockSpec((tile, split), lambda i: (i, 0)),
        ],
        out_specs=[
            pl.BlockSpec((tile, cols), lambda i: (i, 0)),
            pl.BlockSpec((tile, split), lambda i: (i, 0)),
            pl.BlockSpec((8, split), lambda i: (0, 0)),
        ],
        out_shape=[
            jax.ShapeDtypeStruct((order, cols), bf16),
            jax.ShapeDtypeStruct((order, split), bf16),
            jax.ShapeDtypeStruct((8, split), f32),
        ],
        name="first_product",
    )(left, right, owned, so_far)


def other_products(mid, right, so_far, start):
    order, cols = mid.shape
    rest = so_far.shape[1]
    split = order - rest
    tile = order // 2
    at = start // cols
    wanted = RETURNED[1:]

    def body(mid_ref, right_ref, before, *outs):
        squares = outs[-1]
        total = before[...] + jnp.dot(mid_ref[...], right_ref[:, split:], preferred_element_type=f32)
        rounded = total.astype(bf16)
        for out, (first, size) in zip(outs, wanted):
            out[...] = rounded[:, first - split : first - split + size]
        accumulate(squares, squared(rounded))

    return pl.pallas_call(
        body,
        grid=(2,),
        in_specs=[
            pl.BlockSpec((tile, cols), lambda i: (i, 0)),
            pl.BlockSpec((cols, order), lambda i: (at, 0)),
            pl.BlockSpec((tile, rest), lambda i: (i, 0)),
        ],
        out_specs=[
            *[pl.BlockSpec((tile, size), lambda i: (i, 0)) for _, size in wanted],
            pl.BlockSpec((8, rest), lambda i: (0, 0)),
        ],
        out_shape=[
            *[jax.ShapeDtypeStruct((order, size), bf16) for _, size in wanted],
            jax.ShapeDtypeStruct((8, rest), f32),
        ],
        name="other_products",
    )(mid, right, so_far)


def pick(position, returned, whole):
    blocks = position.shape[0]
    half = blocks // 2
    slots, rows, cols = returned.shape

    def body(position_ref, returned_ref, low, high, blank):
        for block in range(half):
            low[block] = returned_ref[position_ref[block]]
            high[block] = returned_ref[position_ref[half + block]]

    out = pl.BlockSpec((half, rows, cols), lambda i, p: (0, 0, 0))
    shape = jax.ShapeDtypeStruct((half, rows, cols), bf16)
    return pl.pallas_call(
        body,
        grid_spec=pltpu.PrefetchScalarGridSpec(
            num_scalar_prefetch=1,
            grid=(1,),
            in_specs=[pl.BlockSpec((slots, rows, cols), lambda i, p: (0, 0, 0))],
            out_specs=[out, out, pl.BlockSpec(memory_space=pl.ANY)],
        ),
        out_shape=[shape, shape, jax.ShapeDtypeStruct(whole, bf16)],
        name="pick",
    )(position, returned)


def update(position, scale, returned, params, start, cols):
    blocks, rows, _ = params.shape
    half = blocks // 2
    slots = returned.shape[0]
    at = start // cols

    def body(position_ref, scale_ref, returned_ref, params_ref, low, high):
        for block in range(blocks):
            change = scale_ref[block] * returned_ref[position_ref[block]].astype(f32)
            new = (params_ref[block].astype(f32) - change).astype(bf16)
            if block < half:
                low[block] = new
            else:
                high[block - half] = new

    out = pl.BlockSpec((half, rows, cols), lambda i, p, s: (0, 0, 0))
    shape = jax.ShapeDtypeStruct((half, rows, cols), bf16)
    return pl.pallas_call(
        body,
        grid_spec=pltpu.PrefetchScalarGridSpec(
            num_scalar_prefetch=2,
            grid=(1,),
            in_specs=[
                pl.BlockSpec((slots, rows, cols), lambda i, p, s: (0, 0, 0)),
                pl.BlockSpec((blocks, rows, cols), lambda i, p, s: (0, 0, at)),
            ],
            out_specs=[out, out],
        ),
        out_shape=[shape, shape],
        name="update",
    )(position, scale, returned, params)


def everywhere(value):
    swap, near, wrap = [(0, 1), (1, 0)], [(0, 1), (1, 0), (2, 3), (3, 2)], [(0, 3), (3, 0), (1, 2), (2, 1)]
    steps = [("group_2", swap)]
    for axis in ("rep", "group_0", "group_1"):
        steps += [(axis, near), (axis, wrap)]
    for axis, pairs in steps:
        value = value + lax.ppermute(value, axis, pairs)
    return value


def spread(low, high, reps):
    up, down = ring(reps, 1), ring(reps, -1)
    low_up = lax.ppermute(low, "rep", up)
    high_down = lax.ppermute(high, "rep", down)
    high_up = lax.ppermute(high, "rep", up)
    low_down = lax.ppermute(low, "rep", down)
    far_low = lax.ppermute(low_up, "rep", up)
    far_high = lax.ppermute(high_down, "rep", down)
    return (
        (0, 0, low),
        (0, 1, high),
        (3, 0, low_up),
        (1, 1, high_down),
        (3, 1, high_up),
        (1, 0, low_down),
        (2, 0, far_low),
        (2, 1, far_high),
    )


def local(grad_parts, params, accum, left_pre, right_pre, slot_block, layer_of):
    group_size = lax.axis_size(GROUP)
    reps = lax.axis_size("rep")
    me = lax.axis_index("rep")
    group_index = lax.axis_index(GROUP)
    blocks, rows, width = params.shape
    half = blocks // 2
    up, down = ring(reps, 1), ring(reps, -1)
    parts = grad_parts[0].reshape(reps, blocks, rows, width)
    who = lax.rem(me + jnp.arange(reps, dtype=jnp.int32), reps)
    table = lax.dynamic_index_in_dim(slot_block, me, 0, keepdims=False).reshape(-1)
    wanted = jnp.maximum(table, 0)
    left, right = left_pre[0, 0, 0], right_pre[0, 0, 0]
    split = RETURNED[0][1]

    far = lax.rem(me + 2, reps)
    gradients, so_far, owned = [None] * len(SENT), [], None
    for chunk, (start, cols) in enumerate(SENT):
        low = lax.dynamic_slice(parts, (far, 0, 0, start), (1, half, rows, cols))[0]
        high = lax.dynamic_slice(parts, (far, half, 0, start), (1, half, rows, cols))[0]
        far_up = lax.ppermute(low, "rep", up)
        far_down = lax.ppermute(high, "rep", down)
        to_up, to_down = merge(who, parts, far_up, far_down, start, cols)
        near_up = lax.ppermute(to_up, "rep", up)
        near_down = lax.ppermute(to_down, "rep", down)
        gradient, outgoing = finish(who, wanted, parts, near_up, near_down, start, cols)
        gradients[chunk] = gradient
        arrived = lax.all_to_all(outgoing, GROUP, split_axis=0, concat_axis=0, tiled=True)
        if chunk > 0:
            so_far = early(left, right, owned, SENT[chunk - 1][0], so_far, split)
        owned = arrived.reshape(group_size * rows, cols)

    first, size = RETURNED[0]
    columns = params[:, :, first : first + size]
    ahead = spread(columns[:half], columns[half:], reps)

    onehots = (layer_of[:, None] == jnp.arange(LAYERS, dtype=jnp.int32)[None, :]).astype(f32)
    onehot = lax.dynamic_slice_in_dim(onehots, me * blocks, blocks)
    in_order = sorted(range(len(SENT)), key=lambda c: SENT[c][0])
    wide = jnp.concatenate([gradients[c] for c in in_order], axis=2).astype(f32)
    new_accum = accum + wide * wide
    graft = wide * lax.rsqrt(new_accum)
    graft_blocks = jnp.sum(graft * graft, axis=(1, 2))
    graft_layer = jnp.sum(onehot * graft_blocks[:, None], axis=0)
    mine = lax.dynamic_index_in_dim(table, group_index, 0, keepdims=False)
    chosen = (jnp.arange(blocks, dtype=jnp.int32) == mine).astype(f32)
    my_layer = jnp.sum(chosen[:, None] * onehot, axis=0)
    position = jnp.sum(
        jnp.where(
            table[None, :] == jnp.arange(blocks, dtype=jnp.int32)[:, None],
            jnp.arange(group_size, dtype=jnp.int32)[None, :],
            0,
        ),
        axis=1,
    )
    owned, so_far, graft_layer, my_layer, position, onehots, new_accum = lax.optimization_barrier(
        (owned, so_far, graft_layer, my_layer, position, onehots, new_accum)
    )

    last = SENT[-1][0]
    mid, precond, some = first_product(left, right, owned, so_far[0], last)
    *preconds, others = other_products(mid, right, so_far[1], last)
    preconds = [precond, *preconds]
    squares = jnp.sum(some) + jnp.sum(others)
    sums = everywhere(jnp.stack([graft_layer, my_layer * squares]))
    layer_scale = jnp.sqrt(sums[0]) * lax.rsqrt(sums[1] + 1e-06)
    scales = (step_rate * jnp.sum(onehots * layer_scale[None, :], axis=1)).reshape(reps, blocks)

    for chunk, ((start, cols), precond) in enumerate(zip(RETURNED, preconds)):
        outgoing = precond.reshape(group_size, rows, cols)
        returned = lax.all_to_all(outgoing, GROUP, split_axis=0, concat_axis=0, tiled=True)
        if chunk == 0:
            low, high, new_params = pick(position, returned, (reps, blocks, rows, width))
            pieces = []
            for (offset, part, old), (_, _, change) in zip(ahead, spread(low, high, reps)):
                scale = scales[who[offset]][part * half : (part + 1) * half, None, None]
                new = (old.astype(f32) - scale * change.astype(f32)).astype(bf16)
                pieces.append((offset, part, new))
        else:
            low, high = update(position, scales[me], returned, params, start, cols)
            pieces = spread(low, high, reps)
        for offset, part, piece in pieces:
            where = (who[offset], part * half, 0, start)
            new_params = lax.dynamic_update_slice(new_params, piece[None], where)
    return (new_params.reshape(reps * blocks, rows, width), new_accum)


def solution(mesh):
    split = Mesh(mesh.devices.reshape(4, 4, 2, mesh.shape["rep"]), EVERY)
    placed = (
        P("rep", None, GROUP, None),
        P("rep", GROUP, None),
        P("rep", GROUP, None),
        P("rep", GROUP, None, None, None),
        P("rep", GROUP, None, None, None),
        P(),
        P(),
    )
    return jax.shard_map(
        local,
        mesh=split,
        in_specs=placed,
        out_specs=(P(None, GROUP, None), P("rep", GROUP, None)),
        check_vma=False,
    )
```

```python
import jax
import jax.numpy as jnp
from jax import lax
from jax.experimental import pallas as pl
from jax.experimental.pallas import tpu as pltpu
from jax.sharding import Mesh
from jax.sharding import PartitionSpec as P


LAYERS = 8
LANES = 128
GROUP = ("group_0", "group_1", "group_2")
EVERY = ("group_0", "group_1", "group_2", "rep")
SENT = ((768, 256), (0, 768))


step_rate = 0.5
f32 = jnp.float32
bf16 = jnp.bfloat16


def ring(count, step):
    return [(i, (i + step) % count) for i in range(count)]


def merge(who, parts, far_up, far_down, start, cols):
    _, blocks, rows, _ = parts.shape
    half = blocks // 2
    at = start // cols

    def body(who_ref, above, below, from_down, from_up, out_up, out_down):
        first = pl.program_id(0) == 0

        @pl.when(first)
        def _():
            out_up[...] = (above[0].astype(f32) + from_down[...].astype(f32)).astype(bf16)
            out_down[...] = below[0]

        @pl.when(jnp.logical_not(first))
        def _():
            out_up[...] = above[0]
            out_down[...] = (below[0].astype(f32) + from_up[...].astype(f32)).astype(bf16)

    piece = pl.BlockSpec((half, rows, cols), lambda i, w: (0, 0, 0))
    out = pl.BlockSpec((half, rows, cols), lambda i, w: (i, 0, 0))
    shape = jax.ShapeDtypeStruct((blocks, rows, cols), bf16)
    return pl.pallas_call(
        body,
        grid_spec=pltpu.PrefetchScalarGridSpec(
            num_scalar_prefetch=1,
            grid=(2,),
            in_specs=[
                pl.BlockSpec((1, half, rows, cols), lambda i, w: (w[1], i, 0, at)),
                pl.BlockSpec((1, half, rows, cols), lambda i, w: (w[3], i, 0, at)),
                piece,
                piece,
            ],
            out_specs=[out, out],
        ),
        out_shape=[shape, shape],
        name="merge",
    )(who, parts, parts, far_up, far_down)


def finish(who, table, parts, up, down, start, cols):
    _, blocks, rows, _ = parts.shape
    slots = table.shape[0]
    at = start // cols

    def body(who_ref, table_ref, own, one, two, gradient, slotted):
        total = own[0].astype(f32) + one[...].astype(f32) + two[...].astype(f32)
        gradient[...] = total.astype(bf16)
        for slot in range(slots):
            slotted[slot] = gradient[table_ref[slot]]

    block = pl.BlockSpec((blocks, rows, cols), lambda i, w, t: (0, 0, 0))
    return pl.pallas_call(
        body,
        grid_spec=pltpu.PrefetchScalarGridSpec(
            num_scalar_prefetch=2,
            grid=(1,),
            in_specs=[
                pl.BlockSpec((1, blocks, rows, cols), lambda i, w, t: (w[0], 0, 0, at)),
                block,
                block,
            ],
            out_specs=[block, pl.BlockSpec((slots, rows, cols), lambda i, w, t: (0, 0, 0))],
        ),
        out_shape=[
            jax.ShapeDtypeStruct((blocks, rows, cols), bf16),
            jax.ShapeDtypeStruct((slots, rows, cols), bf16),
        ],
        name="finish",
    )(who, table, parts, up, down)


def left_times(left, owned):
    order, cols = owned.shape
    tile = order // 2

    def body(left_ref, owned_ref, out):
        out[...] = jnp.dot(left_ref[...], owned_ref[...], preferred_element_type=f32).astype(bf16)

    return pl.pallas_call(
        body,
        grid=(2,),
        in_specs=[
            pl.BlockSpec((tile, order), lambda i: (i, 0)),
            pl.BlockSpec((order, cols), lambda i: (0, 0)),
        ],
        out_specs=pl.BlockSpec((tile, cols), lambda i: (i, 0)),
        out_shape=jax.ShapeDtypeStruct((order, cols), bf16),
        name="left_times",
    )(left, owned)


def products(left, right, owned, earlier, graft_row, layer_row):
    order, cols = owned.shape
    steps = 2
    tile = order // steps
    last = SENT[-1][0]

    def body(left_ref, right_ref, owned_ref, graft_ref, layer_ref, *rest):
        before, (out, sums, mid) = rest[: len(earlier)], rest[len(earlier) :]
        mid[:, last : last + cols] = jnp.dot(
            left_ref[...], owned_ref[...], preferred_element_type=f32
        ).astype(bf16)
        for ref, (start, size) in zip(before, SENT):
            mid[:, start : start + size] = ref[...]
        out[...] = jnp.dot(mid[...], right_ref[...], preferred_element_type=f32).astype(bf16)
        wide = out[...].astype(f32)
        squares = jnp.sum(jnp.sum(wide * wide, axis=0, keepdims=True), axis=1, keepdims=True)

        @pl.when(pl.program_id(0) == 0)
        def _():
            sums[0:1] = graft_ref[...]
            sums[1:2] = layer_ref[...] * squares

        @pl.when(pl.program_id(0) > 0)
        def _():
            sums[1:2] += layer_ref[...] * squares

    row = pl.BlockSpec((1, LANES), lambda i: (0, 0))
    return pl.pallas_call(
        body,
        grid=(steps,),
        in_specs=[
            pl.BlockSpec((tile, order), lambda i: (i, 0)),
            pl.BlockSpec((order, order), lambda i: (0, 0)),
            pl.BlockSpec((order, cols), lambda i: (0, 0)),
            row,
            row,
            *[pl.BlockSpec((tile, e.shape[1]), lambda i: (i, 0)) for e in earlier],
        ],
        out_specs=[pl.BlockSpec((tile, order), lambda i: (i, 0)), pl.BlockSpec((2, LANES), lambda i: (0, 0))],
        out_shape=[jax.ShapeDtypeStruct((order, order), bf16), jax.ShapeDtypeStruct((2, LANES), f32)],
        scratch_shapes=[pltpu.VMEM((tile, order), bf16)],
        name="products",
    )(left, right, owned, graft_row, layer_row, *earlier)


def update(who, position, scale, returned, params, reps):
    blocks, rows, cols = params.shape
    half = blocks // 2
    slots = returned.shape[0]

    def body(who_ref, position_ref, scale_ref, returned_ref, params_ref, low, high, whole):
        for block in range(blocks):
            change = scale_ref[block] * returned_ref[position_ref[block]].astype(f32)
            new = (params_ref[block].astype(f32) - change).astype(bf16)
            whole[0, block] = new
            if block < half:
                low[block] = new
            else:
                high[block - half] = new

    out = pl.BlockSpec((half, rows, cols), lambda i, w, p, s: (0, 0, 0))
    shape = jax.ShapeDtypeStruct((half, rows, cols), bf16)
    return pl.pallas_call(
        body,
        grid_spec=pltpu.PrefetchScalarGridSpec(
            num_scalar_prefetch=3,
            grid=(1,),
            in_specs=[
                pl.BlockSpec((slots, rows, cols), lambda i, w, p, s: (0, 0, 0)),
                pl.BlockSpec((blocks, rows, cols), lambda i, w, p, s: (0, 0, 0)),
            ],
            out_specs=[out, out, pl.BlockSpec((1, blocks, rows, cols), lambda i, w, p, s: (w[0], 0, 0, 0))],
        ),
        out_shape=[shape, shape, jax.ShapeDtypeStruct((reps, blocks, rows, cols), bf16)],
        name="update",
    )(who, position, scale, returned, params)


def everywhere(value):
    swap, near, wrap = [(0, 1), (1, 0)], [(0, 1), (1, 0), (2, 3), (3, 2)], [(0, 3), (3, 0), (1, 2), (2, 1)]
    steps = [("group_2", swap)]
    for axis in ("rep", "group_0", "group_1"):
        steps += [(axis, near), (axis, wrap)]
    for axis, pairs in steps:
        value = value + lax.ppermute(value, axis, pairs)
    return value


def spread(low, high, reps):
    up, down = ring(reps, 1), ring(reps, -1)
    low_up = lax.ppermute(low, "rep", up)
    high_down = lax.ppermute(high, "rep", down)
    high_up = lax.ppermute(high, "rep", up)
    low_down = lax.ppermute(low, "rep", down)
    far_low = lax.ppermute(low_up, "rep", up)
    far_high = lax.ppermute(high_down, "rep", down)
    return (
        (3, 0, low_up),
        (1, 1, high_down),
        (3, 1, high_up),
        (1, 0, low_down),
        (2, 0, far_low),
        (2, 1, far_high),
    )


def local(grad_parts, params, accum, left_pre, right_pre, slot_block, layer_of):
    group_size = lax.axis_size(GROUP)
    reps = lax.axis_size("rep")
    me = lax.axis_index("rep")
    group_index = lax.axis_index(GROUP)
    blocks, rows, width = params.shape
    half = blocks // 2
    up, down = ring(reps, 1), ring(reps, -1)
    parts = grad_parts[0].reshape(reps, blocks, rows, width)
    who = lax.rem(me + jnp.arange(reps, dtype=jnp.int32), reps)
    table = lax.dynamic_index_in_dim(slot_block, me, 0, keepdims=False).reshape(-1)
    wanted = jnp.maximum(table, 0)
    left, right = left_pre[0, 0, 0], right_pre[0, 0, 0]

    far = lax.rem(me + 2, reps)
    gradients, earlier, owned = [None] * len(SENT), [], None
    for chunk, (start, cols) in enumerate(SENT):
        low = lax.dynamic_slice(parts, (far, 0, 0, start), (1, half, rows, cols))[0]
        high = lax.dynamic_slice(parts, (far, half, 0, start), (1, half, rows, cols))[0]
        far_up = lax.ppermute(low, "rep", up)
        far_down = lax.ppermute(high, "rep", down)
        to_up, to_down = merge(who, parts, far_up, far_down, start, cols)
        near_up = lax.ppermute(to_up, "rep", up)
        near_down = lax.ppermute(to_down, "rep", down)
        gradient, outgoing = finish(who, wanted, parts, near_up, near_down, start, cols)
        gradients[chunk] = gradient
        arrived = lax.all_to_all(outgoing, GROUP, split_axis=0, concat_axis=0, tiled=True)
        if chunk > 0:
            earlier.append(left_times(left, owned))
        owned = arrived.reshape(group_size * rows, cols)

    my_layers = lax.dynamic_slice_in_dim(layer_of, me * blocks, blocks)
    onehot = (my_layers[:, None] == jnp.arange(LAYERS, dtype=jnp.int32)[None, :]).astype(f32)
    in_order = sorted(range(len(SENT)), key=lambda c: SENT[c][0])
    wide = jnp.concatenate([gradients[c] for c in in_order], axis=2).astype(f32)
    new_accum = accum + wide * wide
    graft = wide * lax.rsqrt(new_accum)
    graft_blocks = jnp.sum(graft * graft, axis=(1, 2))
    graft_layer = jnp.sum(onehot * graft_blocks[:, None], axis=0)
    mine = lax.dynamic_index_in_dim(table, group_index, 0, keepdims=False)
    chosen = (jnp.arange(blocks, dtype=jnp.int32) == mine).astype(f32)
    my_layer = jnp.sum(chosen[:, None] * onehot, axis=0)
    position = jnp.sum(
        jnp.where(
            table[None, :] == jnp.arange(blocks, dtype=jnp.int32)[:, None],
            jnp.arange(group_size, dtype=jnp.int32)[None, :],
            0,
        ),
        axis=1,
    )
    to_lanes = ((0, 0), (0, LANES - LAYERS))
    graft_row = jnp.pad(graft_layer[None, :], to_lanes)
    layer_row = jnp.pad(my_layer[None, :], to_lanes)
    owned, earlier, graft_row, layer_row, position, onehot, new_accum = lax.optimization_barrier(
        (owned, earlier, graft_row, layer_row, position, onehot, new_accum)
    )

    precond, sums = products(left, right, owned, earlier, graft_row, layer_row)
    outgoing = precond.reshape(group_size, rows, width)
    returned = lax.all_to_all(outgoing, GROUP, split_axis=0, concat_axis=0, tiled=True)
    sums = everywhere(sums)
    layer_scale = jnp.sqrt(sums[0, :LAYERS]) * lax.rsqrt(sums[1, :LAYERS] + 1e-06)
    scale = step_rate * jnp.sum(onehot * layer_scale[None, :], axis=1)

    low, high, new_params = update(who, position, scale, returned, params, reps)
    for offset, part, piece in spread(low, high, reps):
        new_params = lax.dynamic_update_slice(new_params, piece[None], (who[offset], part * half, 0, 0))
    return (new_params.reshape(reps * blocks, rows, width), new_accum)


def solution(mesh):
    split = Mesh(mesh.devices.reshape(4, 4, 2, mesh.shape["rep"]), EVERY)
    placed = (
        P("rep", None, GROUP, None),
        P("rep", GROUP, None),
        P("rep", GROUP, None),
        P("rep", GROUP, None, None, None),
        P("rep", GROUP, None, None, None),
        P(),
        P(),
    )
    return jax.shard_map(
        local,
        mesh=split,
        in_specs=placed,
        out_specs=(P(None, GROUP, None), P("rep", GROUP, None)),
        check_vma=False,
    )
```

```python
import jax
import jax.numpy as jnp
from jax import lax
from jax.experimental import pallas as pl
from jax.experimental.pallas import tpu as pltpu
from jax.sharding import Mesh
from jax.sharding import PartitionSpec as P


LAYERS = 8
LANES = 128
GROUP = ("group_0", "group_1", "group_2")
EVERY = ("group_0", "group_1", "group_2", "rep")
SENT = ((0, 384), (384, 640))


step_rate = 0.5
f32 = jnp.float32
bf16 = jnp.bfloat16


def ring(count, step):
    return [(i, (i + step) % count) for i in range(count)]


def elements(*sizes):
    return tuple(pl.Element(size) for size in sizes)


def merge(who, parts, far_up, far_down, start, cols):
    _, blocks, rows, _ = parts.shape
    half = blocks // 2

    def body(who_ref, above, below, from_down, from_up, out_up, out_down):
        first = pl.program_id(0) == 0

        @pl.when(first)
        def _():
            out_up[...] = (above[0].astype(f32) + from_down[...].astype(f32)).astype(bf16)
            out_down[...] = below[0]

        @pl.when(jnp.logical_not(first))
        def _():
            out_up[...] = above[0]
            out_down[...] = (below[0].astype(f32) + from_up[...].astype(f32)).astype(bf16)

    piece = pl.BlockSpec((half, rows, cols), lambda i, w: (0, 0, 0))
    out = pl.BlockSpec((half, rows, cols), lambda i, w: (i, 0, 0))
    shape = jax.ShapeDtypeStruct((blocks, rows, cols), bf16)
    return pl.pallas_call(
        body,
        grid_spec=pltpu.PrefetchScalarGridSpec(
            num_scalar_prefetch=1,
            grid=(2,),
            in_specs=[
                pl.BlockSpec(elements(1, half, rows, cols), lambda i, w: (w[1], i * half, 0, start)),
                pl.BlockSpec(elements(1, half, rows, cols), lambda i, w: (w[3], i * half, 0, start)),
                piece,
                piece,
            ],
            out_specs=[out, out],
        ),
        out_shape=[shape, shape],
        name="merge",
    )(who, parts, parts, far_up, far_down)


def finish(who, table, parts, up, down, start, cols):
    _, blocks, rows, _ = parts.shape
    slots = table.shape[0]

    def body(who_ref, table_ref, own, one, two, gradient, slotted):
        total = own[0].astype(f32) + one[...].astype(f32) + two[...].astype(f32)
        gradient[...] = total.astype(bf16)
        for slot in range(slots):
            slotted[slot] = gradient[table_ref[slot]]

    block = pl.BlockSpec((blocks, rows, cols), lambda i, w, t: (0, 0, 0))
    return pl.pallas_call(
        body,
        grid_spec=pltpu.PrefetchScalarGridSpec(
            num_scalar_prefetch=2,
            grid=(1,),
            in_specs=[
                pl.BlockSpec(elements(1, blocks, rows, cols), lambda i, w, t: (w[0], 0, 0, start)),
                block,
                block,
            ],
            out_specs=[block, pl.BlockSpec((slots, rows, cols), lambda i, w, t: (0, 0, 0))],
        ),
        out_shape=[
            jax.ShapeDtypeStruct((blocks, rows, cols), bf16),
            jax.ShapeDtypeStruct((slots, rows, cols), bf16),
        ],
        name="finish",
    )(who, table, parts, up, down)


def left_times(left, owned):
    order, cols = owned.shape
    tile = order // 2

    def body(left_ref, owned_ref, out):
        out[...] = jnp.dot(left_ref[...], owned_ref[...], preferred_element_type=f32).astype(bf16)

    return pl.pallas_call(
        body,
        grid=(2,),
        in_specs=[
            pl.BlockSpec((tile, order), lambda i: (i, 0)),
            pl.BlockSpec((order, cols), lambda i: (0, 0)),
        ],
        out_specs=pl.BlockSpec((tile, cols), lambda i: (i, 0)),
        out_shape=jax.ShapeDtypeStruct((order, cols), bf16),
        name="left_times",
    )(left, owned)


def products(left, right, owned, earlier, graft_row, layer_row):
    order, cols = owned.shape
    steps = 2
    tile = order // steps
    last = SENT[-1][0]

    def body(left_ref, right_ref, owned_ref, graft_ref, layer_ref, *rest):
        before, (out, sums, mid) = rest[: len(earlier)], rest[len(earlier) :]
        mid[:, last : last + cols] = jnp.dot(
            left_ref[...], owned_ref[...], preferred_element_type=f32
        ).astype(bf16)
        for ref, (start, size) in zip(before, SENT):
            mid[:, start : start + size] = ref[...]
        out[...] = jnp.dot(mid[...], right_ref[...], preferred_element_type=f32).astype(bf16)
        wide = out[...].astype(f32)
        squares = jnp.sum(jnp.sum(wide * wide, axis=0, keepdims=True), axis=1, keepdims=True)

        @pl.when(pl.program_id(0) == 0)
        def _():
            sums[0:1] = graft_ref[...]
            sums[1:2] = layer_ref[...] * squares

        @pl.when(pl.program_id(0) > 0)
        def _():
            sums[1:2] += layer_ref[...] * squares

    row = pl.BlockSpec((1, LANES), lambda i: (0, 0))
    return pl.pallas_call(
        body,
        grid=(steps,),
        in_specs=[
            pl.BlockSpec((tile, order), lambda i: (i, 0)),
            pl.BlockSpec((order, order), lambda i: (0, 0)),
            pl.BlockSpec((order, cols), lambda i: (0, 0)),
            row,
            row,
            *[pl.BlockSpec((tile, e.shape[1]), lambda i: (i, 0)) for e in earlier],
        ],
        out_specs=[pl.BlockSpec((tile, order), lambda i: (i, 0)), pl.BlockSpec((2, LANES), lambda i: (0, 0))],
        out_shape=[jax.ShapeDtypeStruct((order, order), bf16), jax.ShapeDtypeStruct((2, LANES), f32)],
        scratch_shapes=[pltpu.VMEM((tile, order), bf16)],
        name="products",
    )(left, right, owned, graft_row, layer_row, *earlier)


def pick(position, returned, count):
    slots, rows, cols = returned.shape

    def body(position_ref, returned_ref, out):
        for block in range(count):
            out[block] = returned_ref[position_ref[block]]

    return pl.pallas_call(
        body,
        grid_spec=pltpu.PrefetchScalarGridSpec(
            num_scalar_prefetch=1,
            grid=(1,),
            in_specs=[pl.BlockSpec((slots, rows, cols), lambda i, p: (0, 0, 0))],
            out_specs=pl.BlockSpec((count, rows, cols), lambda i, p: (0, 0, 0)),
        ),
        out_shape=jax.ShapeDtypeStruct((count, rows, cols), bf16),
        name="pick",
    )(position, returned)


def update(who, position, scale, returned, params, reps):
    blocks, rows, cols = params.shape
    half = blocks // 2
    slots = returned.shape[0]

    def body(who_ref, position_ref, scale_ref, returned_ref, params_ref, high, whole):
        for block in range(blocks):
            change = scale_ref[block] * returned_ref[position_ref[block]].astype(f32)
            new = (params_ref[block].astype(f32) - change).astype(bf16)
            whole[0, block] = new
            if block >= half:
                high[block - half] = new

    return pl.pallas_call(
        body,
        grid_spec=pltpu.PrefetchScalarGridSpec(
            num_scalar_prefetch=3,
            grid=(1,),
            in_specs=[
                pl.BlockSpec((slots, rows, cols), lambda i, w, p, s: (0, 0, 0)),
                pl.BlockSpec((blocks, rows, cols), lambda i, w, p, s: (0, 0, 0)),
            ],
            out_specs=[
                pl.BlockSpec((half, rows, cols), lambda i, w, p, s: (0, 0, 0)),
                pl.BlockSpec((1, blocks, rows, cols), lambda i, w, p, s: (w[0], 0, 0, 0)),
            ],
        ),
        out_shape=[
            jax.ShapeDtypeStruct((half, rows, cols), bf16),
            jax.ShapeDtypeStruct((reps, blocks, rows, cols), bf16),
        ],
        name="update",
    )(who, position, scale, returned, params)


def everywhere(value):
    swap, near, wrap = [(0, 1), (1, 0)], [(0, 1), (1, 0), (2, 3), (3, 2)], [(0, 3), (3, 0), (1, 2), (2, 1)]
    steps = [("group_2", swap)]
    for axis in ("rep", "group_0", "group_1"):
        steps += [(axis, near), (axis, wrap)]
    for axis, pairs in steps:
        value = value + lax.ppermute(value, axis, pairs)
    return value


def spread(value, reps, onward):
    up, down = ring(reps, 1), ring(reps, -1)
    from_down = lax.ppermute(value, "rep", up)
    from_up = lax.ppermute(value, "rep", down)
    far = lax.ppermute(from_down, "rep", up) if onward > 0 else lax.ppermute(from_up, "rep", down)
    return ((3, from_down), (1, from_up), (2, far))


def local(grad_parts, params, accum, left_pre, right_pre, slot_block, layer_of):
    group_size = lax.axis_size(GROUP)
    reps = lax.axis_size("rep")
    me = lax.axis_index("rep")
    group_index = lax.axis_index(GROUP)
    blocks, rows, width = params.shape
    half = blocks // 2
    up, down = ring(reps, 1), ring(reps, -1)
    parts = grad_parts[0].reshape(reps, blocks, rows, width)
    who = lax.rem(me + jnp.arange(reps, dtype=jnp.int32), reps)
    table = lax.dynamic_index_in_dim(slot_block, me, 0, keepdims=False).reshape(-1)
    wanted = jnp.maximum(table, 0)
    left, right = left_pre[0, 0, 0], right_pre[0, 0, 0]

    far = lax.rem(me + 2, reps)
    gradients, earlier, owned = [None] * len(SENT), [], None
    for chunk, (start, cols) in enumerate(SENT):
        low = lax.dynamic_slice(parts, (far, 0, 0, start), (1, half, rows, cols))[0]
        high = lax.dynamic_slice(parts, (far, half, 0, start), (1, half, rows, cols))[0]
        far_up = lax.ppermute(low, "rep", up)
        far_down = lax.ppermute(high, "rep", down)
        to_up, to_down = merge(who, parts, far_up, far_down, start, cols)
        near_up = lax.ppermute(to_up, "rep", up)
        near_down = lax.ppermute(to_down, "rep", down)
        gradient, outgoing = finish(who, wanted, parts, near_up, near_down, start, cols)
        gradients[chunk] = gradient
        arrived = lax.all_to_all(outgoing, GROUP, split_axis=0, concat_axis=0, tiled=True)
        if chunk > 0:
            earlier.append(left_times(left, owned))
        owned = arrived.reshape(group_size * rows, cols)

    ahead = spread(params[:half], reps, 1)

    onehots = (layer_of[:, None] == jnp.arange(LAYERS, dtype=jnp.int32)[None, :]).astype(f32)
    onehot = lax.dynamic_slice_in_dim(onehots, me * blocks, blocks)
    in_order = sorted(range(len(SENT)), key=lambda c: SENT[c][0])
    wide = jnp.concatenate([gradients[c] for c in in_order], axis=2).astype(f32)
    new_accum = accum + wide * wide
    graft = wide * lax.rsqrt(new_accum)
    graft_blocks = jnp.sum(graft * graft, axis=(1, 2))
    graft_layer = jnp.sum(onehot * graft_blocks[:, None], axis=0)
    mine = lax.dynamic_index_in_dim(table, group_index, 0, keepdims=False)
    chosen = (jnp.arange(blocks, dtype=jnp.int32) == mine).astype(f32)
    my_layer = jnp.sum(chosen[:, None] * onehot, axis=0)
    position = jnp.sum(
        jnp.where(
            table[None, :] == jnp.arange(blocks, dtype=jnp.int32)[:, None],
            jnp.arange(group_size, dtype=jnp.int32)[None, :],
            0,
        ),
        axis=1,
    )
    to_lanes = ((0, 0), (0, LANES - LAYERS))
    graft_row = jnp.pad(graft_layer[None, :], to_lanes)
    layer_row = jnp.pad(my_layer[None, :], to_lanes)
    owned, earlier, graft_row, layer_row, position, onehots, new_accum = lax.optimization_barrier(
        (owned, earlier, graft_row, layer_row, position, onehots, new_accum)
    )

    precond, sums = products(left, right, owned, earlier, graft_row, layer_row)
    outgoing = precond.reshape(group_size, rows, width)
    returned = lax.all_to_all(outgoing, GROUP, split_axis=0, concat_axis=0, tiled=True)
    sums = everywhere(sums)
    layer_scale = jnp.sqrt(sums[0, :LAYERS]) * lax.rsqrt(sums[1, :LAYERS] + 1e-06)
    scales = (step_rate * jnp.sum(onehots * layer_scale[None, :], axis=1)).reshape(reps, blocks)

    changes = spread(pick(position, returned, half), reps, 1)
    high, new_params = update(who, position, scales[me], returned, params, reps)
    finished = spread(high, reps, -1)
    for (offset, old), (_, change) in zip(ahead, changes):
        scale = scales[who[offset]][:half, None, None]
        new = (old.astype(f32) - scale * change.astype(f32)).astype(bf16)
        new_params = lax.dynamic_update_slice(new_params, new[None], (who[offset], 0, 0, 0))
    for offset, piece in finished:
        new_params = lax.dynamic_update_slice(new_params, piece[None], (who[offset], half, 0, 0))
    return (new_params.reshape(reps * blocks, rows, width), new_accum)


def solution(mesh):
    split = Mesh(mesh.devices.reshape(4, 4, 2, mesh.shape["rep"]), EVERY)
    placed = (
        P("rep", None, GROUP, None),
        P("rep", GROUP, None),
        P("rep", GROUP, None),
        P("rep", GROUP, None, None, None),
        P("rep", GROUP, None, None, None),
        P(),
        P(),
    )
    return jax.shard_map(
        local,
        mesh=split,
        in_specs=placed,
        out_specs=(P(None, GROUP, None), P("rep", GROUP, None)),
        check_vma=False,
    )
```

```python
import jax
import jax.numpy as jnp
from jax import lax
from jax.experimental import pallas as pl
from jax.experimental.pallas import tpu as pltpu
from jax.sharding import Mesh
from jax.sharding import PartitionSpec as P


LAYERS = 8
LANES = 128
GROUP = ("group_0", "group_1", "group_2")
EVERY = ("group_0", "group_1", "group_2", "rep")
SENT = ((0, 384), (384, 640))
RAW = 16


step_rate = 0.5
f32 = jnp.float32
bf16 = jnp.bfloat16


def ring(count, step):
    return [(i, (i + step) % count) for i in range(count)]


def elements(*sizes):
    return tuple(pl.Element(size) for size in sizes)


def merge(who, parts, far_up, far_down, start, cols):
    _, blocks, rows, _ = parts.shape
    half = blocks // 2

    def body(who_ref, above, below, from_down, from_up, out_up, out_down):
        first = pl.program_id(0) == 0

        @pl.when(first)
        def _():
            out_up[...] = (above[0].astype(f32) + from_down[...].astype(f32)).astype(bf16)
            out_down[...] = below[0]

        @pl.when(jnp.logical_not(first))
        def _():
            out_up[...] = above[0]
            out_down[...] = (below[0].astype(f32) + from_up[...].astype(f32)).astype(bf16)

    piece = pl.BlockSpec((half, rows, cols), lambda i, w: (0, 0, 0))
    out = pl.BlockSpec((half, rows, cols), lambda i, w: (i, 0, 0))
    shape = jax.ShapeDtypeStruct((blocks, rows, cols), bf16)
    return pl.pallas_call(
        body,
        grid_spec=pltpu.PrefetchScalarGridSpec(
            num_scalar_prefetch=1,
            grid=(2,),
            in_specs=[
                pl.BlockSpec(elements(1, half, rows, cols), lambda i, w: (w[1], i * half, 0, start)),
                pl.BlockSpec(elements(1, half, rows, cols), lambda i, w: (w[3], i * half, 0, start)),
                piece,
                piece,
            ],
            out_specs=[out, out],
        ),
        out_shape=[shape, shape],
        name="merge",
    )(who, parts, parts, far_up, far_down)


def finish(who, table, parts, up, down, start, cols):
    _, blocks, rows, _ = parts.shape
    slots = table.shape[0]

    def body(who_ref, table_ref, own, one, two, gradient, slotted):
        total = own[0].astype(f32) + one[...].astype(f32) + two[...].astype(f32)
        gradient[...] = total.astype(bf16)
        for slot in range(slots):
            slotted[slot] = gradient[table_ref[slot]]

    block = pl.BlockSpec((blocks, rows, cols), lambda i, w, t: (0, 0, 0))
    return pl.pallas_call(
        body,
        grid_spec=pltpu.PrefetchScalarGridSpec(
            num_scalar_prefetch=2,
            grid=(1,),
            in_specs=[
                pl.BlockSpec(elements(1, blocks, rows, cols), lambda i, w, t: (w[0], 0, 0, start)),
                block,
                block,
            ],
            out_specs=[block, pl.BlockSpec((slots, rows, cols), lambda i, w, t: (0, 0, 0))],
        ),
        out_shape=[
            jax.ShapeDtypeStruct((blocks, rows, cols), bf16),
            jax.ShapeDtypeStruct((slots, rows, cols), bf16),
        ],
        name="finish",
    )(who, table, parts, up, down)


def left_times(left, owned):
    order, cols = owned.shape
    tile = order // 2

    def body(left_ref, owned_ref, out):
        out[...] = jnp.dot(left_ref[...], owned_ref[...], preferred_element_type=f32).astype(bf16)

    return pl.pallas_call(
        body,
        grid=(2,),
        in_specs=[
            pl.BlockSpec((tile, order), lambda i: (i, 0)),
            pl.BlockSpec((order, cols), lambda i: (0, 0)),
        ],
        out_specs=pl.BlockSpec((tile, cols), lambda i: (i, 0)),
        out_shape=jax.ShapeDtypeStruct((order, cols), bf16),
        name="left_times",
    )(left, owned)


def products(left, right, owned, earlier, graft_row, layer_row):
    order, cols = owned.shape
    steps = 2
    tile = order // steps
    last = SENT[-1][0]

    def body(left_ref, right_ref, owned_ref, graft_ref, layer_ref, *rest):
        before, (out, sums, mid) = rest[: len(earlier)], rest[len(earlier) :]
        mid[:, last : last + cols] = jnp.dot(
            left_ref[...], owned_ref[...], preferred_element_type=f32
        ).astype(bf16)
        for ref, (start, size) in zip(before, SENT):
            mid[:, start : start + size] = ref[...]
        out[...] = jnp.dot(mid[...], right_ref[...], preferred_element_type=f32).astype(bf16)
        wide = out[...].astype(f32)
        squares = jnp.sum(jnp.sum(wide * wide, axis=0, keepdims=True), axis=1, keepdims=True)

        @pl.when(pl.program_id(0) == 0)
        def _():
            sums[0:1] = graft_ref[...]
            sums[1:2] = layer_ref[...] * squares

        @pl.when(pl.program_id(0) > 0)
        def _():
            sums[1:2] += layer_ref[...] * squares

    row = pl.BlockSpec((1, LANES), lambda i: (0, 0))
    return pl.pallas_call(
        body,
        grid=(steps,),
        in_specs=[
            pl.BlockSpec((tile, order), lambda i: (i, 0)),
            pl.BlockSpec((order, order), lambda i: (0, 0)),
            pl.BlockSpec((order, cols), lambda i: (0, 0)),
            row,
            row,
            *[pl.BlockSpec((tile, e.shape[1]), lambda i: (i, 0)) for e in earlier],
        ],
        out_specs=[pl.BlockSpec((tile, order), lambda i: (i, 0)), pl.BlockSpec((2, LANES), lambda i: (0, 0))],
        out_shape=[jax.ShapeDtypeStruct((order, order), bf16), jax.ShapeDtypeStruct((2, LANES), f32)],
        scratch_shapes=[pltpu.VMEM((tile, order), bf16)],
        name="products",
    )(left, right, owned, graft_row, layer_row, *earlier)


def pick(position, returned):
    _, rows, cols = returned.shape
    half = RAW // 2

    def body(position_ref, returned_ref, low, high, sems):
        copies = []
        for block in range(RAW):
            out = low.at[block] if block < half else high.at[block - half]
            copies.append(pltpu.make_async_copy(returned_ref.at[position_ref[block]], out, sems.at[block]))
        for copy in copies:
            copy.start()
        for copy in copies:
            copy.wait()

    hbm = pl.BlockSpec(memory_space=pltpu.HBM)
    shape = jax.ShapeDtypeStruct((half, rows, cols), bf16)
    return pl.pallas_call(
        body,
        in_specs=[pl.BlockSpec(memory_space=pltpu.SMEM), hbm],
        out_specs=[hbm, hbm],
        out_shape=[shape, shape],
        scratch_shapes=[pltpu.SemaphoreType.DMA((RAW,))],
        name="pick",
    )(position, returned)


def update(who, position, scale, returned, params, reps):
    blocks, rows, cols = params.shape
    part = (blocks - RAW) // 2

    def body(who_ref, position_ref, scale_ref, returned_ref, params_ref, low, high, whole, picked, sems):
        copies = [
            pltpu.make_async_copy(returned_ref.at[position_ref[block]], picked.at[block], sems.at[block])
            for block in range(blocks)
        ]
        for copy in copies:
            copy.start()
        for block, copy in enumerate(copies):
            copy.wait()
            change = scale_ref[block] * picked[block].astype(f32)
            new = (params_ref[block].astype(f32) - change).astype(bf16)
            whole[0, block] = new
            if RAW <= block < RAW + part:
                low[block - RAW] = new
            elif block >= RAW + part:
                high[block - RAW - part] = new

    piece = pl.BlockSpec((part, rows, cols), lambda i, w, p, s: (0, 0, 0))
    shape = jax.ShapeDtypeStruct((part, rows, cols), bf16)
    return pl.pallas_call(
        body,
        grid_spec=pltpu.PrefetchScalarGridSpec(
            num_scalar_prefetch=3,
            grid=(1,),
            in_specs=[
                pl.BlockSpec(memory_space=pltpu.HBM),
                pl.BlockSpec((blocks, rows, cols), lambda i, w, p, s: (0, 0, 0)),
            ],
            out_specs=[
                piece,
                piece,
                pl.BlockSpec((1, blocks, rows, cols), lambda i, w, p, s: (w[0], 0, 0, 0)),
            ],
            scratch_shapes=[pltpu.VMEM((blocks, rows, cols), bf16), pltpu.SemaphoreType.DMA((blocks,))],
        ),
        out_shape=[shape, shape, jax.ShapeDtypeStruct((reps, blocks, rows, cols), bf16)],
        name="update",
    )(who, position, scale, returned, params)


def everywhere(value):
    swap, near, wrap = [(0, 1), (1, 0)], [(0, 1), (1, 0), (2, 3), (3, 2)], [(0, 3), (3, 0), (1, 2), (2, 1)]
    steps = [("group_2", swap)]
    for axis in ("rep", "group_0", "group_1"):
        steps += [(axis, near), (axis, wrap)]
    for axis, pairs in steps:
        value = value + lax.ppermute(value, axis, pairs)
    return value


def spread(low, high, reps):
    up, down = ring(reps, 1), ring(reps, -1)
    low_up = lax.ppermute(low, "rep", up)
    high_down = lax.ppermute(high, "rep", down)
    high_up = lax.ppermute(high, "rep", up)
    low_down = lax.ppermute(low, "rep", down)
    far_low = lax.ppermute(low_up, "rep", up)
    far_high = lax.ppermute(high_down, "rep", down)
    return (
        (3, 0, low_up),
        (1, 1, high_down),
        (3, 1, high_up),
        (1, 0, low_down),
        (2, 0, far_low),
        (2, 1, far_high),
    )


def local(grad_parts, params, accum, left_pre, right_pre, slot_block, layer_of):
    group_size = lax.axis_size(GROUP)
    reps = lax.axis_size("rep")
    me = lax.axis_index("rep")
    group_index = lax.axis_index(GROUP)
    blocks, rows, width = params.shape
    half = blocks // 2
    up, down = ring(reps, 1), ring(reps, -1)
    parts = grad_parts[0].reshape(reps, blocks, rows, width)
    who = lax.rem(me + jnp.arange(reps, dtype=jnp.int32), reps)
    table = lax.dynamic_index_in_dim(slot_block, me, 0, keepdims=False).reshape(-1)
    wanted = jnp.maximum(table, 0)
    left, right = left_pre[0, 0, 0], right_pre[0, 0, 0]

    far = lax.rem(me + 2, reps)
    gradients, earlier, owned = [None] * len(SENT), [], None
    for chunk, (start, cols) in enumerate(SENT):
        low = lax.dynamic_slice(parts, (far, 0, 0, start), (1, half, rows, cols))[0]
        high = lax.dynamic_slice(parts, (far, half, 0, start), (1, half, rows, cols))[0]
        far_up = lax.ppermute(low, "rep", up)
        far_down = lax.ppermute(high, "rep", down)
        to_up, to_down = merge(who, parts, far_up, far_down, start, cols)
        near_up = lax.ppermute(to_up, "rep", up)
        near_down = lax.ppermute(to_down, "rep", down)
        gradient, outgoing = finish(who, wanted, parts, near_up, near_down, start, cols)
        gradients[chunk] = gradient
        arrived = lax.all_to_all(outgoing, GROUP, split_axis=0, concat_axis=0, tiled=True)
        if chunk > 0:
            earlier.append(left_times(left, owned))
        owned = arrived.reshape(group_size * rows, cols)

    ahead = spread(params[: RAW // 2], params[RAW // 2 : RAW], reps)

    onehots = (layer_of[:, None] == jnp.arange(LAYERS, dtype=jnp.int32)[None, :]).astype(f32)
    onehot = lax.dynamic_slice_in_dim(onehots, me * blocks, blocks)
    in_order = sorted(range(len(SENT)), key=lambda c: SENT[c][0])
    wide = jnp.concatenate([gradients[c] for c in in_order], axis=2).astype(f32)
    new_accum = accum + wide * wide
    graft = wide * lax.rsqrt(new_accum)
    graft_blocks = jnp.sum(graft * graft, axis=(1, 2))
    graft_layer = jnp.sum(onehot * graft_blocks[:, None], axis=0)
    mine = lax.dynamic_index_in_dim(table, group_index, 0, keepdims=False)
    chosen = (jnp.arange(blocks, dtype=jnp.int32) == mine).astype(f32)
    my_layer = jnp.sum(chosen[:, None] * onehot, axis=0)
    position = jnp.sum(
        jnp.where(
            table[None, :] == jnp.arange(blocks, dtype=jnp.int32)[:, None],
            jnp.arange(group_size, dtype=jnp.int32)[None, :],
            0,
        ),
        axis=1,
    )
    to_lanes = ((0, 0), (0, LANES - LAYERS))
    graft_row = jnp.pad(graft_layer[None, :], to_lanes)
    layer_row = jnp.pad(my_layer[None, :], to_lanes)
    owned, earlier, graft_row, layer_row, position, onehots, new_accum = lax.optimization_barrier(
        (owned, earlier, graft_row, layer_row, position, onehots, new_accum)
    )

    precond, sums = products(left, right, owned, earlier, graft_row, layer_row)
    outgoing = precond.reshape(group_size, rows, width)
    returned = lax.all_to_all(outgoing, GROUP, split_axis=0, concat_axis=0, tiled=True)
    sums = everywhere(sums)
    layer_scale = jnp.sqrt(sums[0, :LAYERS]) * lax.rsqrt(sums[1, :LAYERS] + 1e-06)
    scales = (step_rate * jnp.sum(onehots * layer_scale[None, :], axis=1)).reshape(reps, blocks)

    def owner(offset):
        return lax.rem(me + offset, reps)

    changes = spread(*pick(position, returned), reps)
    low, high, new_params = update(who, position, scales[me], returned, params, reps)
    finished = spread(low, high, reps)
    for (offset, part, old), (_, _, change) in zip(ahead, changes):
        size = RAW // 2
        scale = lax.dynamic_slice(scales, (owner(offset), part * size), (1, size))[0, :, None, None]
        new = (old.astype(f32) - scale * change.astype(f32)).astype(bf16)
        new_params = lax.dynamic_update_slice(new_params, new[None], (owner(offset), part * size, 0, 0))
    for offset, part, piece in finished:
        first = RAW + part * piece.shape[0]
        new_params = lax.dynamic_update_slice(new_params, piece[None], (owner(offset), first, 0, 0))
    return (new_params.reshape(reps * blocks, rows, width), new_accum)


def solution(mesh):
    split = Mesh(mesh.devices.reshape(4, 4, 2, mesh.shape["rep"]), EVERY)
    placed = (
        P("rep", None, GROUP, None),
        P("rep", GROUP, None),
        P("rep", GROUP, None),
        P("rep", GROUP, None, None, None),
        P("rep", GROUP, None, None, None),
        P(),
        P(),
    )
    return jax.shard_map(
        local,
        mesh=split,
        in_specs=placed,
        out_specs=(P(None, GROUP, None), P("rep", GROUP, None)),
        check_vma=False,
    )
```

```python
import jax
import jax.numpy as jnp
from jax import lax
from jax.experimental import pallas as pl
from jax.experimental.pallas import tpu as pltpu
from jax.sharding import Mesh
from jax.sharding import PartitionSpec as P


LAYERS = 8
LANES = 128
GROUP = ("group_0", "group_1", "group_2")
EVERY = ("group_0", "group_1", "group_2", "rep")
SENT = ((0, 384), (384, 640))
RAW = (4, 12)


step_rate = 0.5
f32 = jnp.float32
bf16 = jnp.bfloat16


def ring(count, step):
    return [(i, (i + step) % count) for i in range(count)]


def elements(*sizes):
    return tuple(pl.Element(size) for size in sizes)


def merge(who, parts, far_up, far_down, start, cols):
    _, blocks, rows, _ = parts.shape
    half = blocks // 2

    def body(who_ref, above, below, from_down, from_up, out_up, out_down):
        first = pl.program_id(0) == 0

        @pl.when(first)
        def _():
            out_up[...] = (above[0].astype(f32) + from_down[...].astype(f32)).astype(bf16)
            out_down[...] = below[0]

        @pl.when(jnp.logical_not(first))
        def _():
            out_up[...] = above[0]
            out_down[...] = (below[0].astype(f32) + from_up[...].astype(f32)).astype(bf16)

    piece = pl.BlockSpec((half, rows, cols), lambda i, w: (0, 0, 0))
    out = pl.BlockSpec((half, rows, cols), lambda i, w: (i, 0, 0))
    shape = jax.ShapeDtypeStruct((blocks, rows, cols), bf16)
    return pl.pallas_call(
        body,
        grid_spec=pltpu.PrefetchScalarGridSpec(
            num_scalar_prefetch=1,
            grid=(2,),
            in_specs=[
                pl.BlockSpec(elements(1, half, rows, cols), lambda i, w: (w[1], i * half, 0, start)),
                pl.BlockSpec(elements(1, half, rows, cols), lambda i, w: (w[3], i * half, 0, start)),
                piece,
                piece,
            ],
            out_specs=[out, out],
        ),
        out_shape=[shape, shape],
        name="merge",
    )(who, parts, parts, far_up, far_down)


def finish(who, table, parts, up, down, start, cols):
    _, blocks, rows, _ = parts.shape
    slots = table.shape[0]

    def body(who_ref, table_ref, own, one, two, gradient, slotted):
        total = own[0].astype(f32) + one[...].astype(f32) + two[...].astype(f32)
        gradient[...] = total.astype(bf16)
        for slot in range(slots):
            slotted[slot] = gradient[table_ref[slot]]

    block = pl.BlockSpec((blocks, rows, cols), lambda i, w, t: (0, 0, 0))
    return pl.pallas_call(
        body,
        grid_spec=pltpu.PrefetchScalarGridSpec(
            num_scalar_prefetch=2,
            grid=(1,),
            in_specs=[
                pl.BlockSpec(elements(1, blocks, rows, cols), lambda i, w, t: (w[0], 0, 0, start)),
                block,
                block,
            ],
            out_specs=[block, pl.BlockSpec((slots, rows, cols), lambda i, w, t: (0, 0, 0))],
        ),
        out_shape=[
            jax.ShapeDtypeStruct((blocks, rows, cols), bf16),
            jax.ShapeDtypeStruct((slots, rows, cols), bf16),
        ],
        name="finish",
    )(who, table, parts, up, down)


def left_times(left, owned):
    order, cols = owned.shape
    tile = order // 2

    def body(left_ref, owned_ref, out):
        out[...] = jnp.dot(left_ref[...], owned_ref[...], preferred_element_type=f32).astype(bf16)

    return pl.pallas_call(
        body,
        grid=(2,),
        in_specs=[
            pl.BlockSpec((tile, order), lambda i: (i, 0)),
            pl.BlockSpec((order, cols), lambda i: (0, 0)),
        ],
        out_specs=pl.BlockSpec((tile, cols), lambda i: (i, 0)),
        out_shape=jax.ShapeDtypeStruct((order, cols), bf16),
        name="left_times",
    )(left, owned)


def products(left, right, owned, earlier, graft_row, layer_row):
    order, cols = owned.shape
    steps = 2
    tile = order // steps
    last = SENT[-1][0]

    def body(left_ref, right_ref, owned_ref, graft_ref, layer_ref, *rest):
        before, (out, sums, mid) = rest[: len(earlier)], rest[len(earlier) :]
        mid[:, last : last + cols] = jnp.dot(
            left_ref[...], owned_ref[...], preferred_element_type=f32
        ).astype(bf16)
        for ref, (start, size) in zip(before, SENT):
            mid[:, start : start + size] = ref[...]
        out[...] = jnp.dot(mid[...], right_ref[...], preferred_element_type=f32).astype(bf16)
        wide = out[...].astype(f32)
        squares = jnp.sum(jnp.sum(wide * wide, axis=0, keepdims=True), axis=1, keepdims=True)

        @pl.when(pl.program_id(0) == 0)
        def _():
            sums[0:1] = graft_ref[...]
            sums[1:2] = layer_ref[...] * squares

        @pl.when(pl.program_id(0) > 0)
        def _():
            sums[1:2] += layer_ref[...] * squares

    row = pl.BlockSpec((1, LANES), lambda i: (0, 0))
    return pl.pallas_call(
        body,
        grid=(steps,),
        in_specs=[
            pl.BlockSpec((tile, order), lambda i: (i, 0)),
            pl.BlockSpec((order, order), lambda i: (0, 0)),
            pl.BlockSpec((order, cols), lambda i: (0, 0)),
            row,
            row,
            *[pl.BlockSpec((tile, e.shape[1]), lambda i: (i, 0)) for e in earlier],
        ],
        out_specs=[pl.BlockSpec((tile, order), lambda i: (i, 0)), pl.BlockSpec((2, LANES), lambda i: (0, 0))],
        out_shape=[jax.ShapeDtypeStruct((order, order), bf16), jax.ShapeDtypeStruct((2, LANES), f32)],
        scratch_shapes=[pltpu.VMEM((tile, order), bf16)],
        name="products",
    )(left, right, owned, graft_row, layer_row, *earlier)


def fetch(position_ref, returned_ref, target, sems, blocks):
    copies = []
    for block in blocks:
        copy = pltpu.make_async_copy(returned_ref.at[position_ref[block]], target(block), sems.at[block])
        copy.start()
        copies.append(copy)
    return copies


def pick(position, returned):
    _, rows, cols = returned.shape
    split, total = RAW[0], sum(RAW)

    def body(position_ref, returned_ref, low, high, sems):
        def target(block):
            return low.at[block] if block < split else high.at[block - split]

        for copy in fetch(position_ref, returned_ref, target, sems, range(total)):
            copy.wait()

    return pl.pallas_call(
        body,
        grid_spec=pltpu.PrefetchScalarGridSpec(
            num_scalar_prefetch=1,
            grid=(1,),
            in_specs=[pl.BlockSpec(memory_space=pltpu.HBM)],
            out_specs=[pl.BlockSpec((size, rows, cols), lambda i, p: (0, 0, 0)) for size in RAW],
            scratch_shapes=[pltpu.SemaphoreType.DMA((total,))],
        ),
        out_shape=[jax.ShapeDtypeStruct((size, rows, cols), bf16) for size in RAW],
        name="pick",
    )(position, returned)


def update(who, position, scale, returned, params, reps):
    blocks, rows, cols = params.shape
    first = sum(RAW)

    def body(who_ref, position_ref, scale_ref, returned_ref, params_ref, last, whole, picked, sems):
        copies = fetch(position_ref, returned_ref, lambda block: picked.at[block], sems, range(blocks))
        for block, copy in enumerate(copies):
            copy.wait()
            change = scale_ref[block] * picked[block].astype(f32)
            new = (params_ref[block].astype(f32) - change).astype(bf16)
            whole[0, block] = new
            if block >= first:
                last[block - first] = new

    return pl.pallas_call(
        body,
        grid_spec=pltpu.PrefetchScalarGridSpec(
            num_scalar_prefetch=3,
            grid=(1,),
            in_specs=[
                pl.BlockSpec(memory_space=pltpu.HBM),
                pl.BlockSpec((blocks, rows, cols), lambda i, w, p, s: (0, 0, 0)),
            ],
            out_specs=[
                pl.BlockSpec((blocks - first, rows, cols), lambda i, w, p, s: (0, 0, 0)),
                pl.BlockSpec((1, blocks, rows, cols), lambda i, w, p, s: (w[0], 0, 0, 0)),
            ],
            scratch_shapes=[pltpu.VMEM((blocks, rows, cols), bf16), pltpu.SemaphoreType.DMA((blocks,))],
        ),
        out_shape=[
            jax.ShapeDtypeStruct((blocks - first, rows, cols), bf16),
            jax.ShapeDtypeStruct((reps, blocks, rows, cols), bf16),
        ],
        name="update",
    )(who, position, scale, returned, params)


def everywhere(value):
    value = value + lax.ppermute(value, "group_2", [(0, 1), (1, 0)])
    for axis in ("rep", "group_0", "group_1"):
        one, two, three = [lax.ppermute(value, axis, ring(4, step)) for step in (1, 2, 3)]
        value = (value + two) + (one + three)
    return value


def spread(low, high, reps):
    up, down = ring(reps, 1), ring(reps, -1)
    high_up = lax.ppermute(high, "rep", up)
    high_down = lax.ppermute(high, "rep", down)
    low_up = lax.ppermute(low, "rep", up)
    low_down = lax.ppermute(low, "rep", down)
    far_high = lax.ppermute(high_down, "rep", down)
    far_low = lax.ppermute(low_up, "rep", up)
    return (
        (3, 1, high_up),
        (1, 1, high_down),
        (3, 0, low_up),
        (1, 0, low_down),
        (2, 0, far_low),
        (2, 1, far_high),
    )


def local(grad_parts, params, accum, left_pre, right_pre, slot_block, layer_of):
    group_size = lax.axis_size(GROUP)
    reps = lax.axis_size("rep")
    me = lax.axis_index("rep")
    group_index = lax.axis_index(GROUP)
    blocks, rows, width = params.shape
    half = blocks // 2
    up, down = ring(reps, 1), ring(reps, -1)
    parts = grad_parts[0].reshape(reps, blocks, rows, width)
    who = lax.rem(me + jnp.arange(reps, dtype=jnp.int32), reps)
    table = lax.dynamic_index_in_dim(slot_block, me, 0, keepdims=False).reshape(-1)
    wanted = jnp.maximum(table, 0)
    left, right = left_pre[0, 0, 0], right_pre[0, 0, 0]

    far = lax.rem(me + 2, reps)
    gradients, earlier, owned = [None] * len(SENT), [], None
    for chunk, (start, cols) in enumerate(SENT):
        low = lax.dynamic_slice(parts, (far, 0, 0, start), (1, half, rows, cols))[0]
        high = lax.dynamic_slice(parts, (far, half, 0, start), (1, half, rows, cols))[0]
        far_up = lax.ppermute(low, "rep", up)
        far_down = lax.ppermute(high, "rep", down)
        to_up, to_down = merge(who, parts, far_up, far_down, start, cols)
        near_up = lax.ppermute(to_up, "rep", up)
        near_down = lax.ppermute(to_down, "rep", down)
        gradient, outgoing = finish(who, wanted, parts, near_up, near_down, start, cols)
        gradients[chunk] = gradient
        arrived = lax.all_to_all(outgoing, GROUP, split_axis=0, concat_axis=0, tiled=True)
        if chunk > 0:
            earlier.append(left_times(left, owned))
        owned = arrived.reshape(group_size * rows, cols)

    ahead = spread(params[: RAW[0]], params[RAW[0] : sum(RAW)], reps)

    onehots = (layer_of[:, None] == jnp.arange(LAYERS, dtype=jnp.int32)[None, :]).astype(f32)
    onehot = lax.dynamic_slice_in_dim(onehots, me * blocks, blocks)
    in_order = sorted(range(len(SENT)), key=lambda c: SENT[c][0])
    wide = jnp.concatenate([gradients[c] for c in in_order], axis=2).astype(f32)
    new_accum = accum + wide * wide
    graft = wide * lax.rsqrt(new_accum)
    graft_blocks = jnp.sum(graft * graft, axis=(1, 2))
    graft_layer = jnp.sum(onehot * graft_blocks[:, None], axis=0)
    mine = lax.dynamic_index_in_dim(table, group_index, 0, keepdims=False)
    chosen = (jnp.arange(blocks, dtype=jnp.int32) == mine).astype(f32)
    my_layer = jnp.sum(chosen[:, None] * onehot, axis=0)
    position = jnp.sum(
        jnp.where(
            table[None, :] == jnp.arange(blocks, dtype=jnp.int32)[:, None],
            jnp.arange(group_size, dtype=jnp.int32)[None, :],
            0,
        ),
        axis=1,
    )
    to_lanes = ((0, 0), (0, LANES - LAYERS))
    graft_row = jnp.pad(graft_layer[None, :], to_lanes)
    layer_row = jnp.pad(my_layer[None, :], to_lanes)
    owned, earlier, graft_row, layer_row, position, onehots, new_accum = lax.optimization_barrier(
        (owned, earlier, graft_row, layer_row, position, onehots, new_accum)
    )

    precond, sums = products(left, right, owned, earlier, graft_row, layer_row)
    outgoing = precond.reshape(group_size, rows, width)
    returned = lax.all_to_all(outgoing, GROUP, split_axis=0, concat_axis=0, tiled=True)
    sums = everywhere(sums)
    layer_scale = jnp.sqrt(sums[0, :LAYERS]) * lax.rsqrt(sums[1, :LAYERS] + 1e-06)
    scales = (step_rate * jnp.sum(onehots * layer_scale[None, :], axis=1)).reshape(reps, blocks)

    def owner(offset):
        return lax.rem(me + offset, reps)

    changes = spread(*pick(position, returned), reps)
    last, new_params = update(who, position, scales[me], returned, params, reps)
    from_down = lax.ppermute(last, "rep", up)
    from_up = lax.ppermute(last, "rep", down)
    onward = lax.ppermute(from_down, "rep", up)
    for (offset, part, old), (_, _, change) in zip(ahead, changes):
        first = RAW[0] * part
        scale = lax.dynamic_slice(scales, (owner(offset), first), (1, RAW[part]))[0, :, None, None]
        new = (old.astype(f32) - scale * change.astype(f32)).astype(bf16)
        new_params = lax.dynamic_update_slice(new_params, new[None], (owner(offset), first, 0, 0))
    for offset, piece in ((3, from_down), (1, from_up), (2, onward)):
        new_params = lax.dynamic_update_slice(new_params, piece[None], (owner(offset), sum(RAW), 0, 0))
    return (new_params.reshape(reps * blocks, rows, width), new_accum)


def solution(mesh):
    split = Mesh(mesh.devices.reshape(4, 4, 2, mesh.shape["rep"]), EVERY)
    placed = (
        P("rep", None, GROUP, None),
        P("rep", GROUP, None),
        P("rep", GROUP, None),
        P("rep", GROUP, None, None, None),
        P("rep", GROUP, None, None, None),
        P(),
        P(),
    )
    return jax.shard_map(
        local,
        mesh=split,
        in_specs=placed,
        out_specs=(P(None, GROUP, None), P("rep", GROUP, None)),
        check_vma=False,
    )
```

```python
import jax
import jax.numpy as jnp
from jax import lax
from jax.experimental import pallas as pl
from jax.experimental.pallas import tpu as pltpu
from jax.sharding import Mesh
from jax.sharding import PartitionSpec as P


LAYERS = 8
LANES = 128
GROUP = ("group_0", "group_1", "group_2")
EVERY = ("group_0", "group_1", "group_2", "rep")
SENT = ((0, 384), (384, 640))
RAW = (4, 12)


step_rate = 0.5
f32 = jnp.float32
bf16 = jnp.bfloat16


def ring(count, step):
    return [(i, (i + step) % count) for i in range(count)]


def elements(*sizes):
    return tuple(pl.Element(size) for size in sizes)


def merge(who, parts, far_up, far_down, start, cols):
    _, blocks, rows, _ = parts.shape
    half = blocks // 2

    def body(who_ref, above, below, from_down, from_up, out_up, out_down):
        first = pl.program_id(0) == 0

        @pl.when(first)
        def _():
            out_up[...] = (above[0].astype(f32) + from_down[...].astype(f32)).astype(bf16)
            out_down[...] = below[0]

        @pl.when(jnp.logical_not(first))
        def _():
            out_up[...] = above[0]
            out_down[...] = (below[0].astype(f32) + from_up[...].astype(f32)).astype(bf16)

    piece = pl.BlockSpec((half, rows, cols), lambda i, w: (0, 0, 0))
    out = pl.BlockSpec((half, rows, cols), lambda i, w: (i, 0, 0))
    shape = jax.ShapeDtypeStruct((blocks, rows, cols), bf16)
    return pl.pallas_call(
        body,
        grid_spec=pltpu.PrefetchScalarGridSpec(
            num_scalar_prefetch=1,
            grid=(2,),
            in_specs=[
                pl.BlockSpec(elements(1, half, rows, cols), lambda i, w: (w[1], i * half, 0, start)),
                pl.BlockSpec(elements(1, half, rows, cols), lambda i, w: (w[3], i * half, 0, start)),
                piece,
                piece,
            ],
            out_specs=[out, out],
        ),
        out_shape=[shape, shape],
        name="merge",
    )(who, parts, parts, far_up, far_down)


def finish(who, table, parts, up, down, start, cols):
    _, blocks, rows, _ = parts.shape
    slots = table.shape[0]

    def body(who_ref, table_ref, own, one, two, gradient, slotted):
        total = own[0].astype(f32) + one[...].astype(f32) + two[...].astype(f32)
        gradient[...] = total.astype(bf16)
        for slot in range(slots):
            slotted[slot] = gradient[table_ref[slot]]

    block = pl.BlockSpec((blocks, rows, cols), lambda i, w, t: (0, 0, 0))
    return pl.pallas_call(
        body,
        grid_spec=pltpu.PrefetchScalarGridSpec(
            num_scalar_prefetch=2,
            grid=(1,),
            in_specs=[
                pl.BlockSpec(elements(1, blocks, rows, cols), lambda i, w, t: (w[0], 0, 0, start)),
                block,
                block,
            ],
            out_specs=[block, pl.BlockSpec((slots, rows, cols), lambda i, w, t: (0, 0, 0))],
        ),
        out_shape=[
            jax.ShapeDtypeStruct((blocks, rows, cols), bf16),
            jax.ShapeDtypeStruct((slots, rows, cols), bf16),
        ],
    )(who, table, parts, up, down)


def left_times(left, owned):
    order, cols = owned.shape
    tile = order // 2

    def body(left_ref, owned_ref, out):
        out[...] = jnp.dot(left_ref[...], owned_ref[...], preferred_element_type=f32).astype(bf16)

    return pl.pallas_call(
        body,
        grid=(2,),
        in_specs=[
            pl.BlockSpec((tile, order), lambda i: (i, 0)),
            pl.BlockSpec((order, cols), lambda i: (0, 0)),
        ],
        out_specs=pl.BlockSpec((tile, cols), lambda i: (i, 0)),
        out_shape=jax.ShapeDtypeStruct((order, cols), bf16),
        name="left_times",
    )(left, owned)


def products(left, right, owned, earlier, layer_row):
    order, cols = owned.shape
    steps = 2
    tile = order // steps
    last = SENT[-1][0]

    def body(left_ref, right_ref, owned_ref, layer_ref, *rest):
        before, (out, sums, mid) = rest[: len(earlier)], rest[len(earlier) :]
        mid[:, last : last + cols] = jnp.dot(
            left_ref[...], owned_ref[...], preferred_element_type=f32
        ).astype(bf16)
        for ref, (start, size) in zip(before, SENT):
            mid[:, start : start + size] = ref[...]
        out[...] = jnp.dot(mid[...], right_ref[...], preferred_element_type=f32).astype(bf16)
        wide = out[...].astype(f32)
        squares = jnp.sum(jnp.sum(wide * wide, axis=0, keepdims=True), axis=1, keepdims=True)

        @pl.when(pl.program_id(0) == 0)
        def _():
            sums[0:1] = jnp.zeros_like(squares * layer_ref[...])
            sums[1:2] = layer_ref[...] * squares

        @pl.when(pl.program_id(0) > 0)
        def _():
            sums[1:2] += layer_ref[...] * squares

    row = pl.BlockSpec((1, LANES), lambda i: (0, 0))
    return pl.pallas_call(
        body,
        grid=(steps,),
        in_specs=[
            pl.BlockSpec((tile, order), lambda i: (i, 0)),
            pl.BlockSpec((order, order), lambda i: (0, 0)),
            pl.BlockSpec((order, cols), lambda i: (0, 0)),
            row,
            *[pl.BlockSpec((tile, e.shape[1]), lambda i: (i, 0)) for e in earlier],
        ],
        out_specs=[pl.BlockSpec((tile, order), lambda i: (i, 0)), pl.BlockSpec((2, LANES), lambda i: (0, 0))],
        out_shape=[jax.ShapeDtypeStruct((order, order), bf16), jax.ShapeDtypeStruct((2, LANES), f32)],
        scratch_shapes=[pltpu.VMEM((tile, order), bf16)],
        name="products",
    )(left, right, owned, layer_row, *earlier)


def fetch(position_ref, returned_ref, target, sems, blocks):
    copies = []
    for block in blocks:
        copy = pltpu.make_async_copy(returned_ref.at[position_ref[block]], target(block), sems.at[block])
        copy.start()
        copies.append(copy)
    return copies


def pick(position, returned):
    _, rows, cols = returned.shape
    split, total = RAW[0], sum(RAW)

    def body(position_ref, returned_ref, low, high, sems):
        def target(block):
            return low.at[block] if block < split else high.at[block - split]

        for copy in fetch(position_ref, returned_ref, target, sems, range(total)):
            copy.wait()

    return pl.pallas_call(
        body,
        grid_spec=pltpu.PrefetchScalarGridSpec(
            num_scalar_prefetch=1,
            grid=(1,),
            in_specs=[pl.BlockSpec(memory_space=pltpu.HBM)],
            out_specs=[pl.BlockSpec((size, rows, cols), lambda i, p: (0, 0, 0)) for size in RAW],
            scratch_shapes=[pltpu.SemaphoreType.DMA((total,))],
        ),
        out_shape=[jax.ShapeDtypeStruct((size, rows, cols), bf16) for size in RAW],
        name="pick",
    )(position, returned)


def update(who, position, scale, returned, params, reps):
    blocks, rows, cols = params.shape
    first = sum(RAW)

    def body(who_ref, position_ref, scale_ref, returned_ref, params_ref, last, whole, picked, sems):
        copies = fetch(position_ref, returned_ref, lambda block: picked.at[block], sems, range(blocks))
        for block, copy in enumerate(copies):
            copy.wait()
            change = scale_ref[block] * picked[block].astype(f32)
            new = (params_ref[block].astype(f32) - change).astype(bf16)
            whole[0, block] = new
            if block >= first:
                last[block - first] = new

    return pl.pallas_call(
        body,
        grid_spec=pltpu.PrefetchScalarGridSpec(
            num_scalar_prefetch=3,
            grid=(1,),
            in_specs=[
                pl.BlockSpec(memory_space=pltpu.HBM),
                pl.BlockSpec((blocks, rows, cols), lambda i, w, p, s: (0, 0, 0)),
            ],
            out_specs=[
                pl.BlockSpec((blocks - first, rows, cols), lambda i, w, p, s: (0, 0, 0)),
                pl.BlockSpec((1, blocks, rows, cols), lambda i, w, p, s: (w[0], 0, 0, 0)),
            ],
            scratch_shapes=[pltpu.VMEM((blocks, rows, cols), bf16), pltpu.SemaphoreType.DMA((blocks,))],
        ),
        out_shape=[
            jax.ShapeDtypeStruct((blocks - first, rows, cols), bf16),
            jax.ShapeDtypeStruct((reps, blocks, rows, cols), bf16),
        ],
        name="update",
    )(who, position, scale, returned, params)


def everywhere(value):
    value = value + lax.ppermute(value, "group_2", [(0, 1), (1, 0)])
    for axis in ("rep", "group_0", "group_1"):
        one, two, three = [lax.ppermute(value, axis, ring(4, step)) for step in (1, 2, 3)]
        value = (value + two) + (one + three)
    return value


def spread(low, high, reps):
    up, down = ring(reps, 1), ring(reps, -1)
    high_up = lax.ppermute(high, "rep", up)
    high_down = lax.ppermute(high, "rep", down)
    low_up = lax.ppermute(low, "rep", up)
    low_down = lax.ppermute(low, "rep", down)
    far_high = lax.ppermute(high_down, "rep", down)
    far_low = lax.ppermute(low_up, "rep", up)
    return (
        (3, 1, high_up),
        (1, 1, high_down),
        (3, 0, low_up),
        (1, 0, low_down),
        (2, 0, far_low),
        (2, 1, far_high),
    )


def local(grad_parts, params, accum, left_pre, right_pre, slot_block, layer_of):
    group_size = lax.axis_size(GROUP)
    reps = lax.axis_size("rep")
    me = lax.axis_index("rep")
    group_index = lax.axis_index(GROUP)
    blocks, rows, width = params.shape
    half = blocks // 2
    up, down = ring(reps, 1), ring(reps, -1)
    parts = grad_parts[0].reshape(reps, blocks, rows, width)
    who = lax.rem(me + jnp.arange(reps, dtype=jnp.int32), reps)
    table = lax.dynamic_index_in_dim(slot_block, me, 0, keepdims=False).reshape(-1)
    wanted = jnp.maximum(table, 0)
    left, right = left_pre[0, 0, 0], right_pre[0, 0, 0]

    far = lax.rem(me + 2, reps)
    gradients, earlier, owned = [None] * len(SENT), [], None
    for chunk, (start, cols) in enumerate(SENT):
        low = lax.dynamic_slice(parts, (far, 0, 0, start), (1, half, rows, cols))[0]
        high = lax.dynamic_slice(parts, (far, half, 0, start), (1, half, rows, cols))[0]
        far_up = lax.ppermute(low, "rep", up)
        far_down = lax.ppermute(high, "rep", down)
        to_up, to_down = merge(who, parts, far_up, far_down, start, cols)
        near_up = lax.ppermute(to_up, "rep", up)
        near_down = lax.ppermute(to_down, "rep", down)
        gradient, outgoing = finish(who, wanted, parts, near_up, near_down, start, cols)
        gradients[chunk] = gradient
        arrived = lax.all_to_all(outgoing, GROUP, split_axis=0, concat_axis=0, tiled=True)
        if chunk > 0:
            earlier.append(left_times(left, owned))
        owned = arrived.reshape(group_size * rows, cols)

    old_low, old_high = params[: RAW[0]], params[RAW[0] : sum(RAW)]
    ahead = spread(old_low, old_high, reps)

    onehots = (layer_of[:, None] == jnp.arange(LAYERS, dtype=jnp.int32)[None, :]).astype(f32)
    onehot = lax.dynamic_slice_in_dim(onehots, me * blocks, blocks)
    mine = lax.dynamic_index_in_dim(table, group_index, 0, keepdims=False)
    chosen = (jnp.arange(blocks, dtype=jnp.int32) == mine).astype(f32)
    my_layer = jnp.sum(chosen[:, None] * onehot, axis=0)
    layer_row = jnp.pad(my_layer[None, :], ((0, 0), (0, LANES - LAYERS)))
    position = jnp.sum(
        jnp.where(
            table[None, :] == jnp.arange(blocks, dtype=jnp.int32)[:, None],
            jnp.arange(group_size, dtype=jnp.int32)[None, :],
            0,
        ),
        axis=1,
    )

    owned, earlier, layer_row, onehot, gradients = lax.optimization_barrier(
        (owned, earlier, layer_row, onehot, gradients)
    )

    wide = jnp.concatenate(gradients, axis=2).astype(f32)
    new_accum = accum + wide * wide
    graft = wide * lax.rsqrt(new_accum)
    graft_blocks = jnp.sum(graft * graft, axis=(1, 2))
    graft_layer = jnp.sum(onehot * graft_blocks[:, None], axis=0)
    graft_row = jnp.pad(graft_layer[None, :], ((0, 1), (0, LANES - LAYERS)))
    precond, sums = products(left, right, owned, earlier, layer_row)
    outgoing = precond.reshape(group_size, rows, width)
    returned = lax.all_to_all(outgoing, GROUP, split_axis=0, concat_axis=0, tiled=True)
    sums = everywhere(sums + graft_row)
    layer_scale = jnp.sqrt(sums[0, :LAYERS]) * lax.rsqrt(sums[1, :LAYERS] + 1e-06)
    scales = (step_rate * jnp.sum(onehots * layer_scale[None, :], axis=1)).reshape(reps, blocks)

    def owner(offset):
        return lax.rem(me + offset, reps)

    changes = spread(*pick(position, returned), reps)
    last, new_params = update(who, position, scales[me], returned, params, reps)
    from_down = lax.ppermute(last, "rep", up)
    from_up = lax.ppermute(last, "rep", down)
    onward = lax.ppermute(from_down, "rep", up)

    def place(whole, offset, first, piece):
        return lax.dynamic_update_slice(whole, piece[None], (owner(offset), first, 0, 0))

    pairs = list(zip(ahead, changes))
    for group, name in ((pairs[:4], "place_near"), (pairs[4:], "place_far")):
        for (offset, part, old), (_, _, change) in group:
            first = RAW[0] * part
            scale = lax.dynamic_slice(scales, (owner(offset), first), (1, RAW[part]))[0, :, None, None]
            new = (old.astype(f32) - scale * change.astype(f32)).astype(bf16)
            new_params = place(new_params, offset, first, new)
        if name == "place_near":
            new_params = place(new_params, 3, sum(RAW), from_down)
            new_params = place(new_params, 1, sum(RAW), from_up)
    new_params = place(new_params, 2, sum(RAW), onward)
    return (new_params.reshape(reps * blocks, rows, width), new_accum)


def solution(mesh):
    split = Mesh(mesh.devices.reshape(4, 4, 2, mesh.shape["rep"]), EVERY)
    placed = (
        P("rep", None, GROUP, None),
        P("rep", GROUP, None),
        P("rep", GROUP, None),
        P("rep", GROUP, None, None, None),
        P("rep", GROUP, None, None, None),
        P(),
        P(),
    )
    return jax.shard_map(
        local,
        mesh=split,
        in_specs=placed,
        out_specs=(P(None, GROUP, None), P("rep", GROUP, None)),
        check_vma=False,
    )
```

```python
import jax
import jax.numpy as jnp
from jax import lax
from jax.experimental import pallas as pl
from jax.experimental.pallas import tpu as pltpu
from jax.sharding import Mesh
from jax.sharding import PartitionSpec as P


LAYERS = 8
LANES = 128
GROUP = ("group_0", "group_1", "group_2")
EVERY = ("group_0", "group_1", "group_2", "rep")
SENT = ((0, 384), (384, 640))
RAW = 512


step_rate = 0.5
f32 = jnp.float32
bf16 = jnp.bfloat16


def ring(count, step):
    return [(i, (i + step) % count) for i in range(count)]


def elements(*sizes):
    return tuple(pl.Element(size) for size in sizes)


def merge(who, parts, far_up, far_down, start, cols):
    _, blocks, rows, _ = parts.shape
    half = blocks // 2

    def body(who_ref, above, below, from_down, from_up, out_up, out_down):
        first = pl.program_id(0) == 0

        @pl.when(first)
        def _():
            out_up[...] = (above[0].astype(f32) + from_down[...].astype(f32)).astype(bf16)
            out_down[...] = below[0]

        @pl.when(jnp.logical_not(first))
        def _():
            out_up[...] = above[0]
            out_down[...] = (below[0].astype(f32) + from_up[...].astype(f32)).astype(bf16)

    piece = pl.BlockSpec((half, rows, cols), lambda i, w: (0, 0, 0))
    out = pl.BlockSpec((half, rows, cols), lambda i, w: (i, 0, 0))
    shape = jax.ShapeDtypeStruct((blocks, rows, cols), bf16)
    return pl.pallas_call(
        body,
        grid_spec=pltpu.PrefetchScalarGridSpec(
            num_scalar_prefetch=1,
            grid=(2,),
            in_specs=[
                pl.BlockSpec(elements(1, half, rows, cols), lambda i, w: (w[1], i * half, 0, start)),
                pl.BlockSpec(elements(1, half, rows, cols), lambda i, w: (w[3], i * half, 0, start)),
                piece,
                piece,
            ],
            out_specs=[out, out],
        ),
        out_shape=[shape, shape],
        name="merge",
    )(who, parts, parts, far_up, far_down)


def finish(who, table, parts, up, down, start, cols):
    _, blocks, rows, _ = parts.shape
    slots = table.shape[0]

    def body(who_ref, table_ref, own, one, two, gradient, slotted):
        total = own[0].astype(f32) + one[...].astype(f32) + two[...].astype(f32)
        gradient[...] = total.astype(bf16)
        for slot in range(slots):
            slotted[slot] = gradient[table_ref[slot]]

    block = pl.BlockSpec((blocks, rows, cols), lambda i, w, t: (0, 0, 0))
    return pl.pallas_call(
        body,
        grid_spec=pltpu.PrefetchScalarGridSpec(
            num_scalar_prefetch=2,
            grid=(1,),
            in_specs=[
                pl.BlockSpec(elements(1, blocks, rows, cols), lambda i, w, t: (w[0], 0, 0, start)),
                block,
                block,
            ],
            out_specs=[block, pl.BlockSpec((slots, rows, cols), lambda i, w, t: (0, 0, 0))],
        ),
        out_shape=[
            jax.ShapeDtypeStruct((blocks, rows, cols), bf16),
            jax.ShapeDtypeStruct((slots, rows, cols), bf16),
        ],
    )(who, table, parts, up, down)


def left_times(left, owned):
    order, cols = owned.shape
    tile = order // 2

    def body(left_ref, owned_ref, out):
        out[...] = jnp.dot(left_ref[...], owned_ref[...], preferred_element_type=f32).astype(bf16)

    return pl.pallas_call(
        body,
        grid=(2,),
        in_specs=[
            pl.BlockSpec((tile, order), lambda i: (i, 0)),
            pl.BlockSpec((order, cols), lambda i: (0, 0)),
        ],
        out_specs=pl.BlockSpec((tile, cols), lambda i: (i, 0)),
        out_shape=jax.ShapeDtypeStruct((order, cols), bf16),
        name="left_times",
    )(left, owned)


def products(left, right, owned, earlier, layer_row):
    order, cols = owned.shape
    steps = 2
    tile = order // steps
    last = SENT[-1][0]

    def body(left_ref, right_ref, owned_ref, layer_ref, *rest):
        before, (first, second, sums, mid) = rest[: len(earlier)], rest[len(earlier) :]
        mid[:, last : last + cols] = jnp.dot(
            left_ref[...], owned_ref[...], preferred_element_type=f32
        ).astype(bf16)
        for ref, (start, size) in zip(before, SENT):
            mid[:, start : start + size] = ref[...]
        product = jnp.dot(mid[...], right_ref[...], preferred_element_type=f32).astype(bf16)
        first[...] = product[:, :RAW]
        second[...] = product[:, RAW:]
        wide = product.astype(f32)
        squares = jnp.sum(jnp.sum(wide * wide, axis=0, keepdims=True), axis=1, keepdims=True)

        @pl.when(pl.program_id(0) == 0)
        def _():
            sums[0:1] = jnp.zeros_like(squares * layer_ref[...])
            sums[1:2] = layer_ref[...] * squares

        @pl.when(pl.program_id(0) > 0)
        def _():
            sums[1:2] += layer_ref[...] * squares

    row = pl.BlockSpec((1, LANES), lambda i: (0, 0))
    return pl.pallas_call(
        body,
        grid=(steps,),
        in_specs=[
            pl.BlockSpec((tile, order), lambda i: (i, 0)),
            pl.BlockSpec((order, order), lambda i: (0, 0)),
            pl.BlockSpec((order, cols), lambda i: (0, 0)),
            row,
            *[pl.BlockSpec((tile, e.shape[1]), lambda i: (i, 0)) for e in earlier],
        ],
        out_specs=[
            pl.BlockSpec((tile, RAW), lambda i: (i, 0)),
            pl.BlockSpec((tile, order - RAW), lambda i: (i, 0)),
            pl.BlockSpec((2, LANES), lambda i: (0, 0)),
        ],
        out_shape=[
            jax.ShapeDtypeStruct((order, RAW), bf16),
            jax.ShapeDtypeStruct((order, order - RAW), bf16),
            jax.ShapeDtypeStruct((2, LANES), f32),
        ],
        scratch_shapes=[pltpu.VMEM((tile, order), bf16)],
        name="products",
    )(left, right, owned, layer_row, *earlier)


def pick(position, returned):
    blocks = position.shape[0]
    half = blocks // 2
    _, rows, cols = returned.shape

    def body(position_ref, returned_ref, low, high, sems):
        copies = []
        for block in range(blocks):
            out = low.at[block] if block < half else high.at[block - half]
            copies.append(pltpu.make_async_copy(returned_ref.at[position_ref[block]], out, sems.at[block]))
            copies[-1].start()
        for copy in copies:
            copy.wait()

    piece = pl.BlockSpec((half, rows, cols), lambda i, p: (0, 0, 0))
    shape = jax.ShapeDtypeStruct((half, rows, cols), bf16)
    return pl.pallas_call(
        body,
        grid_spec=pltpu.PrefetchScalarGridSpec(
            num_scalar_prefetch=1,
            grid=(1,),
            in_specs=[pl.BlockSpec(memory_space=pltpu.HBM)],
            out_specs=[piece, piece],
            scratch_shapes=[pltpu.SemaphoreType.DMA((blocks,))],
        ),
        out_shape=[shape, shape],
        name="pick",
    )(position, returned)


def update(who, position, scale, returned, params, reps):
    blocks, rows, width = params.shape
    half = blocks // 2

    def body(who_ref, position_ref, scale_ref, one, two, params_ref, low, high, whole, picked, sems):
        copies = []
        for block in range(blocks):
            slot = position_ref[block]
            pair = (
                pltpu.make_async_copy(one.at[slot], picked.at[block, :, pl.ds(0, RAW)], sems.at[0, block]),
                pltpu.make_async_copy(
                    two.at[slot], picked.at[block, :, pl.ds(RAW, width - RAW)], sems.at[1, block]
                ),
            )
            for copy in pair:
                copy.start()
            copies.append(pair)
        for block, pair in enumerate(copies):
            for copy in pair:
                copy.wait()
            change = scale_ref[block] * picked[block].astype(f32)
            new = (params_ref[block].astype(f32) - change).astype(bf16)
            whole[0, block] = new
            if block < half:
                low[block] = new[:, RAW:]
            else:
                high[block - half] = new[:, RAW:]

    hbm = pl.BlockSpec(memory_space=pltpu.HBM)
    piece = pl.BlockSpec((half, rows, width - RAW), lambda i, w, p, s: (0, 0, 0))
    shape = jax.ShapeDtypeStruct((half, rows, width - RAW), bf16)
    return pl.pallas_call(
        body,
        grid_spec=pltpu.PrefetchScalarGridSpec(
            num_scalar_prefetch=3,
            grid=(1,),
            in_specs=[hbm, hbm, pl.BlockSpec((blocks, rows, width), lambda i, w, p, s: (0, 0, 0))],
            out_specs=[
                piece,
                piece,
                pl.BlockSpec((1, blocks, rows, width), lambda i, w, p, s: (w[0], 0, 0, 0)),
            ],
            scratch_shapes=[
                pltpu.VMEM((blocks, rows, width), bf16),
                pltpu.SemaphoreType.DMA((2, blocks)),
            ],
        ),
        out_shape=[shape, shape, jax.ShapeDtypeStruct((reps, blocks, rows, width), bf16)],
        name="update",
    )(who, position, scale, *returned, params)


def everywhere(value):
    value = value + lax.ppermute(value, "group_2", [(0, 1), (1, 0)])
    for axis in ("rep", "group_0", "group_1"):
        one, two, three = [lax.ppermute(value, axis, ring(4, step)) for step in (1, 2, 3)]
        value = (value + two) + (one + three)
    return value


def spread(low, high, reps):
    up, down = ring(reps, 1), ring(reps, -1)
    low_up = lax.ppermute(low, "rep", up)
    high_down = lax.ppermute(high, "rep", down)
    high_up = lax.ppermute(high, "rep", up)
    low_down = lax.ppermute(low, "rep", down)
    far_low = lax.ppermute(low_up, "rep", up)
    far_high = lax.ppermute(high_down, "rep", down)
    return (
        (3, 0, low_up),
        (1, 1, high_down),
        (3, 1, high_up),
        (1, 0, low_down),
        (2, 0, far_low),
        (2, 1, far_high),
    )


def local(grad_parts, params, accum, left_pre, right_pre, slot_block, layer_of):
    group_size = lax.axis_size(GROUP)
    reps = lax.axis_size("rep")
    me = lax.axis_index("rep")
    group_index = lax.axis_index(GROUP)
    blocks, rows, width = params.shape
    half = blocks // 2
    up, down = ring(reps, 1), ring(reps, -1)
    parts = grad_parts[0].reshape(reps, blocks, rows, width)
    who = lax.rem(me + jnp.arange(reps, dtype=jnp.int32), reps)
    table = lax.dynamic_index_in_dim(slot_block, me, 0, keepdims=False).reshape(-1)
    wanted = jnp.maximum(table, 0)
    left, right = left_pre[0, 0, 0], right_pre[0, 0, 0]

    far = lax.rem(me + 2, reps)
    gradients, earlier, owned = [None] * len(SENT), [], None
    for chunk, (start, cols) in enumerate(SENT):
        low = lax.dynamic_slice(parts, (far, 0, 0, start), (1, half, rows, cols))[0]
        high = lax.dynamic_slice(parts, (far, half, 0, start), (1, half, rows, cols))[0]
        far_up = lax.ppermute(low, "rep", up)
        far_down = lax.ppermute(high, "rep", down)
        to_up, to_down = merge(who, parts, far_up, far_down, start, cols)
        near_up = lax.ppermute(to_up, "rep", up)
        near_down = lax.ppermute(to_down, "rep", down)
        gradient, outgoing = finish(who, wanted, parts, near_up, near_down, start, cols)
        gradients[chunk] = gradient
        arrived = lax.all_to_all(outgoing, GROUP, split_axis=0, concat_axis=0, tiled=True)
        if chunk > 0:
            earlier.append(left_times(left, owned))
        owned = arrived.reshape(group_size * rows, cols)

    old_low, old_high = params[:half, :, :RAW], params[half:, :, :RAW]
    ahead = spread(old_low, old_high, reps)

    onehots = (layer_of[:, None] == jnp.arange(LAYERS, dtype=jnp.int32)[None, :]).astype(f32)
    onehot = lax.dynamic_slice_in_dim(onehots, me * blocks, blocks)
    mine = lax.dynamic_index_in_dim(table, group_index, 0, keepdims=False)
    chosen = (jnp.arange(blocks, dtype=jnp.int32) == mine).astype(f32)
    my_layer = jnp.sum(chosen[:, None] * onehot, axis=0)
    layer_row = jnp.pad(my_layer[None, :], ((0, 0), (0, LANES - LAYERS)))
    position = jnp.sum(
        jnp.where(
            table[None, :] == jnp.arange(blocks, dtype=jnp.int32)[:, None],
            jnp.arange(group_size, dtype=jnp.int32)[None, :],
            0,
        ),
        axis=1,
    )

    owned, earlier, layer_row, onehot, gradients = lax.optimization_barrier(
        (owned, earlier, layer_row, onehot, gradients)
    )

    wide = jnp.concatenate(gradients, axis=2).astype(f32)
    new_accum = accum + wide * wide
    graft = wide * lax.rsqrt(new_accum)
    graft_blocks = jnp.sum(graft * graft, axis=(1, 2))
    graft_layer = jnp.sum(onehot * graft_blocks[:, None], axis=0)
    graft_row = jnp.pad(graft_layer[None, :], ((0, 1), (0, LANES - LAYERS)))
    *preconds, sums = products(left, right, owned, earlier, layer_row)
    returned = []
    for precond in preconds:
        outgoing = precond.reshape(group_size, rows, precond.shape[1])
        returned.append(lax.all_to_all(outgoing, GROUP, split_axis=0, concat_axis=0, tiled=True))
    sums = everywhere(sums + graft_row)
    layer_scale = jnp.sqrt(sums[0, :LAYERS]) * lax.rsqrt(sums[1, :LAYERS] + 1e-06)
    scales = (step_rate * jnp.sum(onehots * layer_scale[None, :], axis=1)).reshape(reps, blocks)

    changes = spread(*pick(position, returned[0]), reps)
    low, high, new_params = update(who, position, scales[me], returned, params, reps)
    finished = spread(low, high, reps)

    for (offset, part, old), (_, _, change) in zip(ahead, changes):
        owner = lax.rem(me + offset, reps)
        scale = lax.dynamic_slice(scales, (owner, part * half), (1, half))[0, :, None, None]
        new = (old.astype(f32) - scale * change.astype(f32)).astype(bf16)
        new_params = lax.dynamic_update_slice(new_params, new[None], (owner, part * half, 0, 0))
    for offset, part, piece in finished:
        owner = lax.rem(me + offset, reps)
        new_params = lax.dynamic_update_slice(new_params, piece[None], (owner, part * half, 0, RAW))
    return (new_params.reshape(reps * blocks, rows, width), new_accum)


def solution(mesh):
    split = Mesh(mesh.devices.reshape(4, 4, 2, mesh.shape["rep"]), EVERY)
    placed = (
        P("rep", None, GROUP, None),
        P("rep", GROUP, None),
        P("rep", GROUP, None),
        P("rep", GROUP, None, None, None),
        P("rep", GROUP, None, None, None),
        P(),
        P(),
    )
    return jax.shard_map(
        local,
        mesh=split,
        in_specs=placed,
        out_specs=(P(None, GROUP, None), P("rep", GROUP, None)),
        check_vma=False,
    )
```

```python
import jax
import jax.numpy as jnp
from jax import lax
from jax.experimental import pallas as pl
from jax.experimental.pallas import tpu as pltpu
from jax.sharding import Mesh
from jax.sharding import PartitionSpec as P


LAYERS = 8
LANES = 128
GROUP = ("group_0", "group_1", "group_2")
EVERY = ("group_0", "group_1", "group_2", "rep")
SENT = ((0, 384), (384, 640))
RAW = 512


step_rate = 0.5
f32 = jnp.float32
bf16 = jnp.bfloat16


def ring(count, step):
    return [(i, (i + step) % count) for i in range(count)]


def elements(*sizes):
    return tuple(pl.Element(size) for size in sizes)


def merge(who, parts, far_up, far_down, start, cols):
    _, blocks, rows, _ = parts.shape
    half = blocks // 2

    def body(who_ref, above, below, from_down, from_up, out_up, out_down):
        first = pl.program_id(0) == 0

        @pl.when(first)
        def _():
            out_up[...] = (above[0].astype(f32) + from_down[...].astype(f32)).astype(bf16)
            out_down[...] = below[0]

        @pl.when(jnp.logical_not(first))
        def _():
            out_up[...] = above[0]
            out_down[...] = (below[0].astype(f32) + from_up[...].astype(f32)).astype(bf16)

    piece = pl.BlockSpec((half, rows, cols), lambda i, w: (0, 0, 0))
    out = pl.BlockSpec((half, rows, cols), lambda i, w: (i, 0, 0))
    shape = jax.ShapeDtypeStruct((blocks, rows, cols), bf16)
    return pl.pallas_call(
        body,
        grid_spec=pltpu.PrefetchScalarGridSpec(
            num_scalar_prefetch=1,
            grid=(2,),
            in_specs=[
                pl.BlockSpec(elements(1, half, rows, cols), lambda i, w: (w[1], i * half, 0, start)),
                pl.BlockSpec(elements(1, half, rows, cols), lambda i, w: (w[3], i * half, 0, start)),
                piece,
                piece,
            ],
            out_specs=[out, out],
        ),
        out_shape=[shape, shape],
        name="merge",
    )(who, parts, parts, far_up, far_down)


def finish(who, table, parts, up, down, start, cols):
    _, blocks, rows, _ = parts.shape
    slots = table.shape[0]

    def body(who_ref, table_ref, own, one, two, gradient, slotted):
        total = own[0].astype(f32) + one[...].astype(f32) + two[...].astype(f32)
        gradient[...] = total.astype(bf16)
        for slot in range(slots):
            slotted[slot] = gradient[table_ref[slot]]

    block = pl.BlockSpec((blocks, rows, cols), lambda i, w, t: (0, 0, 0))
    return pl.pallas_call(
        body,
        grid_spec=pltpu.PrefetchScalarGridSpec(
            num_scalar_prefetch=2,
            grid=(1,),
            in_specs=[
                pl.BlockSpec(elements(1, blocks, rows, cols), lambda i, w, t: (w[0], 0, 0, start)),
                block,
                block,
            ],
            out_specs=[block, pl.BlockSpec((slots, rows, cols), lambda i, w, t: (0, 0, 0))],
        ),
        out_shape=[
            jax.ShapeDtypeStruct((blocks, rows, cols), bf16),
            jax.ShapeDtypeStruct((slots, rows, cols), bf16),
        ],
    )(who, table, parts, up, down)


def left_times(left, owned):
    order, cols = owned.shape
    tile = order // 2

    def body(left_ref, owned_ref, out):
        out[...] = jnp.dot(left_ref[...], owned_ref[...], preferred_element_type=f32).astype(bf16)

    return pl.pallas_call(
        body,
        grid=(2,),
        in_specs=[
            pl.BlockSpec((tile, order), lambda i: (i, 0)),
            pl.BlockSpec((order, cols), lambda i: (0, 0)),
        ],
        out_specs=pl.BlockSpec((tile, cols), lambda i: (i, 0)),
        out_shape=jax.ShapeDtypeStruct((order, cols), bf16),
        name="left_times",
    )(left, owned)


def products(left, right, owned, earlier, layer_row):
    order, cols = owned.shape
    steps = 2
    tile = order // steps
    last = SENT[-1][0]

    def body(left_ref, right_ref, owned_ref, layer_ref, *rest):
        before, (first, second, sums, mid) = rest[: len(earlier)], rest[len(earlier) :]
        mid[:, last : last + cols] = jnp.dot(
            left_ref[...], owned_ref[...], preferred_element_type=f32
        ).astype(bf16)
        for ref, (start, size) in zip(before, SENT):
            mid[:, start : start + size] = ref[...]
        product = jnp.dot(mid[...], right_ref[...], preferred_element_type=f32).astype(bf16)
        first[...] = product[:, :RAW]
        second[...] = product[:, RAW:]
        wide = product.astype(f32)
        squares = jnp.sum(jnp.sum(wide * wide, axis=0, keepdims=True), axis=1, keepdims=True)

        @pl.when(pl.program_id(0) == 0)
        def _():
            sums[0:1] = jnp.zeros_like(squares * layer_ref[...])
            sums[1:2] = layer_ref[...] * squares

        @pl.when(pl.program_id(0) > 0)
        def _():
            sums[1:2] += layer_ref[...] * squares

    row = pl.BlockSpec((1, LANES), lambda i: (0, 0))
    return pl.pallas_call(
        body,
        grid=(steps,),
        in_specs=[
            pl.BlockSpec((tile, order), lambda i: (i, 0)),
            pl.BlockSpec((order, order), lambda i: (0, 0)),
            pl.BlockSpec((order, cols), lambda i: (0, 0)),
            row,
            *[pl.BlockSpec((tile, e.shape[1]), lambda i: (i, 0)) for e in earlier],
        ],
        out_specs=[
            pl.BlockSpec((tile, RAW), lambda i: (i, 0)),
            pl.BlockSpec((tile, order - RAW), lambda i: (i, 0)),
            pl.BlockSpec((2, LANES), lambda i: (0, 0)),
        ],
        out_shape=[
            jax.ShapeDtypeStruct((order, RAW), bf16),
            jax.ShapeDtypeStruct((order, order - RAW), bf16),
            jax.ShapeDtypeStruct((2, LANES), f32),
        ],
        scratch_shapes=[pltpu.VMEM((tile, order), bf16)],
        name="products",
    )(left, right, owned, layer_row, *earlier)


def pick(position, returned):
    blocks = position.shape[0]
    half = blocks // 2
    _, rows, cols = returned.shape

    def body(position_ref, returned_ref, low, high, sems):
        copies = []
        for block in range(blocks):
            out = low.at[block] if block < half else high.at[block - half]
            copies.append(pltpu.make_async_copy(returned_ref.at[position_ref[block]], out, sems.at[block]))
            copies[-1].start()
        for copy in copies:
            copy.wait()

    piece = pl.BlockSpec((half, rows, cols), lambda i, p: (0, 0, 0))
    shape = jax.ShapeDtypeStruct((half, rows, cols), bf16)
    return pl.pallas_call(
        body,
        grid_spec=pltpu.PrefetchScalarGridSpec(
            num_scalar_prefetch=1,
            grid=(1,),
            in_specs=[pl.BlockSpec(memory_space=pltpu.HBM)],
            out_specs=[piece, piece],
            scratch_shapes=[pltpu.SemaphoreType.DMA((blocks,))],
        ),
        out_shape=[shape, shape],
        name="pick",
    )(position, returned)


def update(who, position, scale, returned, params, reps):
    blocks, rows, width = params.shape
    half = blocks // 2

    def body(who_ref, position_ref, scale_ref, one, two, params_ref, low, high, whole, picked, sems):
        copies = []
        for block in range(blocks):
            slot = position_ref[block]
            pair = (
                pltpu.make_async_copy(one.at[slot], picked.at[block, :, pl.ds(0, RAW)], sems.at[0, block]),
                pltpu.make_async_copy(
                    two.at[slot], picked.at[block, :, pl.ds(RAW, width - RAW)], sems.at[1, block]
                ),
            )
            for copy in pair:
                copy.start()
            copies.append(pair)
        for block, pair in enumerate(copies):
            for copy in pair:
                copy.wait()
            change = scale_ref[block] * picked[block].astype(f32)
            new = (params_ref[block].astype(f32) - change).astype(bf16)
            whole[0, block] = new
            if block < half:
                low[block] = new[:, RAW:]
            else:
                high[block - half] = new[:, RAW:]

    hbm = pl.BlockSpec(memory_space=pltpu.HBM)
    piece = pl.BlockSpec((half, rows, width - RAW), lambda i, w, p, s: (0, 0, 0))
    shape = jax.ShapeDtypeStruct((half, rows, width - RAW), bf16)
    return pl.pallas_call(
        body,
        grid_spec=pltpu.PrefetchScalarGridSpec(
            num_scalar_prefetch=3,
            grid=(1,),
            in_specs=[hbm, hbm, pl.BlockSpec((blocks, rows, width), lambda i, w, p, s: (0, 0, 0))],
            out_specs=[
                piece,
                piece,
                pl.BlockSpec((1, blocks, rows, width), lambda i, w, p, s: (w[0], 0, 0, 0)),
            ],
            scratch_shapes=[
                pltpu.VMEM((blocks, rows, width), bf16),
                pltpu.SemaphoreType.DMA((2, blocks)),
            ],
        ),
        out_shape=[shape, shape, jax.ShapeDtypeStruct((reps, blocks, rows, width), bf16)],
        name="update",
    )(who, position, scale, *returned, params)


def place(owners, scales, whole, raw, ready):
    half, rows, _ = raw[0][2].shape
    blocks = 2 * half
    pieces = len(raw) + len(ready)

    def body(owners_ref, scales_ref, *refs):
        olds, changes = refs[: len(raw)], refs[len(raw) : 2 * len(raw)]
        values = refs[2 * len(raw) : 2 * len(raw) + len(ready)]
        out, made, sems = refs[-3:]
        copies = []
        for at, (offset, part, value) in enumerate([(o, p, None) for o, p, _, _ in raw] + list(ready)):
            owner = owners_ref[offset]
            if at < len(raw):
                for block in range(half):
                    scale = scales_ref[owner * blocks + part * half + block]
                    new = olds[at][block].astype(f32) - scale * changes[at][block].astype(f32)
                    made[at, block] = new.astype(bf16)
                source, columns = made.at[at], pl.ds(0, RAW)
            else:
                source = values[at - len(raw)]
                columns = pl.ds(RAW, value.shape[2])
            target = out.at[owner, pl.ds(part * half, half), :, columns]
            copies.append(pltpu.make_async_copy(source, target, sems.at[at]))
            copies[-1].start()
        for copy in copies:
            copy.wait()

    def block_of(array):
        return pl.BlockSpec(array.shape, lambda i, o, s: (0, 0, 0))

    arrays = [old for _, _, old, _ in raw] + [change for _, _, _, change in raw] + [v for _, _, v in ready]
    hbm = pl.BlockSpec(memory_space=pltpu.HBM)
    return pl.pallas_call(
        body,
        grid_spec=pltpu.PrefetchScalarGridSpec(
            num_scalar_prefetch=2,
            grid=(1,),
            in_specs=[*[block_of(array) for array in arrays], hbm],
            out_specs=hbm,
            scratch_shapes=[
                pltpu.VMEM((len(raw), half, rows, RAW), bf16),
                pltpu.SemaphoreType.DMA((pieces,)),
            ],
        ),
        out_shape=jax.ShapeDtypeStruct(whole.shape, bf16),
        input_output_aliases={2 + len(arrays): 0},
    )(owners, scales, *arrays, whole)


def everywhere(value):
    value = value + lax.ppermute(value, "group_2", [(0, 1), (1, 0)])
    for axis in ("rep", "group_0", "group_1"):
        one, two, three = [lax.ppermute(value, axis, ring(4, step)) for step in (1, 2, 3)]
        value = (value + two) + (one + three)
    return value


def spread(low, high, reps):
    up, down = ring(reps, 1), ring(reps, -1)
    low_up = lax.ppermute(low, "rep", up)
    high_down = lax.ppermute(high, "rep", down)
    high_up = lax.ppermute(high, "rep", up)
    low_down = lax.ppermute(low, "rep", down)
    far_low = lax.ppermute(low_up, "rep", up)
    far_high = lax.ppermute(high_down, "rep", down)
    return (
        (3, 0, low_up),
        (1, 1, high_down),
        (3, 1, high_up),
        (1, 0, low_down),
        (2, 0, far_low),
        (2, 1, far_high),
    )


def local(grad_parts, params, accum, left_pre, right_pre, slot_block, layer_of):
    group_size = lax.axis_size(GROUP)
    reps = lax.axis_size("rep")
    me = lax.axis_index("rep")
    group_index = lax.axis_index(GROUP)
    blocks, rows, width = params.shape
    half = blocks // 2
    up, down = ring(reps, 1), ring(reps, -1)
    parts = grad_parts[0].reshape(reps, blocks, rows, width)
    who = lax.rem(me + jnp.arange(reps, dtype=jnp.int32), reps)
    table = lax.dynamic_index_in_dim(slot_block, me, 0, keepdims=False).reshape(-1)
    wanted = jnp.maximum(table, 0)
    left, right = left_pre[0, 0, 0], right_pre[0, 0, 0]

    far = lax.rem(me + 2, reps)
    gradients, earlier, owned = [None] * len(SENT), [], None
    for chunk, (start, cols) in enumerate(SENT):
        low = lax.dynamic_slice(parts, (far, 0, 0, start), (1, half, rows, cols))[0]
        high = lax.dynamic_slice(parts, (far, half, 0, start), (1, half, rows, cols))[0]
        far_up = lax.ppermute(low, "rep", up)
        far_down = lax.ppermute(high, "rep", down)
        to_up, to_down = merge(who, parts, far_up, far_down, start, cols)
        near_up = lax.ppermute(to_up, "rep", up)
        near_down = lax.ppermute(to_down, "rep", down)
        gradient, outgoing = finish(who, wanted, parts, near_up, near_down, start, cols)
        gradients[chunk] = gradient
        arrived = lax.all_to_all(outgoing, GROUP, split_axis=0, concat_axis=0, tiled=True)
        if chunk > 0:
            earlier.append(left_times(left, owned))
        owned = arrived.reshape(group_size * rows, cols)

    old_low, old_high = params[:half, :, :RAW], params[half:, :, :RAW]
    ahead = spread(old_low, old_high, reps)

    onehots = (layer_of[:, None] == jnp.arange(LAYERS, dtype=jnp.int32)[None, :]).astype(f32)
    onehot = lax.dynamic_slice_in_dim(onehots, me * blocks, blocks)
    mine = lax.dynamic_index_in_dim(table, group_index, 0, keepdims=False)
    chosen = (jnp.arange(blocks, dtype=jnp.int32) == mine).astype(f32)
    my_layer = jnp.sum(chosen[:, None] * onehot, axis=0)
    layer_row = jnp.pad(my_layer[None, :], ((0, 0), (0, LANES - LAYERS)))
    position = jnp.sum(
        jnp.where(
            table[None, :] == jnp.arange(blocks, dtype=jnp.int32)[:, None],
            jnp.arange(group_size, dtype=jnp.int32)[None, :],
            0,
        ),
        axis=1,
    )

    owned, earlier, layer_row, onehot, gradients = lax.optimization_barrier(
        (owned, earlier, layer_row, onehot, gradients)
    )

    wide = jnp.concatenate(gradients, axis=2).astype(f32)
    new_accum = accum + wide * wide
    graft = wide * lax.rsqrt(new_accum)
    graft_blocks = jnp.sum(graft * graft, axis=(1, 2))
    graft_layer = jnp.sum(onehot * graft_blocks[:, None], axis=0)
    graft_row = jnp.pad(graft_layer[None, :], ((0, 1), (0, LANES - LAYERS)))
    *preconds, sums = products(left, right, owned, earlier, layer_row)
    returned = []
    for precond in preconds:
        outgoing = precond.reshape(group_size, rows, precond.shape[1])
        returned.append(lax.all_to_all(outgoing, GROUP, split_axis=0, concat_axis=0, tiled=True))
    sums = everywhere(sums + graft_row)
    layer_scale = jnp.sqrt(sums[0, :LAYERS]) * lax.rsqrt(sums[1, :LAYERS] + 1e-06)
    scales = (step_rate * jnp.sum(onehots * layer_scale[None, :], axis=1)).reshape(reps, blocks)

    changes = spread(*pick(position, returned[0]), reps)
    low, high, new_params = update(who, position, scales[me], returned, params, reps)
    finished = spread(low, high, reps)

    raw = [(offset, part, old, change) for (offset, part, old), (_, _, change) in zip(ahead, changes)]
    flat = scales.reshape(-1)
    new_params = place(who, flat, new_params, raw[:4], ())
    new_params = place(who, flat, new_params, raw[4:], finished[:4])
    for offset, part, piece in finished[4:]:
        owner = lax.rem(me + offset, reps)
        new_params = lax.dynamic_update_slice(new_params, piece[None], (owner, part * half, 0, RAW))
    return (new_params.reshape(reps * blocks, rows, width), new_accum)


def solution(mesh):
    split = Mesh(mesh.devices.reshape(4, 4, 2, mesh.shape["rep"]), EVERY)
    placed = (
        P("rep", None, GROUP, None),
        P("rep", GROUP, None),
        P("rep", GROUP, None),
        P("rep", GROUP, None, None, None),
        P("rep", GROUP, None, None, None),
        P(),
        P(),
    )
    return jax.shard_map(
        local,
        mesh=split,
        in_specs=placed,
        out_specs=(P(None, GROUP, None), P("rep", GROUP, None)),
        check_vma=False,
    )
```

```python
import jax
import jax.numpy as jnp
from jax import lax
from jax.experimental import pallas as pl
from jax.experimental.pallas import tpu as pltpu
from jax.sharding import Mesh
from jax.sharding import PartitionSpec as P


LAYERS = 8
LANES = 128
GROUP = ("group_0", "group_1", "group_2")
EVERY = ("group_0", "group_1", "group_2", "rep")
SENT = ((0, 384), (384, 640))
RAW = 512


step_rate = 0.5
f32 = jnp.float32
bf16 = jnp.bfloat16


def ring(count, step):
    return [(i, (i + step) % count) for i in range(count)]


def elements(*sizes):
    return tuple(pl.Element(size) for size in sizes)


def merge(who, parts, far_up, far_down, start, cols):
    _, blocks, rows, _ = parts.shape
    half = blocks // 2

    def body(who_ref, above, below, from_down, from_up, out_up, out_down):
        first = pl.program_id(0) == 0

        @pl.when(first)
        def _():
            out_up[...] = (above[0].astype(f32) + from_down[...].astype(f32)).astype(bf16)
            out_down[...] = below[0]

        @pl.when(jnp.logical_not(first))
        def _():
            out_up[...] = above[0]
            out_down[...] = (below[0].astype(f32) + from_up[...].astype(f32)).astype(bf16)

    piece = pl.BlockSpec((half, rows, cols), lambda i, w: (0, 0, 0))
    out = pl.BlockSpec((half, rows, cols), lambda i, w: (i, 0, 0))
    shape = jax.ShapeDtypeStruct((blocks, rows, cols), bf16)
    return pl.pallas_call(
        body,
        grid_spec=pltpu.PrefetchScalarGridSpec(
            num_scalar_prefetch=1,
            grid=(2,),
            in_specs=[
                pl.BlockSpec(elements(1, half, rows, cols), lambda i, w: (w[1], i * half, 0, start)),
                pl.BlockSpec(elements(1, half, rows, cols), lambda i, w: (w[3], i * half, 0, start)),
                piece,
                piece,
            ],
            out_specs=[out, out],
        ),
        out_shape=[shape, shape],
        name="merge",
    )(who, parts, parts, far_up, far_down)


def finish(who, table, parts, up, down, start, cols):
    _, blocks, rows, _ = parts.shape
    slots = table.shape[0]

    def body(who_ref, table_ref, own, one, two, gradient, slotted):
        total = own[0].astype(f32) + one[...].astype(f32) + two[...].astype(f32)
        gradient[...] = total.astype(bf16)
        for slot in range(slots):
            slotted[slot] = gradient[table_ref[slot]]

    block = pl.BlockSpec((blocks, rows, cols), lambda i, w, t: (0, 0, 0))
    return pl.pallas_call(
        body,
        grid_spec=pltpu.PrefetchScalarGridSpec(
            num_scalar_prefetch=2,
            grid=(1,),
            in_specs=[
                pl.BlockSpec(elements(1, blocks, rows, cols), lambda i, w, t: (w[0], 0, 0, start)),
                block,
                block,
            ],
            out_specs=[block, pl.BlockSpec((slots, rows, cols), lambda i, w, t: (0, 0, 0))],
        ),
        out_shape=[
            jax.ShapeDtypeStruct((blocks, rows, cols), bf16),
            jax.ShapeDtypeStruct((slots, rows, cols), bf16),
        ],
    )(who, table, parts, up, down)


def left_times(left, owned):
    order, cols = owned.shape
    tile = order // 2

    def body(left_ref, owned_ref, out):
        out[...] = jnp.dot(left_ref[...], owned_ref[...], preferred_element_type=f32).astype(bf16)

    return pl.pallas_call(
        body,
        grid=(2,),
        in_specs=[
            pl.BlockSpec((tile, order), lambda i: (i, 0)),
            pl.BlockSpec((order, cols), lambda i: (0, 0)),
        ],
        out_specs=pl.BlockSpec((tile, cols), lambda i: (i, 0)),
        out_shape=jax.ShapeDtypeStruct((order, cols), bf16),
        name="left_times",
    )(left, owned)


def products(left, right, owned, earlier, layer_row):
    order, cols = owned.shape
    steps = 2
    tile = order // steps
    last = SENT[-1][0]

    def body(left_ref, right_ref, owned_ref, layer_ref, *rest):
        before, (first, second, sums, mid) = rest[: len(earlier)], rest[len(earlier) :]
        mid[:, last : last + cols] = jnp.dot(
            left_ref[...], owned_ref[...], preferred_element_type=f32
        ).astype(bf16)
        for ref, (start, size) in zip(before, SENT):
            mid[:, start : start + size] = ref[...]
        product = jnp.dot(mid[...], right_ref[...], preferred_element_type=f32).astype(bf16)
        first[...] = product[:, :RAW]
        second[...] = product[:, RAW:]
        wide = product.astype(f32)
        squares = jnp.sum(jnp.sum(wide * wide, axis=0, keepdims=True), axis=1, keepdims=True)

        @pl.when(pl.program_id(0) == 0)
        def _():
            sums[0:1] = jnp.zeros_like(squares * layer_ref[...])
            sums[1:2] = layer_ref[...] * squares

        @pl.when(pl.program_id(0) > 0)
        def _():
            sums[1:2] += layer_ref[...] * squares

    row = pl.BlockSpec((1, LANES), lambda i: (0, 0))
    return pl.pallas_call(
        body,
        grid=(steps,),
        in_specs=[
            pl.BlockSpec((tile, order), lambda i: (i, 0)),
            pl.BlockSpec((order, order), lambda i: (0, 0)),
            pl.BlockSpec((order, cols), lambda i: (0, 0)),
            row,
            *[pl.BlockSpec((tile, e.shape[1]), lambda i: (i, 0)) for e in earlier],
        ],
        out_specs=[
            pl.BlockSpec((tile, RAW), lambda i: (i, 0)),
            pl.BlockSpec((tile, order - RAW), lambda i: (i, 0)),
            pl.BlockSpec((2, LANES), lambda i: (0, 0)),
        ],
        out_shape=[
            jax.ShapeDtypeStruct((order, RAW), bf16),
            jax.ShapeDtypeStruct((order, order - RAW), bf16),
            jax.ShapeDtypeStruct((2, LANES), f32),
        ],
        scratch_shapes=[pltpu.VMEM((tile, order), bf16)],
        name="products",
    )(left, right, owned, layer_row, *earlier)


def pick(position, returned):
    blocks = position.shape[0]
    half = blocks // 2
    _, rows, cols = returned.shape

    def body(position_ref, returned_ref, low, high, sems):
        copies = []
        for block in range(blocks):
            out = low.at[block] if block < half else high.at[block - half]
            copies.append(pltpu.make_async_copy(returned_ref.at[position_ref[block]], out, sems.at[block]))
            copies[-1].start()
        for copy in copies:
            copy.wait()

    piece = pl.BlockSpec((half, rows, cols), lambda i, p: (0, 0, 0))
    shape = jax.ShapeDtypeStruct((half, rows, cols), bf16)
    return pl.pallas_call(
        body,
        grid_spec=pltpu.PrefetchScalarGridSpec(
            num_scalar_prefetch=1,
            grid=(1,),
            in_specs=[pl.BlockSpec(memory_space=pltpu.HBM)],
            out_specs=[piece, piece],
            scratch_shapes=[pltpu.SemaphoreType.DMA((blocks,))],
        ),
        out_shape=[shape, shape],
        name="pick",
    )(position, returned)


def update(who, position, scale, returned, params, reps):
    blocks, rows, width = params.shape
    half = blocks // 2

    def body(who_ref, position_ref, scale_ref, one, two, params_ref, low, high, whole, picked, sems):
        copies = []
        for block in range(blocks):
            slot = position_ref[block]
            pair = (
                pltpu.make_async_copy(one.at[slot], picked.at[block, :, pl.ds(0, RAW)], sems.at[0, block]),
                pltpu.make_async_copy(
                    two.at[slot], picked.at[block, :, pl.ds(RAW, width - RAW)], sems.at[1, block]
                ),
            )
            for copy in pair:
                copy.start()
            copies.append(pair)
        for block, pair in enumerate(copies):
            for copy in pair:
                copy.wait()
            change = scale_ref[block] * picked[block].astype(f32)
            new = (params_ref[block].astype(f32) - change).astype(bf16)
            whole[0, block] = new
            if block < half:
                low[block] = new[:, RAW:]
            else:
                high[block - half] = new[:, RAW:]

    hbm = pl.BlockSpec(memory_space=pltpu.HBM)
    piece = pl.BlockSpec((half, rows, width - RAW), lambda i, w, p, s: (0, 0, 0))
    shape = jax.ShapeDtypeStruct((half, rows, width - RAW), bf16)
    return pl.pallas_call(
        body,
        grid_spec=pltpu.PrefetchScalarGridSpec(
            num_scalar_prefetch=3,
            grid=(1,),
            in_specs=[hbm, hbm, pl.BlockSpec((blocks, rows, width), lambda i, w, p, s: (0, 0, 0))],
            out_specs=[
                piece,
                piece,
                pl.BlockSpec((1, blocks, rows, width), lambda i, w, p, s: (w[0], 0, 0, 0)),
            ],
            scratch_shapes=[
                pltpu.VMEM((blocks, rows, width), bf16),
                pltpu.SemaphoreType.DMA((2, blocks)),
            ],
        ),
        out_shape=[shape, shape, jax.ShapeDtypeStruct((reps, blocks, rows, width), bf16)],
        name="update",
    )(who, position, scale, *returned, params)


def place(owners, scales, whole, raw, ready):
    half, rows, _ = (raw or ready)[0][2].shape
    blocks = 2 * half
    pieces = len(raw) + len(ready)

    def body(owners_ref, scales_ref, *refs):
        olds, changes = refs[: len(raw)], refs[len(raw) : 2 * len(raw)]
        values = refs[2 * len(raw) : 2 * len(raw) + len(ready)]
        out, made, sems = refs[-3:]
        copies = []
        for at, (offset, part, value) in enumerate([(o, p, None) for o, p, _, _ in raw] + list(ready)):
            owner = owners_ref[offset]
            if at < len(raw):
                for block in range(half):
                    scale = scales_ref[owner * blocks + part * half + block]
                    new = olds[at][block].astype(f32) - scale * changes[at][block].astype(f32)
                    made[at, block] = new.astype(bf16)
                source, columns = made.at[at], pl.ds(0, RAW)
            else:
                source = values[at - len(raw)]
                columns = pl.ds(RAW, value.shape[2])
            target = out.at[owner, pl.ds(part * half, half), :, columns]
            copies.append(pltpu.make_async_copy(source, target, sems.at[at]))
            copies[-1].start()
        for copy in copies:
            copy.wait()

    def block_of(array):
        return pl.BlockSpec(array.shape, lambda i, o, s: (0, 0, 0))

    arrays = [old for _, _, old, _ in raw] + [change for _, _, _, change in raw] + [v for _, _, v in ready]
    hbm = pl.BlockSpec(memory_space=pltpu.HBM)
    return pl.pallas_call(
        body,
        grid_spec=pltpu.PrefetchScalarGridSpec(
            num_scalar_prefetch=2,
            grid=(1,),
            in_specs=[*[block_of(array) for array in arrays], hbm],
            out_specs=hbm,
            scratch_shapes=[
                pltpu.VMEM((max(len(raw), 1), half, rows, RAW), bf16),
                pltpu.SemaphoreType.DMA((pieces,)),
            ],
        ),
        out_shape=jax.ShapeDtypeStruct(whole.shape, bf16),
        input_output_aliases={2 + len(arrays): 0},
    )(owners, scales, *arrays, whole)


def everywhere(value):
    value = value + lax.ppermute(value, "group_2", [(0, 1), (1, 0)])
    for axis in ("rep", "group_0", "group_1"):
        one, two, three = [lax.ppermute(value, axis, ring(4, step)) for step in (1, 2, 3)]
        value = (value + two) + (one + three)
    return value


def spread(low, high, reps):
    up, down = ring(reps, 1), ring(reps, -1)
    low_up = lax.ppermute(low, "rep", up)
    high_down = lax.ppermute(high, "rep", down)
    high_up = lax.ppermute(high, "rep", up)
    low_down = lax.ppermute(low, "rep", down)
    far_low = lax.ppermute(low_up, "rep", up)
    far_high = lax.ppermute(high_down, "rep", down)
    return (
        (3, 0, low_up),
        (1, 1, high_down),
        (3, 1, high_up),
        (1, 0, low_down),
        (2, 0, far_low),
        (2, 1, far_high),
    )


def local(grad_parts, params, accum, left_pre, right_pre, slot_block, layer_of):
    group_size = lax.axis_size(GROUP)
    reps = lax.axis_size("rep")
    me = lax.axis_index("rep")
    group_index = lax.axis_index(GROUP)
    blocks, rows, width = params.shape
    half = blocks // 2
    up, down = ring(reps, 1), ring(reps, -1)
    parts = grad_parts[0].reshape(reps, blocks, rows, width)
    who = lax.rem(me + jnp.arange(reps, dtype=jnp.int32), reps)
    table = lax.dynamic_index_in_dim(slot_block, me, 0, keepdims=False).reshape(-1)
    wanted = jnp.maximum(table, 0)
    left, right = left_pre[0, 0, 0], right_pre[0, 0, 0]

    far = lax.rem(me + 2, reps)
    gradients, earlier, owned = [None] * len(SENT), [], None
    for chunk, (start, cols) in enumerate(SENT):
        low = lax.dynamic_slice(parts, (far, 0, 0, start), (1, half, rows, cols))[0]
        high = lax.dynamic_slice(parts, (far, half, 0, start), (1, half, rows, cols))[0]
        far_up = lax.ppermute(low, "rep", up)
        far_down = lax.ppermute(high, "rep", down)
        to_up, to_down = merge(who, parts, far_up, far_down, start, cols)
        near_up = lax.ppermute(to_up, "rep", up)
        near_down = lax.ppermute(to_down, "rep", down)
        gradient, outgoing = finish(who, wanted, parts, near_up, near_down, start, cols)
        gradients[chunk] = gradient
        arrived = lax.all_to_all(outgoing, GROUP, split_axis=0, concat_axis=0, tiled=True)
        if chunk > 0:
            earlier.append(left_times(left, owned))
        owned = arrived.reshape(group_size * rows, cols)

    old_low, old_high = params[:half, :, :RAW], params[half:, :, :RAW]
    ahead = spread(old_low, old_high, reps)

    onehots = (layer_of[:, None] == jnp.arange(LAYERS, dtype=jnp.int32)[None, :]).astype(f32)
    onehot = lax.dynamic_slice_in_dim(onehots, me * blocks, blocks)
    mine = lax.dynamic_index_in_dim(table, group_index, 0, keepdims=False)
    chosen = (jnp.arange(blocks, dtype=jnp.int32) == mine).astype(f32)
    my_layer = jnp.sum(chosen[:, None] * onehot, axis=0)
    layer_row = jnp.pad(my_layer[None, :], ((0, 0), (0, LANES - LAYERS)))
    position = jnp.sum(
        jnp.where(
            table[None, :] == jnp.arange(blocks, dtype=jnp.int32)[:, None],
            jnp.arange(group_size, dtype=jnp.int32)[None, :],
            0,
        ),
        axis=1,
    )

    owned, earlier, layer_row, onehot, gradients = lax.optimization_barrier(
        (owned, earlier, layer_row, onehot, gradients)
    )

    wide = jnp.concatenate(gradients, axis=2).astype(f32)
    new_accum = accum + wide * wide
    graft = wide * lax.rsqrt(new_accum)
    graft_blocks = jnp.sum(graft * graft, axis=(1, 2))
    graft_layer = jnp.sum(onehot * graft_blocks[:, None], axis=0)
    graft_row = jnp.pad(graft_layer[None, :], ((0, 1), (0, LANES - LAYERS)))
    *preconds, sums = products(left, right, owned, earlier, layer_row)
    returned = []
    for precond in preconds:
        outgoing = precond.reshape(group_size, rows, precond.shape[1])
        returned.append(lax.all_to_all(outgoing, GROUP, split_axis=0, concat_axis=0, tiled=True))
    sums = everywhere(sums + graft_row)
    layer_scale = jnp.sqrt(sums[0, :LAYERS]) * lax.rsqrt(sums[1, :LAYERS] + 1e-06)
    scales = (step_rate * jnp.sum(onehots * layer_scale[None, :], axis=1)).reshape(reps, blocks)

    changes = spread(*pick(position, returned[0]), reps)
    low, high, new_params = update(who, position, scales[me], returned, params, reps)
    finished = spread(low, high, reps)

    raw = [(offset, part, old, change) for (offset, part, old), (_, _, change) in zip(ahead, changes)]
    flat = scales.reshape(-1)
    new_params = place(who, flat, new_params, raw, ())
    new_params = place(who, flat, new_params, (), finished[:4])
    for offset, part, piece in finished[4:]:
        owner = lax.rem(me + offset, reps)
        new_params = lax.dynamic_update_slice(new_params, piece[None], (owner, part * half, 0, RAW))
    return (new_params.reshape(reps * blocks, rows, width), new_accum)


def solution(mesh):
    split = Mesh(mesh.devices.reshape(4, 4, 2, mesh.shape["rep"]), EVERY)
    placed = (
        P("rep", None, GROUP, None),
        P("rep", GROUP, None),
        P("rep", GROUP, None),
        P("rep", GROUP, None, None, None),
        P("rep", GROUP, None, None, None),
        P(),
        P(),
    )
    return jax.shard_map(
        local,
        mesh=split,
        in_specs=placed,
        out_specs=(P(None, GROUP, None), P("rep", GROUP, None)),
        check_vma=False,
    )
```

```python
import jax
import jax.numpy as jnp
from jax import lax
from jax.experimental import pallas as pl
from jax.experimental.pallas import tpu as pltpu
from jax.sharding import Mesh
from jax.sharding import PartitionSpec as P


LAYERS = 8
LANES = 128
GROUP = ("group_0", "group_1", "group_2")
EVERY = ("group_0", "group_1", "group_2", "rep")
SENT = ((0, 384), (384, 640))
RAW = 512


step_rate = 0.5
f32 = jnp.float32
bf16 = jnp.bfloat16


def ring(count, step):
    return [(i, (i + step) % count) for i in range(count)]


def elements(*sizes):
    return tuple(pl.Element(size) for size in sizes)


def merge(who, parts, far_up, far_down, start, cols):
    _, blocks, rows, _ = parts.shape
    half = blocks // 2

    def body(who_ref, above, below, from_down, from_up, out_up, out_down):
        first = pl.program_id(0) == 0

        @pl.when(first)
        def _():
            out_up[...] = (above[0].astype(f32) + from_down[...].astype(f32)).astype(bf16)
            out_down[...] = below[0]

        @pl.when(jnp.logical_not(first))
        def _():
            out_up[...] = above[0]
            out_down[...] = (below[0].astype(f32) + from_up[...].astype(f32)).astype(bf16)

    piece = pl.BlockSpec((half, rows, cols), lambda i, w: (0, 0, 0))
    out = pl.BlockSpec((half, rows, cols), lambda i, w: (i, 0, 0))
    shape = jax.ShapeDtypeStruct((blocks, rows, cols), bf16)
    return pl.pallas_call(
        body,
        grid_spec=pltpu.PrefetchScalarGridSpec(
            num_scalar_prefetch=1,
            grid=(2,),
            in_specs=[
                pl.BlockSpec(elements(1, half, rows, cols), lambda i, w: (w[1], i * half, 0, start)),
                pl.BlockSpec(elements(1, half, rows, cols), lambda i, w: (w[3], i * half, 0, start)),
                piece,
                piece,
            ],
            out_specs=[out, out],
        ),
        out_shape=[shape, shape],
        name="merge",
    )(who, parts, parts, far_up, far_down)


def finish(who, table, parts, up, down, start, cols):
    _, blocks, rows, _ = parts.shape
    slots = table.shape[0]

    def body(who_ref, table_ref, own, one, two, gradient, slotted):
        total = own[0].astype(f32) + one[...].astype(f32) + two[...].astype(f32)
        gradient[...] = total.astype(bf16)
        for slot in range(slots):
            slotted[slot] = gradient[table_ref[slot]]

    block = pl.BlockSpec((blocks, rows, cols), lambda i, w, t: (0, 0, 0))
    return pl.pallas_call(
        body,
        grid_spec=pltpu.PrefetchScalarGridSpec(
            num_scalar_prefetch=2,
            grid=(1,),
            in_specs=[
                pl.BlockSpec(elements(1, blocks, rows, cols), lambda i, w, t: (w[0], 0, 0, start)),
                block,
                block,
            ],
            out_specs=[block, pl.BlockSpec((slots, rows, cols), lambda i, w, t: (0, 0, 0))],
        ),
        out_shape=[
            jax.ShapeDtypeStruct((blocks, rows, cols), bf16),
            jax.ShapeDtypeStruct((slots, rows, cols), bf16),
        ],
    )(who, table, parts, up, down)


def left_times(left, owned):
    order, cols = owned.shape
    tile = order // 2

    def body(left_ref, owned_ref, out):
        out[...] = jnp.dot(left_ref[...], owned_ref[...], preferred_element_type=f32).astype(bf16)

    return pl.pallas_call(
        body,
        grid=(2,),
        in_specs=[
            pl.BlockSpec((tile, order), lambda i: (i, 0)),
            pl.BlockSpec((order, cols), lambda i: (0, 0)),
        ],
        out_specs=pl.BlockSpec((tile, cols), lambda i: (i, 0)),
        out_shape=jax.ShapeDtypeStruct((order, cols), bf16),
        name="left_times",
    )(left, owned)


def products(left, right, owned, earlier, layer_row):
    order, cols = owned.shape
    steps = 2
    tile = order // steps
    last = SENT[-1][0]

    def body(left_ref, right_ref, owned_ref, layer_ref, *rest):
        before, (first, second, sums, mid) = rest[: len(earlier)], rest[len(earlier) :]
        mid[:, last : last + cols] = jnp.dot(
            left_ref[...], owned_ref[...], preferred_element_type=f32
        ).astype(bf16)
        for ref, (start, size) in zip(before, SENT):
            mid[:, start : start + size] = ref[...]
        product = jnp.dot(mid[...], right_ref[...], preferred_element_type=f32).astype(bf16)
        first[...] = product[:, :RAW]
        second[...] = product[:, RAW:]
        wide = product.astype(f32)
        squares = jnp.sum(jnp.sum(wide * wide, axis=0, keepdims=True), axis=1, keepdims=True)

        @pl.when(pl.program_id(0) == 0)
        def _():
            sums[0:1] = jnp.zeros_like(squares * layer_ref[...])
            sums[1:2] = layer_ref[...] * squares

        @pl.when(pl.program_id(0) > 0)
        def _():
            sums[1:2] += layer_ref[...] * squares

    row = pl.BlockSpec((1, LANES), lambda i: (0, 0))
    return pl.pallas_call(
        body,
        grid=(steps,),
        in_specs=[
            pl.BlockSpec((tile, order), lambda i: (i, 0)),
            pl.BlockSpec((order, order), lambda i: (0, 0)),
            pl.BlockSpec((order, cols), lambda i: (0, 0)),
            row,
            *[pl.BlockSpec((tile, e.shape[1]), lambda i: (i, 0)) for e in earlier],
        ],
        out_specs=[
            pl.BlockSpec((tile, RAW), lambda i: (i, 0)),
            pl.BlockSpec((tile, order - RAW), lambda i: (i, 0)),
            pl.BlockSpec((2, LANES), lambda i: (0, 0)),
        ],
        out_shape=[
            jax.ShapeDtypeStruct((order, RAW), bf16),
            jax.ShapeDtypeStruct((order, order - RAW), bf16),
            jax.ShapeDtypeStruct((2, LANES), f32),
        ],
        scratch_shapes=[pltpu.VMEM((tile, order), bf16)],
        name="products",
    )(left, right, owned, layer_row, *earlier)


def pick(position, returned):
    blocks = position.shape[0]
    half = blocks // 2
    _, rows, cols = returned.shape

    def body(position_ref, returned_ref, low, high, sems):
        copies = []
        for block in range(blocks):
            out = low.at[block] if block < half else high.at[block - half]
            copies.append(pltpu.make_async_copy(returned_ref.at[position_ref[block]], out, sems.at[block]))
            copies[-1].start()
        for copy in copies:
            copy.wait()

    piece = pl.BlockSpec((half, rows, cols), lambda i, p: (0, 0, 0))
    shape = jax.ShapeDtypeStruct((half, rows, cols), bf16)
    return pl.pallas_call(
        body,
        grid_spec=pltpu.PrefetchScalarGridSpec(
            num_scalar_prefetch=1,
            grid=(1,),
            in_specs=[pl.BlockSpec(memory_space=pltpu.HBM)],
            out_specs=[piece, piece],
            scratch_shapes=[pltpu.SemaphoreType.DMA((blocks,))],
        ),
        out_shape=[shape, shape],
        name="pick",
    )(position, returned)


def update(who, position, scale, returned, params, reps):
    blocks, rows, width = params.shape
    half = blocks // 2

    def body(who_ref, position_ref, scale_ref, one, two, params_ref, low, high, whole, picked, sems):
        copies = []
        for block in range(blocks):
            slot = position_ref[block]
            pair = (
                pltpu.make_async_copy(one.at[slot], picked.at[block, :, pl.ds(0, RAW)], sems.at[0, block]),
                pltpu.make_async_copy(
                    two.at[slot], picked.at[block, :, pl.ds(RAW, width - RAW)], sems.at[1, block]
                ),
            )
            for copy in pair:
                copy.start()
            copies.append(pair)
        for block, pair in enumerate(copies):
            for copy in pair:
                copy.wait()
            change = scale_ref[block] * picked[block].astype(f32)
            new = (params_ref[block].astype(f32) - change).astype(bf16)
            whole[0, block] = new
            if block < half:
                low[block] = new[:, RAW:]
            else:
                high[block - half] = new[:, RAW:]

    hbm = pl.BlockSpec(memory_space=pltpu.HBM)
    piece = pl.BlockSpec((half, rows, width - RAW), lambda i, w, p, s: (0, 0, 0))
    shape = jax.ShapeDtypeStruct((half, rows, width - RAW), bf16)
    return pl.pallas_call(
        body,
        grid_spec=pltpu.PrefetchScalarGridSpec(
            num_scalar_prefetch=3,
            grid=(1,),
            in_specs=[hbm, hbm, pl.BlockSpec((blocks, rows, width), lambda i, w, p, s: (0, 0, 0))],
            out_specs=[
                piece,
                piece,
                pl.BlockSpec((1, blocks, rows, width), lambda i, w, p, s: (w[0], 0, 0, 0)),
            ],
            scratch_shapes=[
                pltpu.VMEM((blocks, rows, width), bf16),
                pltpu.SemaphoreType.DMA((2, blocks)),
            ],
        ),
        out_shape=[shape, shape, jax.ShapeDtypeStruct((reps, blocks, rows, width), bf16)],
        name="update",
    )(who, position, scale, *returned, params)


def place(owners, scales, whole, raw):
    half, rows, _ = raw[0][2].shape
    blocks = 2 * half

    def body(owners_ref, scales_ref, *refs):
        olds, changes = refs[: len(raw)], refs[len(raw) : 2 * len(raw)]
        out, made, sems = refs[-3:]
        copies = []
        for at, (offset, part, _, _) in enumerate(raw):
            owner = owners_ref[offset]
            for block in range(half):
                scale = scales_ref[owner * blocks + part * half + block]
                new = olds[at][block].astype(f32) - scale * changes[at][block].astype(f32)
                made[at, block] = new.astype(bf16)
            target = out.at[owner, pl.ds(part * half, half), :, pl.ds(0, RAW)]
            copies.append(pltpu.make_async_copy(made.at[at], target, sems.at[at]))
            copies[-1].start()
        for copy in copies:
            copy.wait()

    arrays = [old for _, _, old, _ in raw] + [change for _, _, _, change in raw]
    piece = pl.BlockSpec((half, rows, RAW), lambda i, o, s: (0, 0, 0))
    hbm = pl.BlockSpec(memory_space=pltpu.HBM)
    return pl.pallas_call(
        body,
        grid_spec=pltpu.PrefetchScalarGridSpec(
            num_scalar_prefetch=2,
            grid=(1,),
            in_specs=[*[piece for _ in arrays], hbm],
            out_specs=hbm,
            scratch_shapes=[
                pltpu.VMEM((len(raw), half, rows, RAW), bf16),
                pltpu.SemaphoreType.DMA((len(raw),)),
            ],
        ),
        out_shape=jax.ShapeDtypeStruct(whole.shape, bf16),
        input_output_aliases={2 + len(arrays): 0},
    )(owners, scales, *arrays, whole)


def everywhere(value):
    value = value + lax.ppermute(value, "group_2", [(0, 1), (1, 0)])
    for axis in ("rep", "group_0", "group_1"):
        one, two, three = [lax.ppermute(value, axis, ring(4, step)) for step in (1, 2, 3)]
        value = (value + two) + (one + three)
    return value


def spread(low, high, reps):
    up, down = ring(reps, 1), ring(reps, -1)
    low_up = lax.ppermute(low, "rep", up)
    high_down = lax.ppermute(high, "rep", down)
    high_up = lax.ppermute(high, "rep", up)
    low_down = lax.ppermute(low, "rep", down)
    far_low = lax.ppermute(low_up, "rep", up)
    far_high = lax.ppermute(high_down, "rep", down)
    return (
        (3, 0, low_up),
        (1, 1, high_down),
        (3, 1, high_up),
        (1, 0, low_down),
        (2, 0, far_low),
        (2, 1, far_high),
    )


def local(grad_parts, params, accum, left_pre, right_pre, slot_block, layer_of):
    group_size = lax.axis_size(GROUP)
    reps = lax.axis_size("rep")
    me = lax.axis_index("rep")
    group_index = lax.axis_index(GROUP)
    blocks, rows, width = params.shape
    half = blocks // 2
    up, down = ring(reps, 1), ring(reps, -1)
    parts = grad_parts[0].reshape(reps, blocks, rows, width)
    who = lax.rem(me + jnp.arange(reps, dtype=jnp.int32), reps)
    table = lax.dynamic_index_in_dim(slot_block, me, 0, keepdims=False).reshape(-1)
    wanted = jnp.maximum(table, 0)
    left, right = left_pre[0, 0, 0], right_pre[0, 0, 0]

    far = lax.rem(me + 2, reps)
    gradients, earlier, owned = [None] * len(SENT), [], None
    for chunk, (start, cols) in enumerate(SENT):
        low = lax.dynamic_slice(parts, (far, 0, 0, start), (1, half, rows, cols))[0]
        high = lax.dynamic_slice(parts, (far, half, 0, start), (1, half, rows, cols))[0]
        far_up = lax.ppermute(low, "rep", up)
        far_down = lax.ppermute(high, "rep", down)
        to_up, to_down = merge(who, parts, far_up, far_down, start, cols)
        near_up = lax.ppermute(to_up, "rep", up)
        near_down = lax.ppermute(to_down, "rep", down)
        gradient, outgoing = finish(who, wanted, parts, near_up, near_down, start, cols)
        gradients[chunk] = gradient
        arrived = lax.all_to_all(outgoing, GROUP, split_axis=0, concat_axis=0, tiled=True)
        if chunk > 0:
            earlier.append(left_times(left, owned))
        owned = arrived.reshape(group_size * rows, cols)

    old_low, old_high = params[:half, :, :RAW], params[half:, :, :RAW]
    ahead = spread(old_low, old_high, reps)

    onehots = (layer_of[:, None] == jnp.arange(LAYERS, dtype=jnp.int32)[None, :]).astype(f32)
    onehot = lax.dynamic_slice_in_dim(onehots, me * blocks, blocks)
    mine = lax.dynamic_index_in_dim(table, group_index, 0, keepdims=False)
    chosen = (jnp.arange(blocks, dtype=jnp.int32) == mine).astype(f32)
    my_layer = jnp.sum(chosen[:, None] * onehot, axis=0)
    layer_row = jnp.pad(my_layer[None, :], ((0, 0), (0, LANES - LAYERS)))
    position = jnp.sum(
        jnp.where(
            table[None, :] == jnp.arange(blocks, dtype=jnp.int32)[:, None],
            jnp.arange(group_size, dtype=jnp.int32)[None, :],
            0,
        ),
        axis=1,
    )

    wide = jnp.concatenate(gradients, axis=2).astype(f32)
    new_accum = accum + wide * wide
    graft = wide * lax.rsqrt(new_accum)
    graft_blocks = jnp.sum(graft * graft, axis=(1, 2))
    graft_layer = jnp.sum(onehot * graft_blocks[:, None], axis=0)
    graft_row = jnp.pad(graft_layer[None, :], ((0, 1), (0, LANES - LAYERS)))
    owned, earlier, layer_row, graft_row, new_accum = lax.optimization_barrier(
        (owned, earlier, layer_row, graft_row, new_accum)
    )

    *preconds, sums = products(left, right, owned, earlier, layer_row)
    returned = []
    for precond in preconds:
        outgoing = precond.reshape(group_size, rows, precond.shape[1])
        returned.append(lax.all_to_all(outgoing, GROUP, split_axis=0, concat_axis=0, tiled=True))
    sums = everywhere(sums + graft_row)
    layer_scale = jnp.sqrt(sums[0, :LAYERS]) * lax.rsqrt(sums[1, :LAYERS] + 1e-06)
    scales = (step_rate * jnp.sum(onehots * layer_scale[None, :], axis=1)).reshape(reps, blocks)

    changes = spread(*pick(position, returned[0]), reps)
    low, high, new_params = update(who, position, scales[me], returned, params, reps)
    finished = spread(low, high, reps)

    raw = [(offset, part, old, change) for (offset, part, old), (_, _, change) in zip(ahead, changes)]
    flat = scales.reshape(-1)
    new_params = place(who, flat, new_params, raw[:4])
    new_params = place(who, flat, new_params, raw[4:])
    for offset, part, piece in finished:
        owner = lax.rem(me + offset, reps)
        new_params = lax.dynamic_update_slice(new_params, piece[None], (owner, part * half, 0, RAW))
    return (new_params.reshape(reps * blocks, rows, width), new_accum)


def solution(mesh):
    split = Mesh(mesh.devices.reshape(4, 4, 2, mesh.shape["rep"]), EVERY)
    placed = (
        P("rep", None, GROUP, None),
        P("rep", GROUP, None),
        P("rep", GROUP, None),
        P("rep", GROUP, None, None, None),
        P("rep", GROUP, None, None, None),
        P(),
        P(),
    )
    return jax.shard_map(
        local,
        mesh=split,
        in_specs=placed,
        out_specs=(P(None, GROUP, None), P("rep", GROUP, None)),
        check_vma=False,
    )
```

```python
import jax
import jax.numpy as jnp
from jax import lax
from jax.experimental import pallas as pl
from jax.experimental.pallas import tpu as pltpu
from jax.sharding import Mesh
from jax.sharding import PartitionSpec as P


LAYERS = 8
LANES = 128
GROUP = ("group_0", "group_1", "group_2")
EVERY = ("group_0", "group_1", "group_2", "rep")
SENT = ((0, 384), (384, 640))
RAW = 512


step_rate = 0.5
f32 = jnp.float32
bf16 = jnp.bfloat16


def ring(count, step):
    return [(i, (i + step) % count) for i in range(count)]


def elements(*sizes):
    return tuple(pl.Element(size) for size in sizes)


def merge(who, parts, far_up, far_down, start, cols):
    _, blocks, rows, _ = parts.shape
    half = blocks // 2

    def body(who_ref, above, below, from_down, from_up, out_up, out_down):
        first = pl.program_id(0) == 0

        @pl.when(first)
        def _():
            out_up[...] = (above[0].astype(f32) + from_down[...].astype(f32)).astype(bf16)
            out_down[...] = below[0]

        @pl.when(jnp.logical_not(first))
        def _():
            out_up[...] = above[0]
            out_down[...] = (below[0].astype(f32) + from_up[...].astype(f32)).astype(bf16)

    piece = pl.BlockSpec((half, rows, cols), lambda i, w: (0, 0, 0))
    out = pl.BlockSpec((half, rows, cols), lambda i, w: (i, 0, 0))
    shape = jax.ShapeDtypeStruct((blocks, rows, cols), bf16)
    return pl.pallas_call(
        body,
        grid_spec=pltpu.PrefetchScalarGridSpec(
            num_scalar_prefetch=1,
            grid=(2,),
            in_specs=[
                pl.BlockSpec(elements(1, half, rows, cols), lambda i, w: (w[1], i * half, 0, start)),
                pl.BlockSpec(elements(1, half, rows, cols), lambda i, w: (w[3], i * half, 0, start)),
                piece,
                piece,
            ],
            out_specs=[out, out],
        ),
        out_shape=[shape, shape],
        name="merge",
    )(who, parts, parts, far_up, far_down)


def finish(who, table, parts, up, down, start, cols):
    _, blocks, rows, _ = parts.shape
    slots = table.shape[0]

    def body(who_ref, table_ref, own, one, two, gradient, slotted):
        total = own[0].astype(f32) + one[...].astype(f32) + two[...].astype(f32)
        gradient[...] = total.astype(bf16)
        for slot in range(slots):
            slotted[slot] = gradient[table_ref[slot]]

    block = pl.BlockSpec((blocks, rows, cols), lambda i, w, t: (0, 0, 0))
    return pl.pallas_call(
        body,
        grid_spec=pltpu.PrefetchScalarGridSpec(
            num_scalar_prefetch=2,
            grid=(1,),
            in_specs=[
                pl.BlockSpec(elements(1, blocks, rows, cols), lambda i, w, t: (w[0], 0, 0, start)),
                block,
                block,
            ],
            out_specs=[block, pl.BlockSpec((slots, rows, cols), lambda i, w, t: (0, 0, 0))],
        ),
        out_shape=[
            jax.ShapeDtypeStruct((blocks, rows, cols), bf16),
            jax.ShapeDtypeStruct((slots, rows, cols), bf16),
        ],
    )(who, table, parts, up, down)


def left_times(left, owned):
    order, cols = owned.shape
    tile = order // 2

    def body(left_ref, owned_ref, out):
        out[...] = jnp.dot(left_ref[...], owned_ref[...], preferred_element_type=f32).astype(bf16)

    return pl.pallas_call(
        body,
        grid=(2,),
        in_specs=[
            pl.BlockSpec((tile, order), lambda i: (i, 0)),
            pl.BlockSpec((order, cols), lambda i: (0, 0)),
        ],
        out_specs=pl.BlockSpec((tile, cols), lambda i: (i, 0)),
        out_shape=jax.ShapeDtypeStruct((order, cols), bf16),
        name="left_times",
    )(left, owned)


def products(left, right, owned, earlier, layer_row):
    order, cols = owned.shape
    steps = 2
    tile = order // steps
    last = SENT[-1][0]

    def body(left_ref, right_ref, owned_ref, layer_ref, *rest):
        before, (first, second, sums, mid) = rest[: len(earlier)], rest[len(earlier) :]
        mid[:, last : last + cols] = jnp.dot(
            left_ref[...], owned_ref[...], preferred_element_type=f32
        ).astype(bf16)
        for ref, (start, size) in zip(before, SENT):
            mid[:, start : start + size] = ref[...]
        product = jnp.dot(mid[...], right_ref[...], preferred_element_type=f32).astype(bf16)
        first[...] = product[:, :RAW]
        second[...] = product[:, RAW:]
        wide = product.astype(f32)
        squares = jnp.sum(jnp.sum(wide * wide, axis=0, keepdims=True), axis=1, keepdims=True)

        @pl.when(pl.program_id(0) == 0)
        def _():
            sums[0:1] = jnp.zeros_like(squares * layer_ref[...])
            sums[1:2] = layer_ref[...] * squares

        @pl.when(pl.program_id(0) > 0)
        def _():
            sums[1:2] += layer_ref[...] * squares

    row = pl.BlockSpec((1, LANES), lambda i: (0, 0))
    return pl.pallas_call(
        body,
        grid=(steps,),
        in_specs=[
            pl.BlockSpec((tile, order), lambda i: (i, 0)),
            pl.BlockSpec((order, order), lambda i: (0, 0)),
            pl.BlockSpec((order, cols), lambda i: (0, 0)),
            row,
            *[pl.BlockSpec((tile, e.shape[1]), lambda i: (i, 0)) for e in earlier],
        ],
        out_specs=[
            pl.BlockSpec((tile, RAW), lambda i: (i, 0)),
            pl.BlockSpec((tile, order - RAW), lambda i: (i, 0)),
            pl.BlockSpec((2, LANES), lambda i: (0, 0)),
        ],
        out_shape=[
            jax.ShapeDtypeStruct((order, RAW), bf16),
            jax.ShapeDtypeStruct((order, order - RAW), bf16),
            jax.ShapeDtypeStruct((2, LANES), f32),
        ],
        scratch_shapes=[pltpu.VMEM((tile, order), bf16)],
        name="products",
    )(left, right, owned, layer_row, *earlier)


def pick(position, returned):
    blocks = position.shape[0]
    half = blocks // 2
    _, rows, cols = returned.shape

    def body(position_ref, returned_ref, low, high, sems):
        copies = []
        for block in range(blocks):
            out = low.at[block] if block < half else high.at[block - half]
            copies.append(pltpu.make_async_copy(returned_ref.at[position_ref[block]], out, sems.at[block]))
            copies[-1].start()
        for copy in copies:
            copy.wait()

    piece = pl.BlockSpec((half, rows, cols), lambda i, p: (0, 0, 0))
    shape = jax.ShapeDtypeStruct((half, rows, cols), bf16)
    return pl.pallas_call(
        body,
        grid_spec=pltpu.PrefetchScalarGridSpec(
            num_scalar_prefetch=1,
            grid=(1,),
            in_specs=[pl.BlockSpec(memory_space=pltpu.HBM)],
            out_specs=[piece, piece],
            scratch_shapes=[pltpu.SemaphoreType.DMA((blocks,))],
        ),
        out_shape=[shape, shape],
        name="pick",
    )(position, returned)


def update(who, position, scale, returned, params, reps):
    blocks, rows, width = params.shape
    half = blocks // 2

    def body(who_ref, position_ref, scale_ref, one, two, params_ref, low, high, whole, picked, sems):
        copies = []
        for block in range(blocks):
            slot = position_ref[block]
            pair = (
                pltpu.make_async_copy(one.at[slot], picked.at[block, :, pl.ds(0, RAW)], sems.at[0, block]),
                pltpu.make_async_copy(
                    two.at[slot], picked.at[block, :, pl.ds(RAW, width - RAW)], sems.at[1, block]
                ),
            )
            for copy in pair:
                copy.start()
            copies.append(pair)
        for block, pair in enumerate(copies):
            for copy in pair:
                copy.wait()
            change = scale_ref[block] * picked[block].astype(f32)
            new = (params_ref[block].astype(f32) - change).astype(bf16)
            whole[0, block] = new
            if block < half:
                low[block] = new[:, RAW:]
            else:
                high[block - half] = new[:, RAW:]

    hbm = pl.BlockSpec(memory_space=pltpu.HBM)
    piece = pl.BlockSpec((half, rows, width - RAW), lambda i, w, p, s: (0, 0, 0))
    shape = jax.ShapeDtypeStruct((half, rows, width - RAW), bf16)
    return pl.pallas_call(
        body,
        grid_spec=pltpu.PrefetchScalarGridSpec(
            num_scalar_prefetch=3,
            grid=(1,),
            in_specs=[hbm, hbm, pl.BlockSpec((blocks, rows, width), lambda i, w, p, s: (0, 0, 0))],
            out_specs=[
                piece,
                piece,
                pl.BlockSpec((1, blocks, rows, width), lambda i, w, p, s: (w[0], 0, 0, 0)),
            ],
            scratch_shapes=[
                pltpu.VMEM((blocks, rows, width), bf16),
                pltpu.SemaphoreType.DMA((2, blocks)),
            ],
        ),
        out_shape=[shape, shape, jax.ShapeDtypeStruct((reps, blocks, rows, width), bf16)],
        name="update",
    )(who, position, scale, *returned, params)


def place(owners, scales, whole, raw, ready):
    half, rows, _ = (raw or ready)[0][2].shape
    blocks = 2 * half
    pieces = len(raw) + len(ready)

    def body(owners_ref, scales_ref, *refs):
        olds, changes = refs[: len(raw)], refs[len(raw) : 2 * len(raw)]
        values = refs[2 * len(raw) : 2 * len(raw) + len(ready)]
        out, made, sems = refs[-3:]
        copies = []
        for at, (offset, part, value) in enumerate([(o, p, None) for o, p, _, _ in raw] + list(ready)):
            owner = owners_ref[offset]
            if at < len(raw):
                for block in range(half):
                    scale = scales_ref[owner * blocks + part * half + block]
                    new = olds[at][block].astype(f32) - scale * changes[at][block].astype(f32)
                    made[at, block] = new.astype(bf16)
                source, columns = made.at[at], pl.ds(0, RAW)
            else:
                source = values[at - len(raw)]
                columns = pl.ds(RAW, value.shape[2])
            target = out.at[owner, pl.ds(part * half, half), :, columns]
            copies.append(pltpu.make_async_copy(source, target, sems.at[at]))
            copies[-1].start()
        for copy in copies:
            copy.wait()

    def block_of(array):
        return pl.BlockSpec(array.shape, lambda i, o, s: (0, 0, 0))

    arrays = [old for _, _, old, _ in raw] + [change for _, _, _, change in raw] + [v for _, _, v in ready]
    hbm = pl.BlockSpec(memory_space=pltpu.HBM)
    return pl.pallas_call(
        body,
        grid_spec=pltpu.PrefetchScalarGridSpec(
            num_scalar_prefetch=2,
            grid=(1,),
            in_specs=[*[block_of(array) for array in arrays], hbm],
            out_specs=hbm,
            scratch_shapes=[
                pltpu.VMEM((max(len(raw), 1), half, rows, RAW), bf16),
                pltpu.SemaphoreType.DMA((pieces,)),
            ],
        ),
        out_shape=jax.ShapeDtypeStruct(whole.shape, bf16),
        input_output_aliases={2 + len(arrays): 0},
    )(owners, scales, *arrays, whole)


def everywhere(value):
    value = value + lax.ppermute(value, "group_2", [(0, 1), (1, 0)])
    for axis in ("rep", "group_0", "group_1"):
        one, two, three = [lax.ppermute(value, axis, ring(4, step)) for step in (1, 2, 3)]
        value = (value + two) + (one + three)
    return value


def spread(low, high, reps):
    up, down = ring(reps, 1), ring(reps, -1)
    low_up = lax.ppermute(low, "rep", up)
    high_down = lax.ppermute(high, "rep", down)
    high_up = lax.ppermute(high, "rep", up)
    low_down = lax.ppermute(low, "rep", down)
    far_low = lax.ppermute(low_up, "rep", up)
    far_high = lax.ppermute(high_down, "rep", down)
    return (
        (3, 0, low_up),
        (1, 1, high_down),
        (3, 1, high_up),
        (1, 0, low_down),
        (2, 0, far_low),
        (2, 1, far_high),
    )


def local(grad_parts, params, accum, left_pre, right_pre, slot_block, layer_of):
    group_size = lax.axis_size(GROUP)
    reps = lax.axis_size("rep")
    me = lax.axis_index("rep")
    group_index = lax.axis_index(GROUP)
    blocks, rows, width = params.shape
    half = blocks // 2
    up, down = ring(reps, 1), ring(reps, -1)
    parts = grad_parts[0].reshape(reps, blocks, rows, width)
    who = lax.rem(me + jnp.arange(reps, dtype=jnp.int32), reps)
    table = lax.dynamic_index_in_dim(slot_block, me, 0, keepdims=False).reshape(-1)
    wanted = jnp.maximum(table, 0)
    left, right = left_pre[0, 0, 0], right_pre[0, 0, 0]

    far = lax.rem(me + 2, reps)
    gradients, earlier, owned = [None] * len(SENT), [], None
    for chunk, (start, cols) in enumerate(SENT):
        low = lax.dynamic_slice(parts, (far, 0, 0, start), (1, half, rows, cols))[0]
        high = lax.dynamic_slice(parts, (far, half, 0, start), (1, half, rows, cols))[0]
        far_up = lax.ppermute(low, "rep", up)
        far_down = lax.ppermute(high, "rep", down)
        to_up, to_down = merge(who, parts, far_up, far_down, start, cols)
        near_up = lax.ppermute(to_up, "rep", up)
        near_down = lax.ppermute(to_down, "rep", down)
        gradient, outgoing = finish(who, wanted, parts, near_up, near_down, start, cols)
        gradients[chunk] = gradient
        arrived = lax.all_to_all(outgoing, GROUP, split_axis=0, concat_axis=0, tiled=True)
        if chunk > 0:
            earlier.append(left_times(left, owned))
        owned = arrived.reshape(group_size * rows, cols)

    old_low, old_high = params[:half, :, :RAW], params[half:, :, :RAW]
    ahead = spread(old_low, old_high, reps)

    onehots = (layer_of[:, None] == jnp.arange(LAYERS, dtype=jnp.int32)[None, :]).astype(f32)
    onehot = lax.dynamic_slice_in_dim(onehots, me * blocks, blocks)
    mine = lax.dynamic_index_in_dim(table, group_index, 0, keepdims=False)
    chosen = (jnp.arange(blocks, dtype=jnp.int32) == mine).astype(f32)
    my_layer = jnp.sum(chosen[:, None] * onehot, axis=0)
    layer_row = jnp.pad(my_layer[None, :], ((0, 0), (0, LANES - LAYERS)))
    position = jnp.sum(
        jnp.where(
            table[None, :] == jnp.arange(blocks, dtype=jnp.int32)[:, None],
            jnp.arange(group_size, dtype=jnp.int32)[None, :],
            0,
        ),
        axis=1,
    )

    wide = jnp.concatenate(gradients, axis=2).astype(f32)
    new_accum = accum + wide * wide
    graft = wide * lax.rsqrt(new_accum)
    graft_blocks = jnp.sum(graft * graft, axis=(1, 2))
    graft_layer = jnp.sum(onehot * graft_blocks[:, None], axis=0)
    graft_row = jnp.pad(graft_layer[None, :], ((0, 1), (0, LANES - LAYERS)))
    owned, earlier, layer_row, graft_row, new_accum = lax.optimization_barrier(
        (owned, earlier, layer_row, graft_row, new_accum)
    )

    *preconds, sums = products(left, right, owned, earlier, layer_row)
    returned = []
    for precond in preconds:
        outgoing = precond.reshape(group_size, rows, precond.shape[1])
        returned.append(lax.all_to_all(outgoing, GROUP, split_axis=0, concat_axis=0, tiled=True))
    sums = everywhere(sums + graft_row)
    layer_scale = jnp.sqrt(sums[0, :LAYERS]) * lax.rsqrt(sums[1, :LAYERS] + 1e-06)
    scales = (step_rate * jnp.sum(onehots * layer_scale[None, :], axis=1)).reshape(reps, blocks)

    changes = spread(*pick(position, returned[0]), reps)
    low, high, new_params = update(who, position, scales[me], returned, params, reps)
    finished = spread(low, high, reps)

    raw = [(offset, part, old, change) for (offset, part, old), (_, _, change) in zip(ahead, changes)]
    flat = scales.reshape(-1)
    new_params = place(who, flat, new_params, raw[:4], ())
    new_params = place(who, flat, new_params, raw[4:], finished[:4])
    for offset, part, piece in finished[4:]:
        owner = lax.rem(me + offset, reps)
        new_params = lax.dynamic_update_slice(new_params, piece[None], (owner, part * half, 0, RAW))
    return (new_params.reshape(reps * blocks, rows, width), new_accum)


def solution(mesh):
    split = Mesh(mesh.devices.reshape(4, 4, 2, mesh.shape["rep"]), EVERY)
    placed = (
        P("rep", None, GROUP, None),
        P("rep", GROUP, None),
        P("rep", GROUP, None),
        P("rep", GROUP, None, None, None),
        P("rep", GROUP, None, None, None),
        P(),
        P(),
    )
    return jax.shard_map(
        local,
        mesh=split,
        in_specs=placed,
        out_specs=(P(None, GROUP, None), P("rep", GROUP, None)),
        check_vma=False,
    )
```
